32 devices in a mesh: groups: 2 (over y), rows: 4 (over z), cols: 4 (over x, core).
Axes of the slice: x: 2, y: 2, z: 4, core: 2. Of those that a mesh axis runs over, the one named last changes fastest.
Arguments:
- latent: bfloat16 [4, 32, 16], P(None, ('groups', 'rows'), 'cols'), parts along dimension 1, may hold values from -6 to 6
- w_in: bfloat16 [9, 4, 512], replicated, may hold values from -1 to 1
- w_mid: bfloat16 [9, 256, 512], replicated, may hold values from -0.09375 to 0.09375
- w_low: bfloat16 [9, 128, 256], replicated, may hold values from -0.125 to 0.125
- w_out: bfloat16 [9, 3, 128], replicated, may hold values from -0.1875 to 0.1875
- ramp_rows: int32 [4, 32], replicated, may hold values from 0 to 8, as said below
- ramp_cols: int32 [4, 32], replicated, may hold values from 0 to 8, as said below
- intersection_rows: int32 [4], replicated, may hold values from 1 to 8
- intersection_cols: int32 [4], replicated, may hold values from 1 to 8
Outputs:
- image: float32 [3, 128, 64], P(None, ('groups', 'rows'), 'cols'), parts along dimension 1
The draws below stay inside these ranges and needn't reach their ends.
There are 2 independent parts, one for each index of `groups`. The reference program is written for one: setup_inputs(seed, part) draws one part's arguments, and reference() takes and returns one part's arrays. A program takes and returns all parts, laid end to end along the dimension named above; an argument that names none is the same for every part. Nothing has to cross between parts.
Inputs may be any that keep to these rules, and one draw needn't show every extreme that they name: `ramp_rows`: entries at the inner 4 * 4 pixels of each row of the table are 1 or more. `ramp_cols`: entries at the inner 4 * 4 pixels of each row of the table are 1 or more.
All inputs are finite; a program needn't handle non-finite values.
Results may differ from the reference program's by a relative error of at most 0.0049.
Values may be sent and summed in bfloat16 or wider, within the bound.
A program may use at most 64 MiB of HBM per device.

```python
import jax
import jax.numpy as jnp
from jax import lax

C_LAT = 4
C1 = 512
C2 = 256
C3 = 128
NGROUPS = 32
C_OUT = 3
TILE = 4
HALO = 2
MARGIN = 8
LAT_H = 16
LAT_W = 16
IMG_H = 64
IMG_W = 64
N_ROWS = 4
N_COLS = 4


def ramp_draw(key, count):
    margin = 4 * HALO
    inner_px = 4 * TILE
    positions = jnp.arange(inner_px + 2 * margin, dtype=jnp.int32)
    interior = (positions >= margin) & (positions < margin + inner_px)
    strong = jax.random.randint(jax.random.fold_in(key, 11), (count, inner_px + 2 * margin), 1, 9)
    loose = jax.random.randint(jax.random.fold_in(key, 12), (count, inner_px + 2 * margin), 0, 9)
    return jnp.where(interior[None, :], strong, loose).astype(jnp.int32)


def draw_ramp_rows(key, part):
    return ramp_draw(jax.random.fold_in(key, 21), N_ROWS)


def draw_ramp_cols(key, part):
    return ramp_draw(jax.random.fold_in(key, 22), N_COLS)


def with_ends(values, rng, low, high):
    extent = values.shape
    index_at = [jax.random.randint(jax.random.fold_in(rng, axis), (), 0, extent[axis]) for axis in range(len(extent))]
    values = values.at[tuple(index_at)].set(low)
    longest = extent.index(max(extent))
    index_at[longest] = (index_at[longest] + 1) % extent[longest]
    return values.at[tuple(index_at)].set(high)


def steps_of(stream_key, dims, pieces, least, top_value):
    def one(axis_at, shards_of):
        steps = jax.random.uniform(jax.random.fold_in(jax.random.fold_in(stream_key, 6), axis_at), (shards_of,), jnp.float32, least / len(pieces), top_value / len(pieces))
        return jnp.repeat(jnp.exp(steps), dims[axis_at] // shards_of).reshape((-1,) + (1,) * (len(dims) - axis_at - 1))

    factor_of = one(*pieces[0])
    for cut in pieces[1:]:
        factor_of = factor_of * one(*cut)
    return factor_of


def noise(stream_key, extent, deviation, bound, shards=(), kind=jnp.bfloat16):
    drawn = deviation * jax.random.normal(stream_key, extent, jnp.float32)
    if shards:
        drawn = drawn * steps_of(stream_key, extent, shards, -0.22, 0.18)
    return jnp.clip(drawn, -bound, bound).astype(kind)


def setup_inputs(seed: int = 0, part: int = 0) -> dict:
    keys = jax.random.split(jax.random.key(seed), 10)
    part_keys = jax.random.split(jax.random.fold_in(keys[9], part), 10)
    return {
        "latent": noise(part_keys[0], (C_LAT, LAT_H, LAT_W), 1.0, 6.0, ((1, 4), (2, 4))),
        "w_in": noise(keys[1], (9, C_LAT, C1), (9 * C_LAT) ** -0.5, 1.0),
        "w_mid": noise(keys[2], (9, C2, C1), (9 * C1) ** -0.5, 0.09375),
        "w_low": noise(keys[3], (9, C3, C2), (9 * C2) ** -0.5, 0.125),
        "w_out": noise(keys[4], (9, C_OUT, C3), (9 * C3) ** -0.5, 0.1875),
        "ramp_rows": draw_ramp_rows(jax.random.fold_in(keys[9], 71), part),
        "ramp_cols": draw_ramp_cols(jax.random.fold_in(keys[9], 71), part),
        "intersection_rows": with_ends(jax.random.randint(keys[7], (N_ROWS,), 1, MARGIN + 1), jax.random.fold_in(keys[7], 1), 1, MARGIN).astype(jnp.int32),
        "intersection_cols": with_ends(jax.random.randint(keys[8], (N_COLS,), 1, MARGIN + 1), jax.random.fold_in(keys[8], 1), 1, MARGIN).astype(jnp.int32),
    }


def conv_three(values, kernel, out_first):
    height, across, channels = values.shape
    out_width = kernel.shape[1] if out_first else kernel.shape[2]
    padded = jnp.pad(values, ((1, 1), (1, 1), (0, 0)))
    accumulated = jnp.zeros((height * across, out_width), jnp.float32)
    for kernel_tap in range(9):
        row_off = kernel_tap // 3
        col_off = kernel_tap % 3
        window = padded[row_off:row_off + height, col_off:col_off + across, :].reshape(height * across, channels)
        if out_first:
            product = lax.dot_general(window, kernel[kernel_tap], (((1,), (1,)), ((), ())), preferred_element_type=jnp.float32)
        else:
            product = jnp.dot(window, kernel[kernel_tap], preferred_element_type=jnp.float32)
        accumulated = accumulated + product
    return accumulated.reshape(height, across, out_width)

def group_silu(values):
    height, across, channels = values.shape
    grouped = values.reshape(height * across, NGROUPS, channels // NGROUPS)
    center = lax.optimization_barrier(jnp.mean(grouped, axis=(0, 2), keepdims=True))
    shifted = grouped - center
    spread = lax.optimization_barrier(jnp.mean(shifted * shifted, axis=(0, 2), keepdims=True))
    normed = (shifted * lax.rsqrt(spread + 1e-06)).reshape(height, across, channels)
    return jax.nn.silu(normed).astype(jnp.bfloat16)

def upsample(values):
    return jnp.repeat(jnp.repeat(values, 2, axis=0), 2, axis=1)

def decode_tile(patched, w_in, w_mid, w_low, w_out):
    cell_grid = jnp.transpose(patched, (1, 2, 0))
    first_act = group_silu(conv_three(cell_grid, w_in, False))
    second = group_silu(conv_three(upsample(first_act), w_mid, True))
    third_act = group_silu(conv_three(upsample(second), w_low, True))
    return jnp.transpose(conv_three(third_act, w_out, True), (2, 0, 1))

def masked_ramp(ramp_table, intersection, margin, inner_px):
    positions = jnp.arange(ramp_table.shape[1], dtype=jnp.int32)
    distance = jnp.maximum(jnp.maximum(margin - positions, positions - (margin + inner_px) + 1), 0)
    return jnp.where(distance[None, :] <= intersection[:, None], ramp_table, 0).astype(jnp.float32)

def reference(latent, w_in, w_mid, w_low, w_out, ramp_rows, ramp_cols, intersection_rows, intersection_cols):
    margin = 4 * HALO
    inner_px = 4 * TILE
    row_table = masked_ramp(ramp_rows, intersection_rows, margin, inner_px)
    col_table = masked_ramp(ramp_cols, intersection_cols, margin, inner_px)
    framed = jnp.pad(latent, ((0, 0), (HALO, HALO), (HALO, HALO)))
    canvas = jnp.zeros((C_OUT + 1, IMG_H + 2 * margin, IMG_W + 2 * margin), jnp.float32)

    def place_tile(tile_index, canvas):
        tile_index = jnp.asarray(tile_index).astype(jnp.int32)
        row_idx = tile_index // N_COLS
        col_idx = tile_index % N_COLS
        patched = lax.dynamic_slice(framed, (jnp.int32(0), row_idx * TILE, col_idx * TILE), (C_LAT, TILE + 2 * HALO, TILE + 2 * HALO))
        pixels = decode_tile(patched, w_in, w_mid, w_low, w_out)
        weights = row_table[row_idx][:, None] * col_table[col_idx][None, :]
        stacked = jnp.concatenate([pixels * weights[None], weights[None]], 0)
        corner = (jnp.int32(0), row_idx * inner_px, col_idx * inner_px)
        current = lax.dynamic_slice(canvas, corner, stacked.shape)
        return lax.dynamic_update_slice(canvas, current + stacked, corner)
    canvas = lax.fori_loop(0, N_ROWS * N_COLS, place_tile, canvas)
    inside = canvas[:, margin:margin + IMG_H, margin:margin + IMG_W]
    return inside[:C_OUT] / inside[C_OUT]
```

```python
import functools

import jax
import jax.numpy as jnp
from jax import lax
from jax.experimental import pallas as pl
from jax.experimental.pallas import tpu as pltpu
from jax.sharding import PartitionSpec as P

MESH = pl.DeviceIdType.MESH
NGROUPS = 32
HALO = 2
F32 = jnp.float32
BF16 = jnp.bfloat16
AROUND = [(dr, dc) for dr in (-1, 0, 1) for dc in (-1, 0, 1) if (dr, dc) != (0, 0)]
FAR_FIRST = sorted(enumerate(AROUND), key=lambda e: -abs(e[1][0]) - abs(e[1][1]))
EARLIER = [(k, *to) for k, to in FAR_FIRST if k < 4]
LATER = [(k, *to) for k, to in FAR_FIRST if k >= 4]


def iota(shape, dim):
    return lax.broadcasted_iota(jnp.int32, shape, dim)


def nt_dot(a, b):
    return lax.dot_general(a, b, (((1,), (1,)), ((), ())), preferred_element_type=F32)


def dot(a, b):
    return jnp.dot(a, b, preferred_element_type=F32)


def down(x):
    return jnp.concatenate([jnp.zeros_like(x[:1]), x[:-1]], axis=0)


def up(x):
    return jnp.concatenate([x[1:], jnp.zeros_like(x[:1])], axis=0)


def right(x):
    rolled = pltpu.roll(x, 1, 1)
    return jnp.where(iota(x.shape, 1) == 0, 0.0, rolled)


def left(x):
    n = x.shape[1]
    rolled = pltpu.roll(x, n - 1, 1)
    return jnp.where(iota(x.shape, 1) == n - 1, 0.0, rolled)


def expand(products, fine, before, after):
    out = []
    for q in range(fine):
        t0, t1, t2 = products[q]
        prev = products[q - 1][0] if q > 0 else before(products[fine - 1][0])
        nxt = products[q + 1][2] if q < fine - 1 else after(products[0][2])
        out.append(prev + (t1 + t2))
        out.append((t0 + t1) + nxt)
    return out


def conv_up(taps, fine):
    by_col = [
        [
            expand(
                [[taps[py][px][3 * dy + dx] for dy in range(3)] for py in range(fine)],
                fine,
                down,
                up,
            )
            for dx in range(3)
        ]
        for px in range(fine)
    ]
    return [
        expand(
            [[by_col[px][dx][qy] for dx in range(3)] for px in range(fine)],
            fine,
            right,
            left,
        )
        for qy in range(2 * fine)
    ]


def segment_sum(x, block):
    count = x.shape[1] // 128
    rows = jnp.concatenate([x[:, k * 128 : (k + 1) * 128] for k in range(count)], axis=0)
    top = rows.astype(BF16)
    rest = rows - top.astype(F32)
    mid = rest.astype(BF16)
    low = (rest - mid.astype(F32)).astype(BF16)
    n = rows.shape[0]
    got = dot(jnp.concatenate([top, mid, low], axis=0), block)
    got = got[:n] + got[n : 2 * n] + got[2 * n :]
    sums = [jnp.sum(got[8 * k : 8 * k + 8], axis=0, keepdims=True) for k in range(count)]
    return jnp.concatenate(sums, axis=1) if count > 1 else sums[0]


def group_silu(phases):
    channels = phases[0].shape[-1]
    width = channels // NGROUPS
    positions = len(phases) * phases[0].shape[0] * phases[0].shape[1]
    scale = 1.0 / (positions * width)
    block = (iota((128, 128), 0) // width == iota((128, 128), 1) // width).astype(F32)
    block = block.astype(BF16)
    total = jnp.sum(functools.reduce(jnp.add, phases), axis=0)
    center = (segment_sum(total, block) * scale)[None]
    shifted = [p - center for p in phases]
    squares = jnp.sum(functools.reduce(jnp.add, [s * s for s in shifted]), axis=0)
    spread = segment_sum(squares, block) * scale
    factor = (0.5 * lax.rsqrt(spread + 1e-06))[None]
    result = []
    for s in shifted:
        half = s * factor
        result.append(half + half * jnp.tanh(half))
    return result


def table_rows(table, limits, index, count, margin, inner):
    size = table.shape[1]
    pos = iota((1, size), 1)
    far = jnp.maximum(jnp.maximum(margin - pos, pos - (margin + inner) + 1), 0)
    rows = []
    for d in (-1, 0, 1):
        here = index + d
        limit = limits[jnp.clip(here, 0, count - 1)]
        picked = jnp.where(iota(table.shape, 0) == here, table, 0.0)
        row = jnp.sum(picked, axis=0, keepdims=True)
        rows.append(jnp.where(far <= limit, row, 0.0))
    above, own, below = rows
    other = jnp.where(pos < inner, jnp.roll(above, inner, 1), jnp.roll(below, inner, 1))
    pair = jnp.concatenate([own, own + other, jnp.zeros((6, size), F32)], axis=0)
    return pair.astype(BF16)


def kernel(
    nr, nc, lat, w_in, w_mid, w_low, w_out, ramp_r, ramp_c, lim_r, lim_c, out,
    cells, wi, wm, wl, wo, tr, tc, lr, lc, wi32, wo32, own, side_out, vert_out, sides, corners, verts,
    local_sem, ready, send1, recv1, send2, recv2,
):
    row, col = lax.axis_index("rows"), lax.axis_index("cols")

    def exists(dr, dc):
        ok = None
        for d, here, n in ((dr, row, nr), (dc, col, nc)):
            test = None if d == 0 else (here > 0 if d < 0 else here < n - 1)
            if test is not None:
                ok = test if ok is None else jnp.logical_and(ok, test)
        return ok

    def device(dr, dc):
        return {"rows": row + dr, "cols": col + dc}

    loads = [
        pltpu.make_async_copy(src, dst, local_sem.at[k])
        for k, (src, dst) in enumerate(
            [
                (lat, cells.at[4]),
                (w_in, wi),
                (ramp_r, tr),
                (ramp_c, tc),
                (lim_r, lr),
                (lim_c, lc),
                (w_mid, wm),
                (w_low, wl),
                (w_out, wo),
            ]
        )
    ]
    for load in loads:
        load.start()

    barrier = pltpu.get_barrier_semaphore()
    for k, dr, dc in LATER:

        @pl.when(exists(dr, dc))
        def _():
            pl.semaphore_signal(barrier, inc=1, device_id=device(dr, dc), device_id_type=MESH)

    def slot_of(dr, dc):
        up_down, left_right = (dr + 1) // 2, (dc + 1) // 2
        if dr == 0:
            return sides.at[left_right]
        return verts.at[up_down] if dc == 0 else corners.at[left_right, up_down]

    def packed(dr, dc):
        up_down, left_right = (dr + 1) // 2, (dc + 1) // 2
        if dr == 0:
            return side_out.at[left_right]
        return vert_out.at[up_down] if dc == 0 else side_out.at[left_right, up_down]

    def copies(k, dr, dc):
        first = pltpu.make_async_remote_copy(
            src_ref=cells.at[4],
            dst_ref=cells.at[(1 - dr) * 3 + 1 - dc],
            send_sem=send1.at[k],
            recv_sem=recv1.at[7 - k],
            device_id=device(dr, dc),
            device_id_type=MESH,
        )
        second = pltpu.make_async_remote_copy(
            src_ref=packed(dr, dc),
            dst_ref=slot_of(-dr, -dc),
            send_sem=send2.at[k],
            recv_sem=recv2.at[7 - k],
            device_id=device(dr, dc),
            device_id_type=MESH,
        )
        return first, second

    def arrival(k, dr, dc):
        first = pltpu.make_async_remote_copy(
            src_ref=cells.at[4],
            dst_ref=cells.at[(1 + dr) * 3 + 1 + dc],
            send_sem=send1.at[k],
            recv_sem=recv1.at[k],
            device_id=device(dr, dc),
            device_id_type=MESH,
        )
        second = pltpu.make_async_remote_copy(
            src_ref=packed(dr, dc),
            dst_ref=slot_of(dr, dc),
            send_sem=send2.at[k],
            recv_sem=recv2.at[k],
            device_id=device(dr, dc),
            device_id_type=MESH,
        )
        return first, second

    for k, (dr, dc) in enumerate(AROUND):

        @pl.when(jnp.logical_not(exists(dr, dc)))
        def _():
            slot = cells.at[(1 + dr) * 3 + 1 + dc]
            slot[...] = jnp.zeros(slot.shape, BF16)
            pixels = slot_of(dr, dc)
            pixels[...] = jnp.zeros(pixels.shape, F32)

    earlier = (col > 0).astype(jnp.int32) + (row > 0).astype(jnp.int32) * (
        1 + (col > 0).astype(jnp.int32) + (col < nc - 1).astype(jnp.int32)
    )

    @pl.when(row + col > 0)
    def _():
        pl.semaphore_wait(barrier, earlier)

    for k, dr, dc in EARLIER:

        @pl.when(exists(dr, dc))
        def _():
            pl.semaphore_signal(
                ready.at[3 - k], inc=1, device_id=device(dr, dc), device_id_type=MESH
            )

    loads[0].wait()
    for k, dr, dc in EARLIER:

        @pl.when(exists(dr, dc))
        def _():
            copies(k, dr, dc)[0].start()

    def send_later(entries):
        for k, dr, dc in entries:

            @pl.when(exists(dr, dc))
            def _():
                pl.semaphore_wait(ready.at[k - 4], 1)
                copies(k, dr, dc)[0].start()

    send_later([e for e in LATER if e[1] == 0])
    loads[1].wait()
    wi32[...] = jnp.zeros(wi32.shape, F32)
    wi32[:, 0 : wi.shape[1], :] = wi[...].astype(F32)
    loads[8].wait()
    wo32[...] = jnp.zeros(wo32.shape, F32)
    wo32[:, 0 : wo.shape[1], :] = wo[...].astype(F32)
    for k in (2, 3, 4, 5):
        loads[k].wait()

    tile = lat.shape[1]
    side_cells = tile + 2 * HALO
    margin, inner = 4 * HALO, 4 * tile
    size = inner + 2 * margin
    chans = lat.shape[0]

    span = size * side_cells
    spread_r = (iota((size, span), 1) // side_cells == iota((size, span), 0)).astype(F32)
    spread_c = [
        (4 * (iota((size, span), 1) % side_cells) + q == iota((size, span), 0)).astype(F32)
        for q in range(4)
    ]
    spread_c = jnp.concatenate(spread_c, axis=1)
    row_w = dot(table_rows(tr[...].astype(F32), lr, row, nr, margin, inner), spread_r.astype(BF16))
    col_w = dot(table_rows(tc[...].astype(F32), lc, col, nc, margin, inner), spread_c.astype(BF16))
    lane = iota((1, span), 1)
    r_of, b_of = lane // side_cells, lane % side_cells
    inside = (
        (r_of >= margin) & (r_of < margin + inner) & (b_of >= HALO) & (b_of < HALO + tile)
    )
    blend, inverse = [], []
    for q in range(4):
        cw = col_w[:, q * span : (q + 1) * span]
        blend.append(row_w[0:1] * cw[0:1])
        inverse.append(1.0 / jnp.where(inside, row_w[1:2] * cw[1:2], 1.0))

    wide = chans * side_cells
    src, dst = iota((3 * wide, 72), 0), iota((3 * wide, 72), 1)
    pick = [
        (
            (dst // 8 == 3 * (src // wide) + dx)
            & (dst % 8 == (src // side_cells) % chans)
        ).astype(F32).astype(BF16)
        for dx in range(3)
    ]
    wi72 = wi32[...].reshape(72, wi32.shape[2]).astype(BF16)

    send_later([e for e in LATER if e[1] != 0])
    for k, (dr, dc) in enumerate(AROUND):

        @pl.when(exists(dr, dc))
        def _():
            arrival(k, dr, dc)[0].wait_recv()

    cell = [[cells[3 * i + j].astype(F32) for j in range(3)] for i in range(3)]
    bands = [
        jnp.concatenate([cell[0][j][:, tile - HALO :], cell[1][j], cell[2][j][:, :HALO]], axis=1)
        for j in range(3)
    ]
    grid = jnp.concatenate([bands[0][:, :, tile - HALO :], bands[1], bands[2][:, :, :HALO]], axis=2)
    flat = jnp.concatenate([grid[c] for c in range(chans)], axis=1)
    zero = jnp.zeros((1, wide), F32)
    tall = jnp.concatenate(
        [
            jnp.concatenate([zero, flat[:-1]], axis=0),
            flat,
            jnp.concatenate([flat[1:], zero], axis=0),
        ],
        axis=1,
    )
    shape = (side_cells, side_cells, 3 * wide)
    spreaded = jnp.broadcast_to(tall[:, None, :], shape)
    gap = iota(shape, 2) % side_cells - iota(shape, 1)
    patches = 0.0
    for dx in range(3):
        chosen = jnp.where(gap == dx - 1, spreaded, 0.0)
        patches = patches + dot(chosen.reshape(-1, 3 * wide).astype(BF16), pick[dx])
    first = dot(patches.astype(BF16), wi72).reshape(side_cells, side_cells, -1)
    (first,) = group_silu([first])
    first = first.reshape(side_cells * side_cells, -1).astype(BF16)

    loads[6].wait()
    taps = [nt_dot(first, wm[t]).reshape(side_cells, side_cells, -1) for t in range(9)]
    second = conv_up([[taps]], 1)
    second = group_silu([second[py][px] for py in range(2) for px in range(2)])
    second = jnp.concatenate(second, axis=0)
    second = second.reshape(-1, second.shape[2]).astype(BF16)

    loads[7].wait()
    n = side_cells * side_cells
    products = [nt_dot(second, wl[t]) for t in range(9)]
    taps = [
        [
            [
                p[(2 * py + px) * n : (2 * py + px + 1) * n].reshape(side_cells, side_cells, -1)
                for p in products
            ]
            for px in range(2)
        ]
        for py in range(2)
    ]
    third = conv_up(taps, 2)
    third = group_silu([third[qy][qx] for qy in range(4) for qx in range(4)])

    wo72 = wo32[...].reshape(72, wo32.shape[2]).astype(BF16)
    colour = []
    for qx in range(4):
        rows = jnp.stack([third[4 * qy + qx] for qy in range(4)], axis=1)
        colour.append(nt_dot(wo72, rows.reshape(span, rows.shape[-1]).astype(BF16)))

    def tap(q, t):
        return colour[q][8 * t : 8 * t + 8]

    half = span // 2
    where_b = iota((4, half), 1) % side_cells
    lower_half = iota((4, half), 1) < half // 2
    sub_b = iota((8, span), 1) % side_cells
    sub_r = iota((8, span), 1) // side_cells
    for q in range(4):
        by_row = []
        for dy in range(3):
            if q > 0:
                before = tap(q - 1, 3 * dy)
            else:
                before = jnp.where(sub_b == 0, 0.0, pltpu.roll(tap(3, 3 * dy), 1, 1))
            if q < 3:
                after = tap(q + 1, 3 * dy + 2)
            else:
                after = jnp.where(
                    sub_b == side_cells - 1, 0.0, pltpu.roll(tap(0, 3 * dy + 2), span - 1, 1)
                )
            by_row.append(before + tap(q, 3 * dy + 1) + after)
        value = (
            jnp.where(sub_r == 0, 0.0, pltpu.roll(by_row[0], side_cells, 1))
            + by_row[1]
            + jnp.where(sub_r == size - 1, 0.0, pltpu.roll(by_row[2], span - side_cells, 1))
        ) * blend[q]
        for h in range(2):
            own[h, q] = value[0:4, h * half : (h + 1) * half]

    for h in range(2):
        for k, rim in ((0, 0), (1, side_cells - HALO)):
            dense = pltpu.roll(own[h, 0], (half - rim) % half, 1)
            for q in range(1, 4):
                moved = pltpu.roll(own[h, q], (HALO * q - rim) % half, 1)
                dense = jnp.where(where_b // HALO == q, moved, dense)
            side_out[k, h] = dense
        for pair in range(2):
            even, odd = own[h, 2 * pair], own[h, 2 * pair + 1]
            if h == 0:
                odd = pltpu.roll(odd, half // 2, 1)
            else:
                even = pltpu.roll(even, half // 2, 1)
            vert_out[h, pair] = jnp.where(lower_half, even, odd)

    for k, (dr, dc) in FAR_FIRST:

        @pl.when(exists(dr, dc))
        def _():
            copies(k, dr, dc)[1].start()

    place_src, place_dst = iota((4 * half, inner), 0), iota((4 * half, inner), 1)
    place = (place_dst == 4 * (place_src % side_cells - HALO) + place_src // half)
    place = place.astype(F32).astype(BF16)
    lane_row = iota((8, half), 1) // side_cells
    sublane = iota((8, half), 0)
    keep = [lane_row == sublane + 8, lane_row == sublane]

    for k, (dr, dc) in enumerate(AROUND):

        @pl.when(exists(dr, dc))
        def _():
            arrival(k, dr, dc)[1].wait_recv()

    blocks = [[], [], []]
    for h in range(2):
        pieces = []
        lft = sides[0, h] + corners[0, h]
        rgt = sides[1, h] + corners[1, h]
        for q in range(4):
            beyond = verts[h, q // 2]
            if (q + h) % 2 == 0:
                beyond = pltpu.roll(beyond, half // 2, 1)
            lft_q = pltpu.roll(lft, (HALO - HALO * q) % half, 1)
            rgt_q = pltpu.roll(rgt, (tile - HALO * q) % half, 1)
            mid = own[h, q] + beyond + jnp.where(where_b < side_cells // 2, lft_q, rgt_q)
            pieces.append(mid * inverse[q][:, h * half : (h + 1) * half])
        for c in range(3):
            spread_rows = [
                jnp.where(keep[h], jnp.broadcast_to(p[c : c + 1], (8, half)), 0.0) for p in pieces
            ]
            blocks[c].append(jnp.concatenate(spread_rows, axis=1))
    tall = jnp.concatenate([b for c in range(3) for b in blocks[c]], axis=0)
    top = tall.astype(BF16)
    low = (tall - top.astype(F32)).astype(BF16)
    image = dot(top, place) + dot(low, place)
    out[...] = image.reshape(3, inner, inner)

    for k, (dr, dc) in enumerate(AROUND):

        @pl.when(exists(dr, dc))
        def _():
            for copy in copies(k, dr, dc):
                copy.wait_send()


def solution(mesh):
    nr, nc = mesh.shape["rows"], mesh.shape["cols"]

    def per_device(lat, w_in, w_mid, w_low, w_out, ramp_r, ramp_c, lim_r, lim_c):
        tile = lat.shape[1]
        inner = 4 * tile
        size = inner + 8 * HALO
        half = size * (tile + 2 * HALO) // 2
        anywhere = pl.BlockSpec(memory_space=pltpu.HBM)
        dma = pltpu.SemaphoreType.DMA
        return pl.pallas_call(
            functools.partial(kernel, nr, nc),
            out_shape=pltpu.VMEM((w_out.shape[1], inner, inner), F32),
            in_specs=[anywhere] * 9,
            out_specs=pl.BlockSpec(memory_space=pltpu.VMEM),
            scratch_shapes=[
                pltpu.VMEM((9,) + lat.shape, BF16),
                pltpu.VMEM(w_in.shape, BF16),
                pltpu.VMEM(w_mid.shape, BF16),
                pltpu.VMEM(w_low.shape, BF16),
                pltpu.VMEM(w_out.shape, BF16),
                pltpu.VMEM(ramp_r.shape, jnp.int32),
                pltpu.VMEM(ramp_c.shape, jnp.int32),
                pltpu.SMEM(lim_r.shape, jnp.int32),
                pltpu.SMEM(lim_c.shape, jnp.int32),
                pltpu.VMEM((9, 8, w_in.shape[2]), F32),
                pltpu.VMEM((9, 8, w_out.shape[2]), F32),
                pltpu.VMEM((2, 4, 4, half), F32),
                pltpu.VMEM((2, 2, 4, half), F32),
                pltpu.VMEM((2, 2, 4, half), F32),
                pltpu.VMEM((2, 2, 4, half), F32),
                pltpu.VMEM((2, 2, 4, half), F32),
                pltpu.VMEM((2, 2, 4, half), F32),
                dma((9,)),
                pltpu.SemaphoreType.REGULAR((4,)),
                dma((8,)),
                dma((8,)),
                dma((8,)),
                dma((8,)),
            ],
            compiler_params=pltpu.CompilerParams(
                collective_id=0, has_side_effects=True
            ),
            name="decode",
        )(lat, w_in, w_mid, w_low, w_out, ramp_r, ramp_c, lim_r, lim_c)

    return jax.shard_map(
        per_device,
        mesh=mesh,
        in_specs=(P(None, ("groups", "rows"), "cols"), P(), P(), P(), P(), P(), P(), P(), P()),
        out_specs=P(None, ("groups", "rows"), "cols"),
        check_vma=False,
    )
```

```python
import functools

import jax
import jax.numpy as jnp
from jax import lax
from jax.experimental import pallas as pl
from jax.experimental.pallas import tpu as pltpu
from jax.sharding import PartitionSpec as P

MESH = pl.DeviceIdType.MESH
NGROUPS = 32
HALO = 2
F32 = jnp.float32
BF16 = jnp.bfloat16
AROUND = [(dr, dc) for dr in (-1, 0, 1) for dc in (-1, 0, 1) if (dr, dc) != (0, 0)]
FAR_FIRST = sorted(enumerate(AROUND), key=lambda e: -abs(e[1][0]) - abs(e[1][1]))
EARLIER = [(k, *to) for k, to in FAR_FIRST if k < 4]
LATER = [(k, *AROUND[k]) for k in range(4, 8)]


def iota(shape, dim):
    return lax.broadcasted_iota(jnp.int32, shape, dim)


def nt_dot(a, b):
    return lax.dot_general(a, b, (((1,), (1,)), ((), ())), preferred_element_type=F32)


def dot(a, b):
    return jnp.dot(a, b, preferred_element_type=F32)


def down(x):
    return jnp.concatenate([jnp.zeros_like(x[:1]), x[:-1]], axis=0)


def up(x):
    return jnp.concatenate([x[1:], jnp.zeros_like(x[:1])], axis=0)


def right(x):
    rolled = pltpu.roll(x, 1, 1)
    return jnp.where(iota(x.shape, 1) == 0, 0.0, rolled)


def left(x):
    n = x.shape[1]
    rolled = pltpu.roll(x, n - 1, 1)
    return jnp.where(iota(x.shape, 1) == n - 1, 0.0, rolled)


def expand(products, fine, before, after):
    out = []
    for q in range(fine):
        t0, t1, t2 = products[q]
        prev = products[q - 1][0] if q > 0 else before(products[fine - 1][0])
        nxt = products[q + 1][2] if q < fine - 1 else after(products[0][2])
        out.append(prev + (t1 + t2))
        out.append((t0 + t1) + nxt)
    return out


def conv_up(taps, fine):
    by_col = [
        [
            expand(
                [[taps[py][px][3 * dy + dx] for dy in range(3)] for py in range(fine)],
                fine,
                down,
                up,
            )
            for dx in range(3)
        ]
        for px in range(fine)
    ]
    return [
        expand(
            [[by_col[px][dx][qy] for dx in range(3)] for px in range(fine)],
            fine,
            right,
            left,
        )
        for qy in range(2 * fine)
    ]


def group_silu(phases):
    channels = phases[0].shape[-1]
    width = channels // NGROUPS
    count = channels // 128
    positions = len(phases) * phases[0].shape[0] * phases[0].shape[1]
    scale = 1.0 / (positions * width)
    block = (iota((384, 128), 0) % 128 // width == iota((384, 128), 1) // width).astype(F32)
    block = block.astype(BF16)
    total = jnp.sum(functools.reduce(jnp.add, phases), axis=(0, 1)).reshape(1, channels)
    squares = functools.reduce(jnp.add, [p * p for p in phases])
    squares = jnp.sum(squares, axis=(0, 1)).reshape(1, channels)
    rows = [x[:, k * 128 : (k + 1) * 128] for x in (total, squares) for k in range(count)]
    rows = jnp.concatenate(rows + [jnp.zeros((1, 128), F32)] * (8 - len(rows)), axis=0)
    top = rows.astype(BF16)
    rest = rows - top.astype(F32)
    mid = rest.astype(BF16)
    low = (rest - mid.astype(F32)).astype(BF16)
    got = dot(jnp.concatenate([top, mid, low], axis=1), block) * scale
    center = got[:count]
    spread = jnp.maximum(got[count : 2 * count] - center * center, 0.0)
    factor = 0.5 * lax.rsqrt(spread + 1e-06)
    offset = center * factor
    factor = jnp.concatenate([factor[k : k + 1] for k in range(count)], axis=1)[None]
    offset = jnp.concatenate([offset[k : k + 1] for k in range(count)], axis=1)[None]
    result = []
    for p in phases:
        half = p * factor - offset
        result.append(half + half * jnp.tanh(half))
    return result


def table_rows(table, limits, index, count, margin, inner):
    size = table.shape[1]
    pos = iota((1, size), 1)
    far = jnp.maximum(jnp.maximum(margin - pos, pos - (margin + inner) + 1), 0)
    rows = []
    for d in (-1, 0, 1):
        here = index + d
        limit = limits[jnp.clip(here, 0, count - 1)]
        picked = jnp.where(iota(table.shape, 0) == here, table, 0.0)
        row = jnp.sum(picked, axis=0, keepdims=True)
        rows.append(jnp.where(far <= limit, row, 0.0))
    above, own, below = rows
    other = jnp.where(pos < inner, jnp.roll(above, inner, 1), jnp.roll(below, inner, 1))
    pair = jnp.concatenate([own, own + other, jnp.zeros((6, size), F32)], axis=0)
    return pair.astype(BF16)


def kernel(
    nr, nc, lat, w_in, w_mid, w_low, w_out, ramp_r, ramp_c, lim_r, lim_c, out,
    cells, wi, wm, wl, wo, tr, tc, lr, lc, wi32, wo32, own, side_out, vert_out, rims,
    local_sem, ready, send1, recv1, send2, recv2,
):
    row, col = lax.axis_index("rows"), lax.axis_index("cols")

    def exists(dr, dc):
        ok = None
        for d, here, n in ((dr, row, nr), (dc, col, nc)):
            test = None if d == 0 else (here > 0 if d < 0 else here < n - 1)
            if test is not None:
                ok = test if ok is None else jnp.logical_and(ok, test)
        return ok

    def device(dr, dc):
        return {"rows": row + dr, "cols": col + dc}

    loads = [
        pltpu.make_async_copy(src, dst, local_sem.at[k])
        for k, (src, dst) in enumerate(
            [
                (lat, cells.at[4]),
                (w_in, wi),
                (ramp_r, tr),
                (ramp_c, tc),
                (lim_r, lr),
                (lim_c, lc),
                (w_out, wo),
                (w_mid, wm),
                (w_low, wl),
            ]
        )
    ]
    for load in loads:
        load.start()

    barrier = pltpu.get_barrier_semaphore()
    for k, dr, dc in LATER:

        @pl.when(exists(dr, dc))
        def _():
            pl.semaphore_signal(barrier, inc=1, device_id=device(dr, dc), device_id_type=MESH)

    def slot_of(dr, dc):
        up_down, left_right = (dr + 1) // 2, (dc + 1) // 2
        if dr == 0:
            return rims.at[pl.ds(2 * left_right, 2)]
        if dc == 0:
            return rims.at[pl.ds(8 + 2 * up_down, 2)]
        return rims.at[4 + 2 * left_right + up_down]

    def packed(dr, dc):
        up_down, left_right = (dr + 1) // 2, (dc + 1) // 2
        if dr == 0:
            return side_out.at[left_right]
        return vert_out.at[up_down] if dc == 0 else side_out.at[left_right, up_down]

    def copies(k, dr, dc):
        first = pltpu.make_async_remote_copy(
            src_ref=cells.at[4],
            dst_ref=cells.at[(1 - dr) * 3 + 1 - dc],
            send_sem=send1,
            recv_sem=recv1,
            device_id=device(dr, dc),
            device_id_type=MESH,
        )
        second = pltpu.make_async_remote_copy(
            src_ref=packed(dr, dc),
            dst_ref=slot_of(-dr, -dc),
            send_sem=send2,
            recv_sem=recv2,
            device_id=device(dr, dc),
            device_id_type=MESH,
        )
        return first, second

    above_below = (row > 0).astype(jnp.int32) + (row < nr - 1).astype(jnp.int32)
    beside = (col > 0).astype(jnp.int32) + (col < nc - 1).astype(jnp.int32)

    def for_all(wait):
        for v in range(min(nr, 2) - 1, min(nr, 3)):
            for h in range(min(nc, 2) - 1, min(nc, 3)):
                if v + h == 0:
                    continue

                @pl.when(jnp.logical_and(above_below == v, beside == h))
                def _():
                    wait(v + h + v * h, 2 * (v + h) + v * h)

    def batch(ref, n, send, recv):
        part = ref.at[pl.ds(0, n)]
        return pltpu.make_async_remote_copy(
            src_ref=part,
            dst_ref=part,
            send_sem=send,
            recv_sem=recv,
            device_id=device(0, 0),
            device_id_type=MESH,
        )

    for k, (dr, dc) in enumerate(AROUND):

        @pl.when(jnp.logical_not(exists(dr, dc)))
        def _():
            slot = cells.at[(1 + dr) * 3 + 1 + dc]
            slot[...] = jnp.zeros(slot.shape, BF16)
            pixels = slot_of(dr, dc)
            pixels[...] = jnp.zeros(pixels.shape, F32)

    earlier = (col > 0).astype(jnp.int32) + (row > 0).astype(jnp.int32) * (
        1 + (col > 0).astype(jnp.int32) + (col < nc - 1).astype(jnp.int32)
    )

    @pl.when(row + col > 0)
    def _():
        pl.semaphore_wait(barrier, earlier)

    for k, dr, dc in EARLIER:

        @pl.when(exists(dr, dc))
        def _():
            pl.semaphore_signal(
                ready.at[3 - k], inc=1, device_id=device(dr, dc), device_id_type=MESH
            )

    loads[0].wait()
    for k, dr, dc in EARLIER:

        @pl.when(exists(dr, dc))
        def _():
            copies(k, dr, dc)[0].start()

    def send_later(entries):
        for k, dr, dc in entries:

            @pl.when(exists(dr, dc))
            def _():
                pl.semaphore_wait(ready.at[k - 4], 1)
                copies(k, dr, dc)[0].start()

    send_later(LATER)
    loads[1].wait()
    wi32[...] = jnp.zeros(wi32.shape, F32)
    wi32[:, 0 : wi.shape[1], :] = wi[...].astype(F32)
    loads[6].wait()
    wo32[...] = jnp.zeros(wo32.shape, F32)
    wo32[:, 0 : wo.shape[1], :] = wo[...].astype(F32)
    for k in (2, 3, 4, 5):
        loads[k].wait()

    tile = lat.shape[1]
    side_cells = tile + 2 * HALO
    margin, inner = 4 * HALO, 4 * tile
    size = inner + 2 * margin
    chans = lat.shape[0]

    span = size * side_cells
    spread_r = (iota((size, span), 1) // side_cells == iota((size, span), 0)).astype(F32)
    spread_c = [
        (4 * (iota((size, span), 1) % side_cells) + q == iota((size, span), 0)).astype(F32)
        for q in range(4)
    ]
    spread_c = jnp.concatenate(spread_c, axis=1)
    row_w = dot(table_rows(tr[...].astype(F32), lr, row, nr, margin, inner), spread_r.astype(BF16))
    col_w = dot(table_rows(tc[...].astype(F32), lc, col, nc, margin, inner), spread_c.astype(BF16))
    lane = iota((1, span), 1)
    r_of, b_of = lane // side_cells, lane % side_cells
    inside = (
        (r_of >= margin) & (r_of < margin + inner) & (b_of >= HALO) & (b_of < HALO + tile)
    )
    blend, inverse = [], []
    for q in range(4):
        cw = col_w[:, q * span : (q + 1) * span]
        blend.append(row_w[0:1] * cw[0:1])
        inverse.append(1.0 / jnp.where(inside, row_w[1:2] * cw[1:2], 1.0))

    wide = chans * side_cells
    src, dst = iota((3 * wide, 72), 0), iota((3 * wide, 72), 1)
    pick = [
        (
            (dst // 8 == 3 * (src // wide) + dx)
            & (dst % 8 == (src // side_cells) % chans)
        ).astype(F32).astype(BF16)
        for dx in range(3)
    ]
    wi72 = wi32[...].reshape(72, wi32.shape[2]).astype(BF16)

    for_all(lambda n, m: batch(cells, n, send1, recv1).wait_recv())

    cell = [[cells[3 * i + j].astype(F32) for j in range(3)] for i in range(3)]
    bands = [
        jnp.concatenate([cell[0][j][:, tile - HALO :], cell[1][j], cell[2][j][:, :HALO]], axis=1)
        for j in range(3)
    ]
    grid = jnp.concatenate([bands[0][:, :, tile - HALO :], bands[1], bands[2][:, :, :HALO]], axis=2)
    flat = jnp.concatenate([grid[c] for c in range(chans)], axis=1)
    zero = jnp.zeros((1, wide), F32)
    tall = jnp.concatenate(
        [
            jnp.concatenate([zero, flat[:-1]], axis=0),
            flat,
            jnp.concatenate([flat[1:], zero], axis=0),
        ],
        axis=1,
    )
    shape = (side_cells, side_cells, 3 * wide)
    spreaded = jnp.broadcast_to(tall[:, None, :], shape)
    gap = iota(shape, 2) % side_cells - iota(shape, 1)
    patches = 0.0
    for dx in range(3):
        chosen = jnp.where(gap == dx - 1, spreaded, 0.0)
        patches = patches + dot(chosen.reshape(-1, 3 * wide).astype(BF16), pick[dx])
    first = dot(patches.astype(BF16), wi72).reshape(side_cells, side_cells, -1)
    (first,) = group_silu([first])
    first = first.reshape(side_cells * side_cells, -1).astype(BF16)

    loads[7].wait()
    taps = [nt_dot(first, wm[t]).reshape(side_cells, side_cells, -1) for t in range(9)]
    second = conv_up([[taps]], 1)
    second = group_silu([second[py][px] for py in range(2) for px in range(2)])
    second = jnp.concatenate(second, axis=0)
    second = second.reshape(-1, second.shape[2]).astype(BF16)

    loads[8].wait()
    n = side_cells * side_cells
    products = nt_dot(second, wl[...].reshape(-1, wl.shape[2]))
    products = [products[:, wl.shape[1] * t : wl.shape[1] * (t + 1)] for t in range(9)]
    taps = [
        [
            [
                p[(2 * py + px) * n : (2 * py + px + 1) * n].reshape(side_cells, side_cells, -1)
                for p in products
            ]
            for px in range(2)
        ]
        for py in range(2)
    ]
    third = conv_up(taps, 2)
    third = group_silu([third[qy][qx] for qy in range(4) for qx in range(4)])

    wo72 = wo32[...].reshape(72, wo32.shape[2]).astype(BF16)
    colour = []
    for qx in range(4):
        rows = jnp.stack([third[4 * qy + qx] for qy in range(4)], axis=1)
        colour.append(nt_dot(wo72, rows.reshape(span, rows.shape[-1]).astype(BF16)))

    def tap(q, t):
        return colour[q][8 * t : 8 * t + 8]

    half = span // 2
    where_b = iota((4, half), 1) % side_cells
    lower_half = iota((4, half), 1) < half // 2
    sub_b = iota((8, span), 1) % side_cells
    sub_r = iota((8, span), 1) // side_cells
    for q in range(4):
        by_row = []
        for dy in range(3):
            if q > 0:
                before = tap(q - 1, 3 * dy)
            else:
                before = jnp.where(sub_b == 0, 0.0, pltpu.roll(tap(3, 3 * dy), 1, 1))
            if q < 3:
                after = tap(q + 1, 3 * dy + 2)
            else:
                after = jnp.where(
                    sub_b == side_cells - 1, 0.0, pltpu.roll(tap(0, 3 * dy + 2), span - 1, 1)
                )
            by_row.append(before + tap(q, 3 * dy + 1) + after)
        value = (
            jnp.where(sub_r == 0, 0.0, pltpu.roll(by_row[0], side_cells, 1))
            + by_row[1]
            + jnp.where(sub_r == size - 1, 0.0, pltpu.roll(by_row[2], span - side_cells, 1))
        ) * blend[q]
        for h in range(2):
            own[h, q] = value[0:4, h * half : (h + 1) * half]

    for h in range(2):
        for k, rim in ((0, 0), (1, side_cells - HALO)):
            dense = pltpu.roll(own[h, 0], (half - rim) % half, 1)
            for q in range(1, 4):
                moved = pltpu.roll(own[h, q], (HALO * q - rim) % half, 1)
                dense = jnp.where(where_b // HALO == q, moved, dense)
            side_out[k, h] = dense
        for pair in range(2):
            even, odd = own[h, 2 * pair], own[h, 2 * pair + 1]
            if h == 0:
                odd = pltpu.roll(odd, half // 2, 1)
            else:
                even = pltpu.roll(even, half // 2, 1)
            vert_out[h, pair] = jnp.where(lower_half, even, odd)

    for k, (dr, dc) in FAR_FIRST:

        @pl.when(exists(dr, dc))
        def _():
            copies(k, dr, dc)[1].start()

    place_src, place_dst = iota((4 * half, inner), 0), iota((4 * half, inner), 1)
    place = (place_dst == 4 * (place_src % side_cells - HALO) + place_src // half)
    place = place.astype(F32).astype(BF16)
    lane_row = iota((8, half), 1) // side_cells
    sublane = iota((8, half), 0)
    keep = [lane_row == sublane + 8, lane_row == sublane]

    for_all(lambda n, m: batch(rims, m, send2, recv2).wait_recv())

    blocks = [[], [], []]
    for h in range(2):
        pieces = []
        lft = rims[h] + rims[4 + h]
        rgt = rims[2 + h] + rims[6 + h]
        for q in range(4):
            beyond = rims[8 + 2 * h + q // 2]
            if (q + h) % 2 == 0:
                beyond = pltpu.roll(beyond, half // 2, 1)
            lft_q = pltpu.roll(lft, (HALO - HALO * q) % half, 1)
            rgt_q = pltpu.roll(rgt, (tile - HALO * q) % half, 1)
            mid = own[h, q] + beyond + jnp.where(where_b < side_cells // 2, lft_q, rgt_q)
            pieces.append(mid * inverse[q][:, h * half : (h + 1) * half])
        for c in range(3):
            spread_rows = [
                jnp.where(keep[h], jnp.broadcast_to(p[c : c + 1], (8, half)), 0.0) for p in pieces
            ]
            blocks[c].append(jnp.concatenate(spread_rows, axis=1))
    tall = jnp.concatenate([b for c in range(3) for b in blocks[c]], axis=0)
    top = tall.astype(BF16)
    low = (tall - top.astype(F32)).astype(BF16)
    image = dot(top, place) + dot(low, place)
    out[...] = image.reshape(3, inner, inner)

    for_all(lambda n, m: batch(cells, n, send1, recv1).wait_send())
    for_all(lambda n, m: batch(rims, m, send2, recv2).wait_send())


def solution(mesh):
    nr, nc = mesh.shape["rows"], mesh.shape["cols"]

    def per_device(lat, w_in, w_mid, w_low, w_out, ramp_r, ramp_c, lim_r, lim_c):
        tile = lat.shape[1]
        inner = 4 * tile
        size = inner + 8 * HALO
        half = size * (tile + 2 * HALO) // 2
        anywhere = pl.BlockSpec(memory_space=pltpu.HBM)
        dma = pltpu.SemaphoreType.DMA
        return pl.pallas_call(
            functools.partial(kernel, nr, nc),
            out_shape=pltpu.VMEM((w_out.shape[1], inner, inner), F32),
            in_specs=[anywhere] * 9,
            out_specs=pl.BlockSpec(memory_space=pltpu.VMEM),
            scratch_shapes=[
                pltpu.VMEM((9,) + lat.shape, BF16),
                pltpu.VMEM(w_in.shape, BF16),
                pltpu.VMEM(w_mid.shape, BF16),
                pltpu.VMEM(w_low.shape, BF16),
                pltpu.VMEM(w_out.shape, BF16),
                pltpu.VMEM(ramp_r.shape, jnp.int32),
                pltpu.VMEM(ramp_c.shape, jnp.int32),
                pltpu.SMEM(lim_r.shape, jnp.int32),
                pltpu.SMEM(lim_c.shape, jnp.int32),
                pltpu.VMEM((9, 8, w_in.shape[2]), F32),
                pltpu.VMEM((9, 8, w_out.shape[2]), F32),
                pltpu.VMEM((2, 4, 4, half), F32),
                pltpu.VMEM((2, 2, 4, half), F32),
                pltpu.VMEM((2, 2, 4, half), F32),
                pltpu.VMEM((12, 4, half), F32),
                dma((9,)),
                pltpu.SemaphoreType.REGULAR((4,)),
                dma,
                dma,
                dma,
                dma,
            ],
            compiler_params=pltpu.CompilerParams(
                collective_id=0, has_side_effects=True
            ),
            name="decode",
        )(lat, w_in, w_mid, w_low, w_out, ramp_r, ramp_c, lim_r, lim_c)

    return jax.shard_map(
        per_device,
        mesh=mesh,
        in_specs=(P(None, ("groups", "rows"), "cols"), P(), P(), P(), P(), P(), P(), P(), P()),
        out_specs=P(None, ("groups", "rows"), "cols"),
        check_vma=False,
    )
```

```python
import functools

import jax
import jax.numpy as jnp
from jax import lax
from jax.experimental import pallas as pl
from jax.experimental.pallas import tpu as pltpu
from jax.sharding import PartitionSpec as P

MESH = pl.DeviceIdType.MESH
NGROUPS = 32
HALO = 2
F32 = jnp.float32
BF16 = jnp.bfloat16
AROUND = [(dr, dc) for dr in (-1, 0, 1) for dc in (-1, 0, 1) if (dr, dc) != (0, 0)]
FAR_FIRST = sorted(enumerate(AROUND), key=lambda e: -abs(e[1][0]) - abs(e[1][1]))
EARLIER = [(k, *to) for k, to in FAR_FIRST if k < 4]
LATER = [(k, *AROUND[k]) for k in range(4, 8)]


def iota(shape, dim):
    return lax.broadcasted_iota(jnp.int32, shape, dim)


def nt_dot(a, b):
    return lax.dot_general(a, b, (((1,), (1,)), ((), ())), preferred_element_type=F32)


def dot(a, b):
    return jnp.dot(a, b, preferred_element_type=F32)


def down(x):
    return jnp.concatenate([jnp.zeros_like(x[:1]), x[:-1]], axis=0)


def up(x):
    return jnp.concatenate([x[1:], jnp.zeros_like(x[:1])], axis=0)


def right(x):
    rolled = pltpu.roll(x, 1, 1)
    return jnp.where(iota(x.shape, 1) == 0, 0.0, rolled)


def left(x):
    n = x.shape[1]
    rolled = pltpu.roll(x, n - 1, 1)
    return jnp.where(iota(x.shape, 1) == n - 1, 0.0, rolled)


def expand(products, fine, before, after):
    out = []
    for q in range(fine):
        t0, t1, t2 = products[q]
        prev = products[q - 1][0] if q > 0 else before(products[fine - 1][0])
        nxt = products[q + 1][2] if q < fine - 1 else after(products[0][2])
        out.append(prev + (t1 + t2))
        out.append((t0 + t1) + nxt)
    return out


def conv_up(taps, fine):
    by_col = [
        [
            expand(
                [[taps[py][px][3 * dy + dx] for dy in range(3)] for py in range(fine)],
                fine,
                down,
                up,
            )
            for dx in range(3)
        ]
        for px in range(fine)
    ]
    return [
        expand(
            [[by_col[px][dx][qy] for dx in range(3)] for px in range(fine)],
            fine,
            right,
            left,
        )
        for qy in range(2 * fine)
    ]


def group_silu(phases):
    channels = phases[0].shape[-1]
    width = channels // NGROUPS
    count = channels // 128
    positions = len(phases) * phases[0].shape[0] * phases[0].shape[1]
    scale = 1.0 / (positions * width)
    block = (iota((384, 128), 0) % 128 // width == iota((384, 128), 1) // width).astype(F32)
    block = block.astype(BF16)
    total = jnp.sum(functools.reduce(jnp.add, phases), axis=(0, 1)).reshape(1, channels)
    squares = functools.reduce(jnp.add, [p * p for p in phases])
    squares = jnp.sum(squares, axis=(0, 1)).reshape(1, channels)
    rows = [x[:, k * 128 : (k + 1) * 128] for x in (total, squares) for k in range(count)]
    rows = jnp.concatenate(rows + [jnp.zeros((1, 128), F32)] * (8 - len(rows)), axis=0)
    top = rows.astype(BF16)
    rest = rows - top.astype(F32)
    mid = rest.astype(BF16)
    low = (rest - mid.astype(F32)).astype(BF16)
    got = dot(jnp.concatenate([top, mid, low], axis=1), block) * scale
    center = got[:count]
    spread = jnp.maximum(got[count : 2 * count] - center * center, 0.0)
    factor = 0.5 * lax.rsqrt(spread + 1e-06)
    offset = center * factor
    factor = jnp.concatenate([factor[k : k + 1] for k in range(count)], axis=1)[None]
    offset = jnp.concatenate([offset[k : k + 1] for k in range(count)], axis=1)[None]
    result = []
    for p in phases:
        half = p * factor - offset
        result.append(half + half * jnp.tanh(half))
    return result


def table_rows(table, limits, index, count, margin, inner):
    size = table.shape[1]
    pos = iota((1, size), 1)
    far = jnp.maximum(jnp.maximum(margin - pos, pos - (margin + inner) + 1), 0)
    rows = []
    for d in (-1, 0, 1):
        here = index + d
        limit = limits[jnp.clip(here, 0, count - 1)]
        picked = jnp.where(iota(table.shape, 0) == here, table, 0.0)
        row = jnp.sum(picked, axis=0, keepdims=True)
        rows.append(jnp.where(far <= limit, row, 0.0))
    above, own, below = rows
    other = jnp.where(pos < inner, jnp.roll(above, inner, 1), jnp.roll(below, inner, 1))
    pair = jnp.concatenate([own, own + other, jnp.zeros((6, size), F32)], axis=0)
    return pair.astype(BF16)


def kernel(
    nr, nc, lat, w_in, w_mid, w_low, w_out, ramp_r, ramp_c, lim_r, lim_c, out,
    cells, wi, wm, wl, wo, tr, tc, lr, lc, wi32, wo32, wc, wmt, wlt,
    blend, inverse, own, side_out, vert_out, rims,
    local_sem, ready, send1, recv1, send2, recv2,
):
    row, col = lax.axis_index("rows"), lax.axis_index("cols")

    def exists(dr, dc):
        ok = None
        for d, here, n in ((dr, row, nr), (dc, col, nc)):
            test = None if d == 0 else (here > 0 if d < 0 else here < n - 1)
            if test is not None:
                ok = test if ok is None else jnp.logical_and(ok, test)
        return ok

    def device(dr, dc):
        return {"rows": row + dr, "cols": col + dc}

    loads = [
        pltpu.make_async_copy(src, dst, local_sem.at[k])
        for k, (src, dst) in enumerate(
            [
                (lat, cells.at[4]),
                (w_in, wi),
                (ramp_r, tr),
                (ramp_c, tc),
                (lim_r, lr),
                (lim_c, lc),
                (w_out, wo),
                (w_mid, wm),
                (w_low, wl),
            ]
        )
    ]
    for load in loads:
        load.start()

    barrier = pltpu.get_barrier_semaphore()
    for k, dr, dc in LATER:

        @pl.when(exists(dr, dc))
        def _():
            pl.semaphore_signal(barrier, inc=1, device_id=device(dr, dc), device_id_type=MESH)

    def slot_of(dr, dc):
        up_down, left_right = (dr + 1) // 2, (dc + 1) // 2
        if dr == 0:
            return rims.at[pl.ds(2 * left_right, 2)]
        if dc == 0:
            return rims.at[pl.ds(8 + 2 * up_down, 2)]
        return rims.at[4 + 2 * left_right + up_down]

    def packed(dr, dc):
        up_down, left_right = (dr + 1) // 2, (dc + 1) // 2
        if dr == 0:
            return side_out.at[left_right]
        return vert_out.at[up_down] if dc == 0 else side_out.at[left_right, up_down]

    def copies(k, dr, dc):
        first = pltpu.make_async_remote_copy(
            src_ref=cells.at[4],
            dst_ref=cells.at[(1 - dr) * 3 + 1 - dc],
            send_sem=send1,
            recv_sem=recv1,
            device_id=device(dr, dc),
            device_id_type=MESH,
        )
        second = pltpu.make_async_remote_copy(
            src_ref=packed(dr, dc),
            dst_ref=slot_of(-dr, -dc),
            send_sem=send2,
            recv_sem=recv2,
            device_id=device(dr, dc),
            device_id_type=MESH,
        )
        return first, second

    above_below = (row > 0).astype(jnp.int32) + (row < nr - 1).astype(jnp.int32)
    beside = (col > 0).astype(jnp.int32) + (col < nc - 1).astype(jnp.int32)

    def for_all(wait):
        for v in range(min(nr, 2) - 1, min(nr, 3)):
            for h in range(min(nc, 2) - 1, min(nc, 3)):
                if v + h == 0:
                    continue

                @pl.when(jnp.logical_and(above_below == v, beside == h))
                def _():
                    wait(v + h + v * h, 2 * (v + h) + v * h)

    def batch(ref, n, send, recv):
        part = ref.at[pl.ds(0, n)]
        return pltpu.make_async_remote_copy(
            src_ref=part,
            dst_ref=part,
            send_sem=send,
            recv_sem=recv,
            device_id=device(0, 0),
            device_id_type=MESH,
        )

    for k, (dr, dc) in enumerate(AROUND):

        @pl.when(jnp.logical_not(exists(dr, dc)))
        def _():
            slot = cells.at[(1 + dr) * 3 + 1 + dc]
            slot[...] = jnp.zeros(slot.shape, BF16)
            pixels = slot_of(dr, dc)
            pixels[...] = jnp.zeros(pixels.shape, F32)

    earlier = (col > 0).astype(jnp.int32) + (row > 0).astype(jnp.int32) * (
        1 + (col > 0).astype(jnp.int32) + (col < nc - 1).astype(jnp.int32)
    )

    @pl.when(row + col > 0)
    def _():
        pl.semaphore_wait(barrier, earlier)

    for k, dr, dc in EARLIER:

        @pl.when(exists(dr, dc))
        def _():
            pl.semaphore_signal(
                ready.at[3 - k], inc=1, device_id=device(dr, dc), device_id_type=MESH
            )

    loads[0].wait()
    for k, dr, dc in EARLIER:

        @pl.when(exists(dr, dc))
        def _():
            copies(k, dr, dc)[0].start()

    def send_later(entries):
        for k, dr, dc in entries:

            @pl.when(exists(dr, dc))
            def _():
                pl.semaphore_wait(ready.at[k - 4], 1)
                copies(k, dr, dc)[0].start()

    send_later([e for e in LATER if e[1] == 0])

    tile = lat.shape[1]
    side_cells = tile + 2 * HALO
    margin, inner = 4 * HALO, 4 * tile
    size = inner + 2 * margin
    chans = lat.shape[0]
    span = size * side_cells
    half = span // 2
    wide = chans * side_cells

    loads[1].wait()
    wi32[...] = jnp.zeros(wi32.shape, F32)
    wi32[:, 0 : wi.shape[1], :] = wi[...].astype(F32)
    wi72 = wi32[...].reshape(72, wi32.shape[2]).astype(BF16)
    src, dst = iota((384, 72), 0), iota((384, 72), 1)
    pick = (
        (dst // 8 == 3 * (src % 128 // wide) + src // 128)
        & (dst % 8 == (src // side_cells) % chans)
        & (src % 128 < 3 * wide)
    )
    wc[...] = dot(pick.astype(F32).astype(BF16), wi72).astype(BF16)
    for k in (2, 3, 4, 5):
        loads[k].wait()

    spread_r = (iota((size, span), 1) // side_cells == iota((size, span), 0)).astype(F32)
    spread_c = [
        (4 * (iota((size, span), 1) % side_cells) + q == iota((size, span), 0)).astype(F32)
        for q in range(4)
    ]
    spread_c = jnp.concatenate(spread_c, axis=1)
    row_w = dot(table_rows(tr[...].astype(F32), lr, row, nr, margin, inner), spread_r.astype(BF16))
    col_w = dot(table_rows(tc[...].astype(F32), lc, col, nc, margin, inner), spread_c.astype(BF16))
    lane = iota((1, span), 1)
    r_of, b_of = lane // side_cells, lane % side_cells
    inside = (
        (r_of >= margin) & (r_of < margin + inner) & (b_of >= HALO) & (b_of < HALO + tile)
    )
    for q in range(4):
        cw = col_w[:, q * span : (q + 1) * span]
        blend[q] = jnp.broadcast_to(row_w[0:1] * cw[0:1], (8, span))
        inverse[q] = jnp.broadcast_to(
            1.0 / jnp.where(inside, row_w[1:2] * cw[1:2], 1.0), (8, span)
        )

    send_later([e for e in LATER if e[1] != 0])

    loads[6].wait()
    wo32[...] = jnp.zeros(wo32.shape, F32)
    wo32[:, 0 : wo.shape[1], :] = wo[...].astype(F32)
    loads[7].wait()
    out_mid = wm.shape[1]
    for t in range(9):
        wmt[:, out_mid * t : out_mid * (t + 1)] = wm[t].T
    loads[8].wait()
    out_low = wl.shape[1]
    for t in range(9):
        wlt[:, out_low * t : out_low * (t + 1)] = wl[t].T

    for_all(lambda n, m: batch(cells, n, send1, recv1).wait_recv())

    cell = [cells[k].astype(F32) for k in range(9)]
    pieces = [[], [], []]
    for c in range(chans):
        for j, cut in enumerate((slice(tile - HALO, tile), slice(0, tile), slice(0, HALO))):
            upper, middle, lower = (cell[3 * i + j][c][:, cut] for i in range(3))
            zero = jnp.zeros((1, middle.shape[1]), F32)
            upper, lower = upper[tile - HALO :], lower[:HALO]
            pieces[0].append(jnp.concatenate([zero, upper, middle, lower[:-1]], axis=0))
            pieces[1].append(jnp.concatenate([upper, middle, lower], axis=0))
            pieces[2].append(jnp.concatenate([upper[1:], middle, lower, zero], axis=0))
    pieces = pieces[0] + pieces[1] + pieces[2]
    tall = jnp.concatenate(pieces + [jnp.zeros((side_cells, 128 - 3 * wide), F32)], axis=1)
    shape = (side_cells, side_cells, 128)
    spreaded = jnp.broadcast_to(tall[:, None, :], shape)
    gap = iota(shape, 2) % side_cells - iota(shape, 1)
    patches = [jnp.where(gap == dx - 1, spreaded, 0.0) for dx in range(3)]
    patches = jnp.concatenate(patches, axis=2).reshape(-1, 384).astype(BF16)
    first = dot(patches, wc[...]).reshape(side_cells, side_cells, -1)
    (first,) = group_silu([first])
    first = first.reshape(side_cells * side_cells, -1).astype(BF16)

    taps = dot(first, wmt[...])
    taps = [
        taps[:, out_mid * t : out_mid * (t + 1)].reshape(side_cells, side_cells, -1)
        for t in range(9)
    ]
    second = conv_up([[taps]], 1)
    second = group_silu([second[py][px] for py in range(2) for px in range(2)])
    second = jnp.concatenate(second, axis=0)
    second = second.reshape(-1, second.shape[2]).astype(BF16)

    n = side_cells * side_cells
    products = dot(second, wlt[...])
    products = [products[:, out_low * t : out_low * (t + 1)] for t in range(9)]
    taps = [
        [
            [
                p[(2 * py + px) * n : (2 * py + px + 1) * n].reshape(side_cells, side_cells, -1)
                for p in products
            ]
            for px in range(2)
        ]
        for py in range(2)
    ]
    third = conv_up(taps, 2)
    third = group_silu([third[qy][qx] for qy in range(4) for qx in range(4)])

    wo72 = wo32[...].reshape(72, wo32.shape[2]).astype(BF16)
    colour = []
    for qx in range(4):
        rows = jnp.stack([third[4 * qy + qx] for qy in range(4)], axis=1)
        colour.append(nt_dot(wo72, rows.reshape(span, rows.shape[-1]).astype(BF16)))

    def tap(q, t):
        return colour[q][8 * t : 8 * t + 8]

    where_b = iota((4, half), 1) % side_cells
    lower_half = iota((4, half), 1) < half // 2
    sub_b = iota((8, span), 1) % side_cells
    sub_r = iota((8, span), 1) // side_cells
    row_ok = [sub_r > 0, None, sub_r < size - 1]
    col_ok = [sub_b > 0, None, sub_b < side_cells - 1]

    def moved(x, dy, dx):
        shift = (side_cells * (1 - dy) + 1 - dx) % span
        x = pltpu.roll(x, shift, 1) if shift else x
        ok = [m for m in (row_ok[dy], col_ok[dx]) if m is not None]
        return jnp.where(functools.reduce(jnp.logical_and, ok), x, 0.0) if ok else x

    for q in range(4):
        value = None
        for dy in range(3):
            near = tap(q, 3 * dy + 1)
            if q > 0:
                near = near + tap(q - 1, 3 * dy)
            if q < 3:
                near = near + tap(q + 1, 3 * dy + 2)
            term = moved(near, dy, 1)
            if q == 0:
                term = term + moved(tap(3, 3 * dy), dy, 0)
            if q == 3:
                term = term + moved(tap(0, 3 * dy + 2), dy, 2)
            value = term if value is None else value + term
        value = value * blend[q]
        for h in range(2):
            own[h, q] = value[0:4, h * half : (h + 1) * half]

    for h in range(2):
        for k, rim in ((0, 0), (1, side_cells - HALO)):
            dense = pltpu.roll(own[h, 0], (half - rim) % half, 1)
            for q in range(1, 4):
                turned = pltpu.roll(own[h, q], (HALO * q - rim) % half, 1)
                dense = jnp.where(where_b // HALO == q, turned, dense)
            side_out[k, h] = dense
        for pair in range(2):
            even, odd = own[h, 2 * pair], own[h, 2 * pair + 1]
            if h == 0:
                odd = pltpu.roll(odd, half // 2, 1)
            else:
                even = pltpu.roll(even, half // 2, 1)
            vert_out[h, pair] = jnp.where(lower_half, even, odd)

    for k, (dr, dc) in FAR_FIRST:

        @pl.when(exists(dr, dc))
        def _():
            copies(k, dr, dc)[1].start()

    lane_row = iota((8, half), 1) // side_cells
    sublane = iota((8, half), 0)
    keep = [lane_row == sublane + 8, lane_row == sublane]
    beyond_row = [lane_row % 8 == sublane, lane_row % 8 == sublane]

    def spread_rows(piece, c, mask):
        return jnp.where(mask, jnp.broadcast_to(piece[c : c + 1], (8, half)), 0.0)

    def placed(blocks, place):
        tall = jnp.concatenate(blocks, axis=0)
        top = tall.astype(BF16)
        low = (tall - top.astype(F32)).astype(BF16)
        got = dot(jnp.concatenate([top, low], axis=0), place)
        return got[: tall.shape[0]] + got[tall.shape[0] :]

    place_src, place_dst = iota((4 * half, inner), 0), iota((4 * half, inner), 1)
    place = place_dst == 4 * (place_src % side_cells - HALO) + place_src // half
    place = place.astype(F32).astype(BF16)
    blocks = []
    for c in range(3):
        for h in range(2):
            mine = [own[h, q] * inverse[q, 0:4, h * half : (h + 1) * half] for q in range(4)]
            blocks.append(jnp.concatenate([spread_rows(p, c, keep[h]) for p in mine], axis=1))
    mine = placed(blocks, place)

    slot = place_src % side_cells
    from_left = place_dst == 4 * (slot % HALO) + slot // HALO
    from_right = place_dst == 4 * (tile - HALO + slot % HALO) + slot // HALO
    pair_q = 2 * (place_src // half - 2) + place_src % half // (half // 2)
    from_pair = place_dst == 4 * (slot - HALO) + pair_q
    part = place_src // half
    rim_place = jnp.where(
        part == 0, from_left.astype(F32), jnp.where(part == 1, from_right.astype(F32), from_pair.astype(F32))
    ).astype(BF16)
    scales = []
    for h in range(2):
        here = [inverse[q, 0:4, h * half : (h + 1) * half] for q in range(4)]
        sides = []
        for rim in (HALO, tile):
            dense = pltpu.roll(here[0], (half - rim) % half, 1)
            for q in range(1, 4):
                turned = pltpu.roll(here[q], (HALO * q - rim) % half, 1)
                dense = jnp.where(where_b // HALO == q, turned, dense)
            sides.append(dense)
        for pair in range(2):
            even, odd = here[2 * pair], here[2 * pair + 1]
            if h == 0:
                even = pltpu.roll(even, half // 2, 1)
            else:
                odd = pltpu.roll(odd, half // 2, 1)
            sides.append(jnp.where(lower_half, even, odd))
        scales.append(sides)

    for_all(lambda n, m: batch(rims, m, send2, recv2).wait_recv())

    blocks = []
    for c in range(3):
        for h in range(2):
            got = [
                (rims[h] + rims[4 + h]) * scales[h][0],
                (rims[2 + h] + rims[6 + h]) * scales[h][1],
                rims[8 + 2 * h] * scales[h][2],
                rims[9 + 2 * h] * scales[h][3],
            ]
            masks = [keep[h], keep[h], beyond_row[h], beyond_row[h]]
            blocks.append(
                jnp.concatenate([spread_rows(p, c, m) for p, m in zip(got, masks)], axis=1)
            )
    out[...] = (mine + placed(blocks, rim_place)).reshape(3, inner, inner)

    for_all(lambda n, m: batch(cells, n, send1, recv1).wait_send())
    for_all(lambda n, m: batch(rims, m, send2, recv2).wait_send())


def solution(mesh):
    nr, nc = mesh.shape["rows"], mesh.shape["cols"]

    def per_device(lat, w_in, w_mid, w_low, w_out, ramp_r, ramp_c, lim_r, lim_c):
        tile = lat.shape[1]
        inner = 4 * tile
        size = inner + 8 * HALO
        half = size * (tile + 2 * HALO) // 2
        anywhere = pl.BlockSpec(memory_space=pltpu.HBM)
        dma = pltpu.SemaphoreType.DMA
        return pl.pallas_call(
            functools.partial(kernel, nr, nc),
            out_shape=pltpu.VMEM((w_out.shape[1], inner, inner), F32),
            in_specs=[anywhere] * 9,
            out_specs=pl.BlockSpec(memory_space=pltpu.VMEM),
            scratch_shapes=[
                pltpu.VMEM((9,) + lat.shape, BF16),
                pltpu.VMEM(w_in.shape, BF16),
                pltpu.VMEM(w_mid.shape, BF16),
                pltpu.VMEM(w_low.shape, BF16),
                pltpu.VMEM(w_out.shape, BF16),
                pltpu.VMEM(ramp_r.shape, jnp.int32),
                pltpu.VMEM(ramp_c.shape, jnp.int32),
                pltpu.SMEM(lim_r.shape, jnp.int32),
                pltpu.SMEM(lim_c.shape, jnp.int32),
                pltpu.VMEM((9, 8, w_in.shape[2]), F32),
                pltpu.VMEM((9, 8, w_out.shape[2]), F32),
                pltpu.VMEM((384, w_in.shape[2]), BF16),
                pltpu.VMEM((w_mid.shape[2], 9 * w_mid.shape[1]), BF16),
                pltpu.VMEM((w_low.shape[2], 9 * w_low.shape[1]), BF16),
                pltpu.VMEM((4, 8, 2 * half), F32),
                pltpu.VMEM((4, 8, 2 * half), F32),
                pltpu.VMEM((2, 4, 4, half), F32),
                pltpu.VMEM((2, 2, 4, half), F32),
                pltpu.VMEM((2, 2, 4, half), F32),
                pltpu.VMEM((12, 4, half), F32),
                dma((9,)),
                pltpu.SemaphoreType.REGULAR((4,)),
                dma,
                dma,
                dma,
                dma,
            ],
            compiler_params=pltpu.CompilerParams(
                collective_id=0, has_side_effects=True
            ),
            name="decode",
        )(lat, w_in, w_mid, w_low, w_out, ramp_r, ramp_c, lim_r, lim_c)

    return jax.shard_map(
        per_device,
        mesh=mesh,
        in_specs=(P(None, ("groups", "rows"), "cols"), P(), P(), P(), P(), P(), P(), P(), P()),
        out_specs=P(None, ("groups", "rows"), "cols"),
        check_vma=False,
    )
```

```python
import functools

import jax
import jax.numpy as jnp
from jax import lax
from jax.experimental import pallas as pl
from jax.experimental.pallas import tpu as pltpu
from jax.sharding import PartitionSpec as P

MESH = pl.DeviceIdType.MESH
NGROUPS = 32
HALO = 2
F32 = jnp.float32
BF16 = jnp.bfloat16
AROUND = [(dr, dc) for dr in (-1, 0, 1) for dc in (-1, 0, 1) if (dr, dc) != (0, 0)]
FAR_FIRST = sorted(enumerate(AROUND), key=lambda e: -abs(e[1][0]) - abs(e[1][1]))
EARLIER = [(k, *to) for k, to in FAR_FIRST if k < 4]
LATER = [(k, *AROUND[k]) for k in range(4, 8)]


def iota(shape, dim):
    return lax.broadcasted_iota(jnp.int32, shape, dim)


def nt_dot(a, b):
    return lax.dot_general(a, b, (((1,), (1,)), ((), ())), preferred_element_type=F32)


def dot(a, b):
    return jnp.dot(a, b, preferred_element_type=F32)


def down(x):
    return jnp.concatenate([jnp.zeros_like(x[:1]), x[:-1]], axis=0)


def up(x):
    return jnp.concatenate([x[1:], jnp.zeros_like(x[:1])], axis=0)


def right(x):
    rolled = pltpu.roll(x, 1, 1)
    return jnp.where(iota(x.shape, 1) == 0, 0.0, rolled)


def left(x):
    n = x.shape[1]
    rolled = pltpu.roll(x, n - 1, 1)
    return jnp.where(iota(x.shape, 1) == n - 1, 0.0, rolled)


def expand(products, fine, before, after):
    out = []
    for q in range(fine):
        t0, t1, t2 = products[q]
        prev = products[q - 1][0] if q > 0 else before(products[fine - 1][0])
        nxt = products[q + 1][2] if q < fine - 1 else after(products[0][2])
        out.append(prev + (t1 + t2))
        out.append((t0 + t1) + nxt)
    return out


def conv_up(taps, fine):
    by_col = [
        [
            expand(
                [[taps[py][px][3 * dy + dx] for dy in range(3)] for py in range(fine)],
                fine,
                down,
                up,
            )
            for dx in range(3)
        ]
        for px in range(fine)
    ]
    return [
        expand(
            [[by_col[px][dx][qy] for dx in range(3)] for px in range(fine)],
            fine,
            right,
            left,
        )
        for qy in range(2 * fine)
    ]


def group_silu(phases):
    channels = phases[0].shape[-1]
    width = channels // NGROUPS
    count = channels // 128
    positions = len(phases) * phases[0].shape[0] * phases[0].shape[1]
    scale = 1.0 / (positions * width)
    block = (iota((384, 128), 0) % 128 // width == iota((384, 128), 1) // width).astype(F32)
    block = block.astype(BF16)
    total = jnp.sum(functools.reduce(jnp.add, phases), axis=(0, 1)).reshape(1, channels)
    squares = functools.reduce(jnp.add, [p * p for p in phases])
    squares = jnp.sum(squares, axis=(0, 1)).reshape(1, channels)
    rows = [x[:, k * 128 : (k + 1) * 128] for x in (total, squares) for k in range(count)]
    rows = jnp.concatenate(rows + [jnp.zeros((1, 128), F32)] * (8 - len(rows)), axis=0)
    top = rows.astype(BF16)
    rest = rows - top.astype(F32)
    mid = rest.astype(BF16)
    low = (rest - mid.astype(F32)).astype(BF16)
    got = dot(jnp.concatenate([top, mid, low], axis=1), block) * scale
    center = got[:count]
    spread = jnp.maximum(got[count : 2 * count] - center * center, 0.0)
    factor = 0.5 * lax.rsqrt(spread + 1e-06)
    offset = center * factor
    factor = jnp.concatenate([factor[k : k + 1] for k in range(count)], axis=1)[None]
    offset = jnp.concatenate([offset[k : k + 1] for k in range(count)], axis=1)[None]
    result = []
    for p in phases:
        half = p * factor - offset
        result.append(half + half * jnp.tanh(half))
    return result


def table_rows(table, limits, index, count, margin, inner):
    size = table.shape[1]
    pos = iota((1, size), 1)
    far = jnp.maximum(jnp.maximum(margin - pos, pos - (margin + inner) + 1), 0)
    rows = []
    for d in (-1, 0, 1):
        here = index + d
        limit = limits[jnp.clip(here, 0, count - 1)]
        picked = jnp.where(iota(table.shape, 0) == here, table, 0.0)
        row = jnp.sum(picked, axis=0, keepdims=True)
        rows.append(jnp.where(far <= limit, row, 0.0))
    above, own, below = rows
    other = jnp.where(pos < inner, jnp.roll(above, inner, 1), jnp.roll(below, inner, 1))
    pair = jnp.concatenate([own, own + other, jnp.zeros((6, size), F32)], axis=0)
    return pair.astype(BF16)


def kernel(
    nr, nc, lat, w_in, w_mid, w_low, w_out, ramp_r, ramp_c, lim_r, lim_c, out,
    cells, wi, wm, wl, wo, tables, limits, wi32, wo32, wc, wmt, wlt,
    blend, inverse, own, side_out, vert_out, rims,
    local_sem, ready, recv1, recv2,
):
    row, col = lax.axis_index("rows"), lax.axis_index("cols")

    def exists(dr, dc):
        ok = None
        for d, here, n in ((dr, row, nr), (dc, col, nc)):
            test = None if d == 0 else (here > 0 if d < 0 else here < n - 1)
            if test is not None:
                ok = test if ok is None else jnp.logical_and(ok, test)
        return ok

    def device(dr, dc):
        return {"rows": row + dr, "cols": col + dc}

    loads = [
        pltpu.make_async_copy(src, dst, local_sem.at[k])
        for k, src, dst in [
            (0, lat, cells.at[4]),
            (1, w_in, wi),
            (2, ramp_r, tables.at[0]),
            (2, ramp_c, tables.at[1]),
            (3, lim_r, limits.at[0]),
            (3, lim_c, limits.at[1]),
            (4, w_mid, wm),
            (5, w_low, wl),
        ]
    ]
    load_out = pltpu.make_async_copy(w_out, wo, local_sem.at[1])
    send1, send2 = local_sem.at[0], local_sem.at[0]
    for load in loads:
        load.start()

    def mutual(dr, dc):
        return jnp.logical_and(row == (0 if dr > 0 else 1), col % 2 == (1 if dc > 0 else 0))

    def one_way(dr, dc):
        there = exists(dr, dc)
        return jnp.logical_and(there, jnp.logical_not(mutual(dr, dc))) if dr * dc else there

    barrier = pltpu.get_barrier_semaphore()
    greeted = [(exists(dr, dc), dr, dc) for _, dr, dc in LATER]
    greeted += [(jnp.logical_and(exists(-1, dc), mutual(-1, dc)), -1, dc) for dc in (-1, 1)]
    for there, dr, dc in greeted:

        @pl.when(there)
        def _():
            pl.semaphore_signal(barrier, inc=1, device_id=device(dr, dc), device_id_type=MESH)

    def slot_of(dr, dc):
        up_down, left_right = (dr + 1) // 2, (dc + 1) // 2
        if dr == 0:
            return rims.at[pl.ds(2 * left_right, 2)]
        if dc == 0:
            return rims.at[pl.ds(8 + 2 * up_down, 2)]
        return rims.at[4 + 2 * left_right + up_down]

    def packed(dr, dc):
        up_down, left_right = (dr + 1) // 2, (dc + 1) // 2
        if dr == 0:
            return side_out.at[left_right]
        return vert_out.at[up_down] if dc == 0 else side_out.at[left_right, up_down]

    def copies(k, dr, dc):
        first = pltpu.make_async_remote_copy(
            src_ref=cells.at[4],
            dst_ref=cells.at[(1 - dr) * 3 + 1 - dc],
            send_sem=send1,
            recv_sem=recv1,
            device_id=device(dr, dc),
            device_id_type=MESH,
        )
        second = pltpu.make_async_remote_copy(
            src_ref=packed(dr, dc),
            dst_ref=slot_of(-dr, -dc),
            send_sem=send2,
            recv_sem=recv2,
            device_id=device(dr, dc),
            device_id_type=MESH,
        )
        return first, second

    above_below = (row > 0).astype(jnp.int32) + (row < nr - 1).astype(jnp.int32)
    beside = (col > 0).astype(jnp.int32) + (col < nc - 1).astype(jnp.int32)

    def for_all(wait):
        for v in range(min(nr, 2) - 1, min(nr, 3)):
            for h in range(min(nc, 2) - 1, min(nc, 3)):
                if v + h == 0:
                    continue

                @pl.when(jnp.logical_and(above_below == v, beside == h))
                def _():
                    wait(v + h + v * h, 2 * (v + h) + v * h)

    def batch(ref, n, send, recv):
        part = ref.at[pl.ds(0, n)]
        return pltpu.make_async_remote_copy(
            src_ref=part,
            dst_ref=part,
            send_sem=send,
            recv_sem=recv,
            device_id=device(0, 0),
            device_id_type=MESH,
        )

    for k, (dr, dc) in enumerate(AROUND):

        @pl.when(jnp.logical_not(exists(dr, dc)))
        def _():
            slot = cells.at[(1 + dr) * 3 + 1 + dc]
            slot[...] = jnp.zeros(slot.shape, BF16)
            pixels = slot_of(dr, dc)
            pixels[...] = jnp.zeros(pixels.shape, F32)

    earlier = (col > 0).astype(jnp.int32) + (row > 0).astype(jnp.int32) * (
        1 + (col > 0).astype(jnp.int32) + (col < nc - 1).astype(jnp.int32)
    )
    if nr > 1:
        for dc in (-1, 1):
            earlier += jnp.logical_and(exists(1, dc), mutual(1, dc)).astype(jnp.int32)

    @pl.when(row + col > 0)
    def _():
        pl.semaphore_wait(barrier, earlier)

    for k, dr, dc in EARLIER:

        @pl.when(one_way(dr, dc))
        def _():
            pl.semaphore_signal(
                ready.at[3 - k], inc=1, device_id=device(dr, dc), device_id_type=MESH
            )

    loads[0].wait()
    for k, dr, dc in EARLIER:

        @pl.when(exists(dr, dc))
        def _():
            copies(k, dr, dc)[0].start()

    for k, dr, dc in LATER:
        if dr * dc:

            @pl.when(jnp.logical_and(exists(dr, dc), mutual(dr, dc)))
            def _():
                copies(k, dr, dc)[0].start()

    def send_later(entries):
        for k, dr, dc in entries:

            @pl.when(one_way(dr, dc))
            def _():
                pl.semaphore_wait(ready.at[k - 4], 1)
                copies(k, dr, dc)[0].start()

    send_later([e for e in LATER if e[1] == 0])

    tile = lat.shape[1]
    side_cells = tile + 2 * HALO
    margin, inner = 4 * HALO, 4 * tile
    size = inner + 2 * margin
    chans = lat.shape[0]
    span = size * side_cells
    half = span // 2
    wide = chans * side_cells

    loads[1].wait()
    load_out.start()
    wi32[...] = jnp.zeros(wi32.shape, F32)
    wi32[:, 0 : wi.shape[1], :] = wi[...].astype(F32)
    wi72 = wi32[...].reshape(72, wi32.shape[2]).astype(BF16)
    src, dst = iota((384, 72), 0), iota((384, 72), 1)
    pick = (
        (dst // 8 == 3 * (src % 128 // wide) + src // 128)
        & (dst % 8 == (src // side_cells) % chans)
        & (src % 128 < 3 * wide)
    )
    wc[...] = dot(pick.astype(F32).astype(BF16), wi72).astype(BF16)
    pltpu.make_async_copy(tables, tables, local_sem.at[2]).wait()
    pltpu.make_async_copy(limits, limits, local_sem.at[3]).wait()

    spread_r = (iota((size, span), 1) // side_cells == iota((size, span), 0)).astype(F32)
    spread_c = [
        (4 * (iota((size, span), 1) % side_cells) + q == iota((size, span), 0)).astype(F32)
        for q in range(4)
    ]
    spread_c = jnp.concatenate(spread_c, axis=1)
    row_w = dot(table_rows(tables[0].astype(F32), limits.at[0], row, nr, margin, inner), spread_r.astype(BF16))
    col_w = dot(table_rows(tables[1].astype(F32), limits.at[1], col, nc, margin, inner), spread_c.astype(BF16))
    lane = iota((1, span), 1)
    r_of, b_of = lane // side_cells, lane % side_cells
    inside = (
        (r_of >= margin) & (r_of < margin + inner) & (b_of >= HALO) & (b_of < HALO + tile)
    )
    for q in range(4):
        cw = col_w[:, q * span : (q + 1) * span]
        blend[q] = jnp.broadcast_to(row_w[0:1] * cw[0:1], (8, span))
        inverse[q] = jnp.broadcast_to(
            1.0 / jnp.where(inside, row_w[1:2] * cw[1:2], 1.0), (8, span)
        )

    send_later([e for e in LATER if e[1] != 0])

    load_out.wait()
    wo32[...] = jnp.zeros(wo32.shape, F32)
    wo32[:, 0 : wo.shape[1], :] = wo[...].astype(F32)
    loads[6].wait()
    out_mid = wm.shape[1]
    for t in range(9):
        wmt[:, out_mid * t : out_mid * (t + 1)] = wm[t].T
    loads[7].wait()
    out_low = wl.shape[1]
    for t in range(9):
        wlt[:, out_low * t : out_low * (t + 1)] = wl[t].T

    for_all(lambda n, m: batch(cells, n, send1, recv1).wait_send())
    for_all(lambda n, m: batch(cells, n, send1, recv1).wait_recv())

    cell = [cells[k].astype(F32) for k in range(9)]
    pieces = [[], [], []]
    for c in range(chans):
        for j, cut in enumerate((slice(tile - HALO, tile), slice(0, tile), slice(0, HALO))):
            upper, middle, lower = (cell[3 * i + j][c][:, cut] for i in range(3))
            zero = jnp.zeros((1, middle.shape[1]), F32)
            upper, lower = upper[tile - HALO :], lower[:HALO]
            pieces[0].append(jnp.concatenate([zero, upper, middle, lower[:-1]], axis=0))
            pieces[1].append(jnp.concatenate([upper, middle, lower], axis=0))
            pieces[2].append(jnp.concatenate([upper[1:], middle, lower, zero], axis=0))
    pieces = pieces[0] + pieces[1] + pieces[2]
    tall = jnp.concatenate(pieces + [jnp.zeros((side_cells, 128 - 3 * wide), F32)], axis=1)
    shape = (side_cells, side_cells, 128)
    spreaded = jnp.broadcast_to(tall[:, None, :], shape)
    gap = iota(shape, 2) % side_cells - iota(shape, 1)
    patches = [jnp.where(gap == dx - 1, spreaded, 0.0) for dx in range(3)]
    patches = jnp.concatenate(patches, axis=2).reshape(-1, 384).astype(BF16)
    first = dot(patches, wc[...]).reshape(side_cells, side_cells, -1)
    (first,) = group_silu([first])
    first = first.reshape(side_cells * side_cells, -1).astype(BF16)

    taps = dot(first, wmt[...])
    taps = [
        taps[:, out_mid * t : out_mid * (t + 1)].reshape(side_cells, side_cells, -1)
        for t in range(9)
    ]
    second = conv_up([[taps]], 1)
    second = group_silu([second[py][px] for py in range(2) for px in range(2)])
    second = jnp.concatenate(second, axis=0)
    second = second.reshape(-1, second.shape[2]).astype(BF16)

    n = side_cells * side_cells
    products = dot(second, wlt[...])
    products = [products[:, out_low * t : out_low * (t + 1)] for t in range(9)]
    taps = [
        [
            [
                p[(2 * py + px) * n : (2 * py + px + 1) * n].reshape(side_cells, side_cells, -1)
                for p in products
            ]
            for px in range(2)
        ]
        for py in range(2)
    ]
    third = conv_up(taps, 2)
    third = group_silu([third[qy][qx] for qy in range(4) for qx in range(4)])

    wo72 = wo32[...].reshape(72, wo32.shape[2]).astype(BF16)
    colour = []
    for qx in range(4):
        rows = jnp.stack([third[4 * qy + qx] for qy in range(4)], axis=1)
        colour.append(nt_dot(wo72, rows.reshape(span, rows.shape[-1]).astype(BF16)))

    def tap(q, t):
        return colour[q][8 * t : 8 * t + 8]

    where_b = iota((4, half), 1) % side_cells
    lower_half = iota((4, half), 1) < half // 2
    sub_b = iota((8, span), 1) % side_cells
    sub_r = iota((8, span), 1) // side_cells
    row_ok = [sub_r > 0, None, sub_r < size - 1]
    col_ok = [sub_b > 0, None, sub_b < side_cells - 1]

    def moved(x, dy, dx):
        shift = (side_cells * (1 - dy) + 1 - dx) % span
        x = pltpu.roll(x, shift, 1) if shift else x
        ok = [m for m in (row_ok[dy], col_ok[dx]) if m is not None]
        return jnp.where(functools.reduce(jnp.logical_and, ok), x, 0.0) if ok else x

    for q in range(4):
        value = None
        for dy in range(3):
            near = tap(q, 3 * dy + 1)
            if q > 0:
                near = near + tap(q - 1, 3 * dy)
            if q < 3:
                near = near + tap(q + 1, 3 * dy + 2)
            term = moved(near, dy, 1)
            if q == 0:
                term = term + moved(tap(3, 3 * dy), dy, 0)
            if q == 3:
                term = term + moved(tap(0, 3 * dy + 2), dy, 2)
            value = term if value is None else value + term
        value = value * blend[q]
        for h in range(2):
            own[h, q] = value[0:4, h * half : (h + 1) * half]

    for h in range(2):
        for k, rim in ((0, 0), (1, side_cells - HALO)):
            dense = pltpu.roll(own[h, 0], (half - rim) % half, 1)
            for q in range(1, 4):
                turned = pltpu.roll(own[h, q], (HALO * q - rim) % half, 1)
                dense = jnp.where(where_b // HALO == q, turned, dense)
            side_out[k, h] = dense

    def send_rims(entries):
        for k, (dr, dc) in entries:

            @pl.when(exists(dr, dc))
            def _():
                copies(k, dr, dc)[1].start()

    send_rims([e for e in FAR_FIRST if e[1][1] != 0])
    for h in range(2):
        for pair in range(2):
            even, odd = own[h, 2 * pair], own[h, 2 * pair + 1]
            if h == 0:
                odd = pltpu.roll(odd, half // 2, 1)
            else:
                even = pltpu.roll(even, half // 2, 1)
            vert_out[h, pair] = jnp.where(lower_half, even, odd)
    send_rims([e for e in FAR_FIRST if e[1][1] == 0])

    lane_row = iota((8, half), 1) // side_cells
    sublane = iota((8, half), 0)
    keep = [lane_row == sublane + 8, lane_row == sublane]
    beyond_row = [lane_row % 8 == sublane, lane_row % 8 == sublane]

    def spread_rows(piece, c, mask):
        return jnp.where(mask, jnp.broadcast_to(piece[c : c + 1], (8, half)), 0.0)

    def placed(blocks, place):
        tall = jnp.concatenate(blocks, axis=0)
        top = tall.astype(BF16)
        low = (tall - top.astype(F32)).astype(BF16)
        got = dot(jnp.concatenate([top, low], axis=0), place)
        return got[: tall.shape[0]] + got[tall.shape[0] :]

    place_src, place_dst = iota((4 * half, inner), 0), iota((4 * half, inner), 1)
    place = place_dst == 4 * (place_src % side_cells - HALO) + place_src // half
    place = place.astype(F32).astype(BF16)
    blocks = []
    for c in range(3):
        for h in range(2):
            mine = [own[h, q] * inverse[q, 0:4, h * half : (h + 1) * half] for q in range(4)]
            blocks.append(jnp.concatenate([spread_rows(p, c, keep[h]) for p in mine], axis=1))
    mine = placed(blocks, place)

    slot = place_src % side_cells
    from_left = place_dst == 4 * (slot % HALO) + slot // HALO
    from_right = place_dst == 4 * (tile - HALO + slot % HALO) + slot // HALO
    pair_q = 2 * (place_src // half - 2) + place_src % half // (half // 2)
    from_pair = place_dst == 4 * (slot - HALO) + pair_q
    part = place_src // half
    rim_place = jnp.where(
        part == 0, from_left.astype(F32), jnp.where(part == 1, from_right.astype(F32), from_pair.astype(F32))
    ).astype(BF16)
    scales = []
    for h in range(2):
        here = [inverse[q, 0:4, h * half : (h + 1) * half] for q in range(4)]
        sides = []
        for rim in (HALO, tile):
            dense = pltpu.roll(here[0], (half - rim) % half, 1)
            for q in range(1, 4):
                turned = pltpu.roll(here[q], (HALO * q - rim) % half, 1)
                dense = jnp.where(where_b // HALO == q, turned, dense)
            sides.append(dense)
        for pair in range(2):
            even, odd = here[2 * pair], here[2 * pair + 1]
            if h == 0:
                even = pltpu.roll(even, half // 2, 1)
            else:
                odd = pltpu.roll(odd, half // 2, 1)
            sides.append(jnp.where(lower_half, even, odd))
        scales.append(sides)

    for_all(lambda n, m: batch(rims, m, send2, recv2).wait_recv())

    blocks = []
    for c in range(3):
        for h in range(2):
            got = [
                (rims[h] + rims[4 + h]) * scales[h][0],
                (rims[2 + h] + rims[6 + h]) * scales[h][1],
                rims[8 + 2 * h] * scales[h][2],
                rims[9 + 2 * h] * scales[h][3],
            ]
            masks = [keep[h], keep[h], beyond_row[h], beyond_row[h]]
            blocks.append(
                jnp.concatenate([spread_rows(p, c, m) for p, m in zip(got, masks)], axis=1)
            )
    out[...] = (mine + placed(blocks, rim_place)).reshape(3, inner, inner)

    for_all(lambda n, m: batch(rims, m, send2, recv2).wait_send())


def solution(mesh):
    nr, nc = mesh.shape["rows"], mesh.shape["cols"]

    def per_device(lat, w_in, w_mid, w_low, w_out, ramp_r, ramp_c, lim_r, lim_c):
        tile = lat.shape[1]
        inner = 4 * tile
        size = inner + 8 * HALO
        half = size * (tile + 2 * HALO) // 2
        anywhere = pl.BlockSpec(memory_space=pltpu.HBM)
        dma = pltpu.SemaphoreType.DMA
        return pl.pallas_call(
            functools.partial(kernel, nr, nc),
            out_shape=pltpu.VMEM((w_out.shape[1], inner, inner), F32),
            in_specs=[anywhere] * 9,
            out_specs=pl.BlockSpec(memory_space=pltpu.VMEM),
            scratch_shapes=[
                pltpu.VMEM((9,) + lat.shape, BF16),
                pltpu.VMEM(w_in.shape, BF16),
                pltpu.VMEM(w_mid.shape, BF16),
                pltpu.VMEM(w_low.shape, BF16),
                pltpu.VMEM(w_out.shape, BF16),
                pltpu.VMEM((2,) + ramp_r.shape, jnp.int32),
                pltpu.SMEM((2,) + lim_r.shape, jnp.int32),
                pltpu.VMEM((9, 8, w_in.shape[2]), F32),
                pltpu.VMEM((9, 8, w_out.shape[2]), F32),
                pltpu.VMEM((384, w_in.shape[2]), BF16),
                pltpu.VMEM((w_mid.shape[2], 9 * w_mid.shape[1]), BF16),
                pltpu.VMEM((w_low.shape[2], 9 * w_low.shape[1]), BF16),
                pltpu.VMEM((4, 8, 2 * half), F32),
                pltpu.VMEM((4, 8, 2 * half), F32),
                pltpu.VMEM((2, 4, 4, half), F32),
                pltpu.VMEM((2, 2, 4, half), F32),
                pltpu.VMEM((2, 2, 4, half), F32),
                pltpu.VMEM((12, 4, half), F32),
                dma((6,)),
                pltpu.SemaphoreType.REGULAR((4,)),
                dma,
                dma,
            ],
            compiler_params=pltpu.CompilerParams(
                collective_id=0, has_side_effects=True
            ),
            name="decode",
        )(lat, w_in, w_mid, w_low, w_out, ramp_r, ramp_c, lim_r, lim_c)

    return jax.shard_map(
        per_device,
        mesh=mesh,
        in_specs=(P(None, ("groups", "rows"), "cols"), P(), P(), P(), P(), P(), P(), P(), P()),
        out_specs=P(None, ("groups", "rows"), "cols"),
        check_vma=False,
    )
```

```python
import functools

import jax
import jax.numpy as jnp
from jax import lax
from jax.experimental import pallas as pl
from jax.experimental.pallas import tpu as pltpu
from jax.sharding import PartitionSpec as P

MESH = pl.DeviceIdType.MESH
NGROUPS = 32
HALO = 2
F32 = jnp.float32
BF16 = jnp.bfloat16
AROUND = [(dr, dc) for dr in (-1, 0, 1) for dc in (-1, 0, 1) if (dr, dc) != (0, 0)]
FAR_FIRST = sorted(enumerate(AROUND), key=lambda e: -abs(e[1][0]) - abs(e[1][1]))
READY = {k: n for n, k in enumerate((3, 4, 5, 6, 7))}


def iota(shape, dim):
    return lax.broadcasted_iota(jnp.int32, shape, dim)


def nt_dot(a, b):
    return lax.dot_general(a, b, (((1,), (1,)), ((), ())), preferred_element_type=F32)


def dot(a, b):
    return jnp.dot(a, b, preferred_element_type=F32)


def down(x):
    return jnp.concatenate([jnp.zeros_like(x[:1]), x[:-1]], axis=0)


def up(x):
    return jnp.concatenate([x[1:], jnp.zeros_like(x[:1])], axis=0)


def right(x):
    rolled = pltpu.roll(x, 1, 1)
    return jnp.where(iota(x.shape, 1) == 0, 0.0, rolled)


def left(x):
    n = x.shape[1]
    rolled = pltpu.roll(x, n - 1, 1)
    return jnp.where(iota(x.shape, 1) == n - 1, 0.0, rolled)


def expand(products, fine, before, after):
    out = []
    for q in range(fine):
        t0, t1, t2 = products[q]
        prev = products[q - 1][0] if q > 0 else before(products[fine - 1][0])
        nxt = products[q + 1][2] if q < fine - 1 else after(products[0][2])
        out.append(prev + (t1 + t2))
        out.append((t0 + t1) + nxt)
    return out


def conv_up(taps, fine):
    by_col = [
        [
            expand(
                [[taps[py][px][3 * dy + dx] for dy in range(3)] for py in range(fine)],
                fine,
                down,
                up,
            )
            for dx in range(3)
        ]
        for px in range(fine)
    ]
    return [
        expand(
            [[by_col[px][dx][qy] for dx in range(3)] for px in range(fine)],
            fine,
            right,
            left,
        )
        for qy in range(2 * fine)
    ]


def group_silu(phases):
    channels = phases[0].shape[-1]
    width = channels // NGROUPS
    count = channels // 128
    positions = len(phases) * phases[0].shape[0] * phases[0].shape[1]
    scale = 1.0 / (positions * width)
    block = (iota((384, 128), 0) % 128 // width == iota((384, 128), 1) // width).astype(F32)
    block = block.astype(BF16)
    total = jnp.sum(functools.reduce(jnp.add, phases), axis=(0, 1)).reshape(1, channels)
    squares = functools.reduce(jnp.add, [p * p for p in phases])
    squares = jnp.sum(squares, axis=(0, 1)).reshape(1, channels)
    rows = [x[:, k * 128 : (k + 1) * 128] for x in (total, squares) for k in range(count)]
    rows = jnp.concatenate(rows + [jnp.zeros((1, 128), F32)] * (8 - len(rows)), axis=0)
    top = rows.astype(BF16)
    rest = rows - top.astype(F32)
    mid = rest.astype(BF16)
    low = (rest - mid.astype(F32)).astype(BF16)
    got = dot(jnp.concatenate([top, mid, low], axis=1), block) * scale
    center = got[:count]
    spread = jnp.maximum(got[count : 2 * count] - center * center, 0.0)
    factor = 0.5 * lax.rsqrt(spread + 1e-06)
    offset = center * factor
    factor = jnp.concatenate([factor[k : k + 1] for k in range(count)], axis=1)[None]
    offset = jnp.concatenate([offset[k : k + 1] for k in range(count)], axis=1)[None]
    result = []
    for p in phases:
        half = p * factor - offset
        result.append(half + half * jnp.tanh(half))
    return result


def table_rows(table, limits, index, count, margin, inner):
    size = table.shape[1]
    pos = iota((1, size), 1)
    far = jnp.maximum(jnp.maximum(margin - pos, pos - (margin + inner) + 1), 0)
    rows = []
    for d in (-1, 0, 1):
        here = index + d
        limit = limits[jnp.clip(here, 0, count - 1)]
        picked = jnp.where(iota(table.shape, 0) == here, table, 0.0)
        row = jnp.sum(picked, axis=0, keepdims=True)
        rows.append(jnp.where(far <= limit, row, 0.0))
    above, own, below = rows
    other = jnp.where(pos < inner, jnp.roll(above, inner, 1), jnp.roll(below, inner, 1))
    pair = jnp.concatenate([own, own + other, jnp.zeros((6, size), F32)], axis=0)
    return pair.astype(BF16)


def kernel(
    nr, nc, lat, w_in, w_mid, w_low, w_out, ramp_r, ramp_c, lim_r, lim_c, out,
    cells, wi, wm, wl, wo, tables, limits, wi32, wo32, wc, wmt, wlt,
    blend, inverse, own, side_out, vert_out, rims,
    local_sem, ready, recv1, recv2,
):
    row, col = lax.axis_index("rows"), lax.axis_index("cols")

    def exists(dr, dc):
        ok = None
        for d, here, n in ((dr, row, nr), (dc, col, nc)):
            test = None if d == 0 else (here > 0 if d < 0 else here < n - 1)
            if test is not None:
                ok = test if ok is None else jnp.logical_and(ok, test)
        return ok

    def device(dr, dc):
        return {"rows": row + dr, "cols": col + dc}

    loads = [
        pltpu.make_async_copy(src, dst, local_sem.at[k])
        for k, src, dst in [
            (0, lat, cells.at[4]),
            (1, w_in, wi),
            (2, ramp_r, tables.at[0]),
            (2, ramp_c, tables.at[1]),
            (3, lim_r, limits.at[0]),
            (3, lim_c, limits.at[1]),
            (4, w_mid, wm),
            (5, w_low, wl),
        ]
    ]
    load_out = pltpu.make_async_copy(w_out, wo, local_sem.at[1])
    send1, send2 = local_sem.at[0], local_sem.at[0]
    for load in loads:
        load.start()

    odd = col % 2 == 1

    def mutual(dr, dc):
        return jnp.logical_and(row == (0 if dr > 0 else 1), odd if dc > 0 else jnp.logical_not(odd))

    def leads(dr, dc):
        there = exists(dr, dc)
        return there if dr > 0 else jnp.logical_and(there, odd)

    def greets(dr, dc):
        there = exists(dr, dc)
        if dr < 0:
            return jnp.logical_and(there, mutual(dr, dc)) if dc else None
        return leads(dr, dc)

    def greeted_by(dr, dc):
        there = exists(dr, dc)
        if dr > 0:
            return jnp.logical_and(there, mutual(dr, dc)) if dc else None
        return there if dr < 0 else jnp.logical_and(there, jnp.logical_not(odd))

    def alone(test, other):
        return test if other is None else jnp.logical_and(test, jnp.logical_not(other))

    barrier = pltpu.get_barrier_semaphore()
    earlier = 0
    for dr, dc in AROUND:
        test = greets(dr, dc)
        if test is not None:

            @pl.when(test)
            def _():
                pl.semaphore_signal(barrier, inc=1, device_id=device(dr, dc), device_id_type=MESH)

    for dr, dc in AROUND:
        test = greeted_by(dr, dc)
        if test is not None:
            earlier += test.astype(jnp.int32)

    def slot_of(dr, dc):
        up_down, left_right = (dr + 1) // 2, (dc + 1) // 2
        if dr == 0:
            return rims.at[pl.ds(2 * left_right, 2)]
        if dc == 0:
            return rims.at[pl.ds(8 + 2 * up_down, 2)]
        return rims.at[4 + 2 * left_right + up_down]

    def packed(dr, dc):
        up_down, left_right = (dr + 1) // 2, (dc + 1) // 2
        if dr == 0:
            return side_out.at[left_right]
        return vert_out.at[up_down] if dc == 0 else side_out.at[left_right, up_down]

    def copies(k, dr, dc):
        first = pltpu.make_async_remote_copy(
            src_ref=cells.at[4],
            dst_ref=cells.at[(1 - dr) * 3 + 1 - dc],
            send_sem=send1,
            recv_sem=recv1,
            device_id=device(dr, dc),
            device_id_type=MESH,
        )
        second = pltpu.make_async_remote_copy(
            src_ref=packed(dr, dc),
            dst_ref=slot_of(-dr, -dc),
            send_sem=send2,
            recv_sem=recv2,
            device_id=device(dr, dc),
            device_id_type=MESH,
        )
        return first, second

    above_below = (row > 0).astype(jnp.int32) + (row < nr - 1).astype(jnp.int32)
    beside = (col > 0).astype(jnp.int32) + (col < nc - 1).astype(jnp.int32)

    def for_all(wait):
        for v in range(min(nr, 2) - 1, min(nr, 3)):
            for h in range(min(nc, 2) - 1, min(nc, 3)):
                if v + h == 0:
                    continue

                @pl.when(jnp.logical_and(above_below == v, beside == h))
                def _():
                    wait(v + h + v * h, 2 * (v + h) + v * h)

    def batch(ref, n, send, recv):
        part = ref.at[pl.ds(0, n)]
        return pltpu.make_async_remote_copy(
            src_ref=part,
            dst_ref=part,
            send_sem=send,
            recv_sem=recv,
            device_id=device(0, 0),
            device_id_type=MESH,
        )

    for k, (dr, dc) in enumerate(AROUND):

        @pl.when(jnp.logical_not(exists(dr, dc)))
        def _():
            slot = cells.at[(1 + dr) * 3 + 1 + dc]
            slot[...] = jnp.zeros(slot.shape, BF16)
            pixels = slot_of(dr, dc)
            pixels[...] = jnp.zeros(pixels.shape, F32)

    @pl.when(earlier > 0)
    def _():
        pl.semaphore_wait(barrier, earlier)

    for k, (dr, dc) in FAR_FIRST:
        if dr <= 0:
            by = greeted_by(dr, dc)

            @pl.when(alone(by, greets(dr, dc) if dr * dc else None))
            def _():
                pl.semaphore_signal(
                    ready.at[READY[7 - k]], inc=1, device_id=device(dr, dc), device_id_type=MESH
                )

    loads[0].wait()
    for k, (dr, dc) in FAR_FIRST:
        by = greeted_by(dr, dc)
        if by is not None:

            @pl.when(by)
            def _():
                copies(k, dr, dc)[0].start()

    def send_later(entries):
        for k, (dr, dc) in entries:

            @pl.when(alone(leads(dr, dc), greeted_by(dr, dc) if dr else None))
            def _():
                pl.semaphore_wait(ready.at[READY[k]], 1)
                copies(k, dr, dc)[0].start()

    send_later([e for e in enumerate(AROUND) if e[1][0] == 0])

    tile = lat.shape[1]
    side_cells = tile + 2 * HALO
    margin, inner = 4 * HALO, 4 * tile
    size = inner + 2 * margin
    chans = lat.shape[0]
    span = size * side_cells
    half = span // 2
    wide = chans * side_cells

    loads[1].wait()
    load_out.start()
    wi32[...] = jnp.zeros(wi32.shape, F32)
    wi32[:, 0 : wi.shape[1], :] = wi[...].astype(F32)
    wi72 = wi32[...].reshape(72, wi32.shape[2]).astype(BF16)
    src, dst = iota((384, 72), 0), iota((384, 72), 1)
    pick = (
        (dst // 8 == 3 * (src % 128 // wide) + src // 128)
        & (dst % 8 == (src // side_cells) % chans)
        & (src % 128 < 3 * wide)
    )
    wc[...] = dot(pick.astype(F32).astype(BF16), wi72).astype(BF16)
    pltpu.make_async_copy(tables, tables, local_sem.at[2]).wait()
    pltpu.make_async_copy(limits, limits, local_sem.at[3]).wait()

    spread_r = (iota((size, span), 1) // side_cells == iota((size, span), 0)).astype(F32)
    spread_c = [
        (4 * (iota((size, span), 1) % side_cells) + q == iota((size, span), 0)).astype(F32)
        for q in range(4)
    ]
    spread_c = jnp.concatenate(spread_c, axis=1)
    row_w = dot(table_rows(tables[0].astype(F32), limits.at[0], row, nr, margin, inner), spread_r.astype(BF16))
    col_w = dot(table_rows(tables[1].astype(F32), limits.at[1], col, nc, margin, inner), spread_c.astype(BF16))
    lane = iota((1, span), 1)
    r_of, b_of = lane // side_cells, lane % side_cells
    inside = (
        (r_of >= margin) & (r_of < margin + inner) & (b_of >= HALO) & (b_of < HALO + tile)
    )
    for q in range(4):
        cw = col_w[:, q * span : (q + 1) * span]
        blend[q] = jnp.broadcast_to(row_w[0:1] * cw[0:1], (8, span))
        inverse[q] = jnp.broadcast_to(
            1.0 / jnp.where(inside, row_w[1:2] * cw[1:2], 1.0), (8, span)
        )

    send_later([e for e in enumerate(AROUND) if e[1][0] > 0])

    load_out.wait()
    wo32[...] = jnp.zeros(wo32.shape, F32)
    wo32[:, 0 : wo.shape[1], :] = wo[...].astype(F32)
    loads[6].wait()
    out_mid = wm.shape[1]
    for t in range(9):
        wmt[:, out_mid * t : out_mid * (t + 1)] = wm[t].T
    loads[7].wait()
    out_low = wl.shape[1]
    for t in range(9):
        wlt[:, out_low * t : out_low * (t + 1)] = wl[t].T

    for_all(lambda n, m: batch(cells, n, send1, recv1).wait_send())
    for_all(lambda n, m: batch(cells, n, send1, recv1).wait_recv())

    cell = [cells[k].astype(F32) for k in range(9)]
    pieces = [[], [], []]
    for c in range(chans):
        for j, cut in enumerate((slice(tile - HALO, tile), slice(0, tile), slice(0, HALO))):
            upper, middle, lower = (cell[3 * i + j][c][:, cut] for i in range(3))
            zero = jnp.zeros((1, middle.shape[1]), F32)
            upper, lower = upper[tile - HALO :], lower[:HALO]
            pieces[0].append(jnp.concatenate([zero, upper, middle, lower[:-1]], axis=0))
            pieces[1].append(jnp.concatenate([upper, middle, lower], axis=0))
            pieces[2].append(jnp.concatenate([upper[1:], middle, lower, zero], axis=0))
    pieces = pieces[0] + pieces[1] + pieces[2]
    tall = jnp.concatenate(pieces + [jnp.zeros((side_cells, 128 - 3 * wide), F32)], axis=1)
    shape = (side_cells, side_cells, 128)
    spreaded = jnp.broadcast_to(tall[:, None, :], shape)
    gap = iota(shape, 2) % side_cells - iota(shape, 1)
    patches = [jnp.where(gap == dx - 1, spreaded, 0.0) for dx in range(3)]
    patches = jnp.concatenate(patches, axis=2).reshape(-1, 384).astype(BF16)
    first = dot(patches, wc[...]).reshape(side_cells, side_cells, -1)
    (first,) = group_silu([first])
    first = first.reshape(side_cells * side_cells, -1).astype(BF16)

    taps = dot(first, wmt[...])
    taps = [
        taps[:, out_mid * t : out_mid * (t + 1)].reshape(side_cells, side_cells, -1)
        for t in range(9)
    ]
    second = conv_up([[taps]], 1)
    second = group_silu([second[py][px] for py in range(2) for px in range(2)])
    second = jnp.concatenate(second, axis=0)
    second = second.reshape(-1, second.shape[2]).astype(BF16)

    n = side_cells * side_cells
    products = dot(second, wlt[...])
    products = [products[:, out_low * t : out_low * (t + 1)] for t in range(9)]
    taps = [
        [
            [
                p[(2 * py + px) * n : (2 * py + px + 1) * n].reshape(side_cells, side_cells, -1)
                for p in products
            ]
            for px in range(2)
        ]
        for py in range(2)
    ]
    third = conv_up(taps, 2)
    third = group_silu([third[qy][qx] for qy in range(4) for qx in range(4)])

    wo72 = wo32[...].reshape(72, wo32.shape[2]).astype(BF16)
    colour = []
    for qx in range(4):
        rows = jnp.stack([third[4 * qy + qx] for qy in range(4)], axis=1)
        colour.append(nt_dot(wo72, rows.reshape(span, rows.shape[-1]).astype(BF16)))

    def tap(q, t):
        return colour[q][8 * t : 8 * t + 8]

    where_b = iota((4, half), 1) % side_cells
    lower_half = iota((4, half), 1) < half // 2
    sub_b = iota((8, span), 1) % side_cells
    sub_r = iota((8, span), 1) // side_cells
    row_ok = [sub_r > 0, None, sub_r < size - 1]
    col_ok = [sub_b > 0, None, sub_b < side_cells - 1]

    def moved(x, dy, dx):
        shift = (side_cells * (1 - dy) + 1 - dx) % span
        x = pltpu.roll(x, shift, 1) if shift else x
        ok = [m for m in (row_ok[dy], col_ok[dx]) if m is not None]
        return jnp.where(functools.reduce(jnp.logical_and, ok), x, 0.0) if ok else x

    for q in range(4):
        value = None
        for dy in range(3):
            near = tap(q, 3 * dy + 1)
            if q > 0:
                near = near + tap(q - 1, 3 * dy)
            if q < 3:
                near = near + tap(q + 1, 3 * dy + 2)
            term = moved(near, dy, 1)
            if q == 0:
                term = term + moved(tap(3, 3 * dy), dy, 0)
            if q == 3:
                term = term + moved(tap(0, 3 * dy + 2), dy, 2)
            value = term if value is None else value + term
        value = value * blend[q]
        for h in range(2):
            own[h, q] = value[0:4, h * half : (h + 1) * half]

    for h in range(2):
        for k, rim in ((0, 0), (1, side_cells - HALO)):
            dense = pltpu.roll(own[h, 0], (half - rim) % half, 1)
            for q in range(1, 4):
                turned = pltpu.roll(own[h, q], (HALO * q - rim) % half, 1)
                dense = jnp.where(where_b // HALO == q, turned, dense)
            side_out[k, h] = dense
        for pair in range(2):
            even, odds = own[h, 2 * pair], own[h, 2 * pair + 1]
            if h == 0:
                odds = pltpu.roll(odds, half // 2, 1)
            else:
                even = pltpu.roll(even, half // 2, 1)
            vert_out[h, pair] = jnp.where(lower_half, even, odds)

    for k, (dr, dc) in FAR_FIRST:

        @pl.when(exists(dr, dc))
        def _():
            copies(k, dr, dc)[1].start()

    lane_row = iota((8, half), 1) // side_cells
    sublane = iota((8, half), 0)
    keep = [lane_row == sublane + 8, lane_row == sublane]
    beyond_row = [lane_row % 8 == sublane, lane_row % 8 == sublane]

    def spread_rows(piece, c, mask):
        return jnp.where(mask, jnp.broadcast_to(piece[c : c + 1], (8, half)), 0.0)

    def placed(blocks, place):
        tall = jnp.concatenate(blocks, axis=0)
        top = tall.astype(BF16)
        low = (tall - top.astype(F32)).astype(BF16)
        got = dot(jnp.concatenate([top, low], axis=0), place)
        return got[: tall.shape[0]] + got[tall.shape[0] :]

    place_src, place_dst = iota((4 * half, inner), 0), iota((4 * half, inner), 1)
    place = place_dst == 4 * (place_src % side_cells - HALO) + place_src // half
    place = place.astype(F32).astype(BF16)
    blocks = []
    for c in range(3):
        for h in range(2):
            mine = [own[h, q] * inverse[q, 0:4, h * half : (h + 1) * half] for q in range(4)]
            blocks.append(jnp.concatenate([spread_rows(p, c, keep[h]) for p in mine], axis=1))
    mine = placed(blocks, place)

    slot = place_src % side_cells
    from_left = place_dst == 4 * (slot % HALO) + slot // HALO
    from_right = place_dst == 4 * (tile - HALO + slot % HALO) + slot // HALO
    pair_q = 2 * (place_src // half - 2) + place_src % half // (half // 2)
    from_pair = place_dst == 4 * (slot - HALO) + pair_q
    part = place_src // half
    rim_place = jnp.where(
        part == 0, from_left.astype(F32), jnp.where(part == 1, from_right.astype(F32), from_pair.astype(F32))
    ).astype(BF16)
    scales = []
    for h in range(2):
        here = [inverse[q, 0:4, h * half : (h + 1) * half] for q in range(4)]
        sides = []
        for rim in (HALO, tile):
            dense = pltpu.roll(here[0], (half - rim) % half, 1)
            for q in range(1, 4):
                turned = pltpu.roll(here[q], (HALO * q - rim) % half, 1)
                dense = jnp.where(where_b // HALO == q, turned, dense)
            sides.append(dense)
        for pair in range(2):
            even, odds = here[2 * pair], here[2 * pair + 1]
            if h == 0:
                even = pltpu.roll(even, half // 2, 1)
            else:
                odds = pltpu.roll(odds, half // 2, 1)
            sides.append(jnp.where(lower_half, even, odds))
        scales.append(sides)

    for_all(lambda n, m: batch(rims, m, send2, recv2).wait_recv())

    blocks = []
    for c in range(3):
        for h in range(2):
            got = [
                (rims[h] + rims[4 + h]) * scales[h][0],
                (rims[2 + h] + rims[6 + h]) * scales[h][1],
                rims[8 + 2 * h] * scales[h][2],
                rims[9 + 2 * h] * scales[h][3],
            ]
            masks = [keep[h], keep[h], beyond_row[h], beyond_row[h]]
            blocks.append(
                jnp.concatenate([spread_rows(p, c, m) for p, m in zip(got, masks)], axis=1)
            )
    out[...] = (mine + placed(blocks, rim_place)).reshape(3, inner, inner)

    for_all(lambda n, m: batch(rims, m, send2, recv2).wait_send())


def solution(mesh):
    nr, nc = mesh.shape["rows"], mesh.shape["cols"]

    def per_device(lat, w_in, w_mid, w_low, w_out, ramp_r, ramp_c, lim_r, lim_c):
        tile = lat.shape[1]
        inner = 4 * tile
        size = inner + 8 * HALO
        half = size * (tile + 2 * HALO) // 2
        anywhere = pl.BlockSpec(memory_space=pltpu.HBM)
        dma = pltpu.SemaphoreType.DMA
        return pl.pallas_call(
            functools.partial(kernel, nr, nc),
            out_shape=pltpu.VMEM((w_out.shape[1], inner, inner), F32),
            in_specs=[anywhere] * 9,
            out_specs=pl.BlockSpec(memory_space=pltpu.VMEM),
            scratch_shapes=[
                pltpu.VMEM((9,) + lat.shape, BF16),
                pltpu.VMEM(w_in.shape, BF16),
                pltpu.VMEM(w_mid.shape, BF16),
                pltpu.VMEM(w_low.shape, BF16),
                pltpu.VMEM(w_out.shape, BF16),
                pltpu.VMEM((2,) + ramp_r.shape, jnp.int32),
                pltpu.SMEM((2,) + lim_r.shape, jnp.int32),
                pltpu.VMEM((9, 8, w_in.shape[2]), F32),
                pltpu.VMEM((9, 8, w_out.shape[2]), F32),
                pltpu.VMEM((384, w_in.shape[2]), BF16),
                pltpu.VMEM((w_mid.shape[2], 9 * w_mid.shape[1]), BF16),
                pltpu.VMEM((w_low.shape[2], 9 * w_low.shape[1]), BF16),
                pltpu.VMEM((4, 8, 2 * half), F32),
                pltpu.VMEM((4, 8, 2 * half), F32),
                pltpu.VMEM((2, 4, 4, half), F32),
                pltpu.VMEM((2, 2, 4, half), F32),
                pltpu.VMEM((2, 2, 4, half), F32),
                pltpu.VMEM((12, 4, half), F32),
                dma((6,)),
                pltpu.SemaphoreType.REGULAR((5,)),
                dma,
                dma,
            ],
            compiler_params=pltpu.CompilerParams(
                collective_id=0, has_side_effects=True
            ),
            name="decode",
        )(lat, w_in, w_mid, w_low, w_out, ramp_r, ramp_c, lim_r, lim_c)

    return jax.shard_map(
        per_device,
        mesh=mesh,
        in_specs=(P(None, ("groups", "rows"), "cols"), P(), P(), P(), P(), P(), P(), P(), P()),
        out_specs=P(None, ("groups", "rows"), "cols"),
        check_vma=False,
    )
```

```python
import functools

import jax
import jax.numpy as jnp
from jax import lax
from jax.experimental import pallas as pl
from jax.experimental.pallas import tpu as pltpu
from jax.sharding import PartitionSpec as P

MESH = pl.DeviceIdType.MESH
NGROUPS = 32
HALO = 2
F32 = jnp.float32
BF16 = jnp.bfloat16
AROUND = [(dr, dc) for dr in (-1, 0, 1) for dc in (-1, 0, 1) if (dr, dc) != (0, 0)]
FAR_FIRST = sorted(enumerate(AROUND), key=lambda e: -abs(e[1][0]) - abs(e[1][1]))
READY = {k: n for n, k in enumerate((3, 4, 5, 6, 7))}


def iota(shape, dim):
    return lax.broadcasted_iota(jnp.int32, shape, dim)


def nt_dot(a, b):
    return lax.dot_general(a, b, (((1,), (1,)), ((), ())), preferred_element_type=F32)


def dot(a, b):
    return jnp.dot(a, b, preferred_element_type=F32)


def down(x):
    return jnp.concatenate([jnp.zeros_like(x[:1]), x[:-1]], axis=0)


def up(x):
    return jnp.concatenate([x[1:], jnp.zeros_like(x[:1])], axis=0)


def right(x):
    rolled = pltpu.roll(x, 1, 1)
    return jnp.where(iota(x.shape, 1) == 0, 0.0, rolled)


def left(x):
    n = x.shape[1]
    rolled = pltpu.roll(x, n - 1, 1)
    return jnp.where(iota(x.shape, 1) == n - 1, 0.0, rolled)


def expand(products, fine, before, after):
    out = []
    for q in range(fine):
        t0, t1, t2 = products[q]
        prev = products[q - 1][0] if q > 0 else before(products[fine - 1][0])
        nxt = products[q + 1][2] if q < fine - 1 else after(products[0][2])
        out.append(prev + (t1 + t2))
        out.append((t0 + t1) + nxt)
    return out


def conv_up(taps, fine):
    by_col = [
        [
            expand(
                [[taps[py][px][3 * dy + dx] for dy in range(3)] for py in range(fine)],
                fine,
                down,
                up,
            )
            for dx in range(3)
        ]
        for px in range(fine)
    ]
    return [
        expand(
            [[by_col[px][dx][qy] for dx in range(3)] for px in range(fine)],
            fine,
            right,
            left,
        )
        for qy in range(2 * fine)
    ]


def group_silu(phases):
    channels = phases[0].shape[-1]
    width = channels // NGROUPS
    count = channels // 128
    positions = len(phases) * phases[0].shape[0] * phases[0].shape[1]
    scale = 1.0 / (positions * width)
    block = (iota((384, 128), 0) % 128 // width == iota((384, 128), 1) // width).astype(F32)
    block = block.astype(BF16)
    total = jnp.sum(functools.reduce(jnp.add, phases), axis=(0, 1)).reshape(1, channels)
    squares = functools.reduce(jnp.add, [p * p for p in phases])
    squares = jnp.sum(squares, axis=(0, 1)).reshape(1, channels)
    rows = [x[:, k * 128 : (k + 1) * 128] for x in (total, squares) for k in range(count)]
    rows = jnp.concatenate(rows + [jnp.zeros((1, 128), F32)] * (8 - len(rows)), axis=0)
    top = rows.astype(BF16)
    rest = rows - top.astype(F32)
    mid = rest.astype(BF16)
    low = (rest - mid.astype(F32)).astype(BF16)
    got = dot(jnp.concatenate([top, mid, low], axis=1), block) * scale
    center = got[:count]
    spread = jnp.maximum(got[count : 2 * count] - center * center, 0.0)
    factor = 0.5 * lax.rsqrt(spread + 1e-06)
    offset = center * factor
    factor = jnp.concatenate([factor[k : k + 1] for k in range(count)], axis=1)[None]
    offset = jnp.concatenate([offset[k : k + 1] for k in range(count)], axis=1)[None]
    result = []
    for p in phases:
        half = p * factor - offset
        result.append(half + half * jnp.tanh(half))
    return result


def table_rows(table, limits, index, count, margin, inner):
    size = table.shape[1]
    pos = iota((1, size), 1)
    far = jnp.maximum(jnp.maximum(margin - pos, pos - (margin + inner) + 1), 0)
    rows = []
    for d in (-1, 0, 1):
        here = index + d
        limit = limits[jnp.clip(here, 0, count - 1)]
        picked = jnp.where(iota(table.shape, 0) == here, table, 0.0)
        row = jnp.sum(picked, axis=0, keepdims=True)
        rows.append(jnp.where(far <= limit, row, 0.0))
    above, own, below = rows
    other = jnp.where(pos < inner, jnp.roll(above, inner, 1), jnp.roll(below, inner, 1))
    pair = jnp.concatenate([own, own + other, jnp.zeros((6, size), F32)], axis=0)
    return pair.astype(BF16)


def kernel(
    nr, nc, lat, w_in, w_mid, w_low, w_out, ramp_r, ramp_c, lim_r, lim_c, out,
    cells, wi, wm, wl, wo, tables, limits, wi32, wo32, wc, wmt, wlt,
    blend, inverse, own, side_out, vert_out, rims,
    local_sem, ready, recv1, recv2,
):
    row, col = lax.axis_index("rows"), lax.axis_index("cols")

    def exists(dr, dc):
        ok = None
        for d, here, n in ((dr, row, nr), (dc, col, nc)):
            test = None if d == 0 else (here > 0 if d < 0 else here < n - 1)
            if test is not None:
                ok = test if ok is None else jnp.logical_and(ok, test)
        return ok

    def device(dr, dc):
        return {"rows": row + dr, "cols": col + dc}

    loads = [
        pltpu.make_async_copy(src, dst, local_sem.at[k])
        for k, src, dst in [
            (0, lat, cells.at[4]),
            (1, w_in, wi),
            (2, ramp_r, tables.at[0]),
            (2, ramp_c, tables.at[1]),
            (3, lim_r, limits.at[0]),
            (3, lim_c, limits.at[1]),
            (4, w_mid, wm),
            (5, w_low, wl),
        ]
    ]
    load_out = pltpu.make_async_copy(w_out, wo, local_sem.at[1])
    send1, send2 = local_sem.at[0], local_sem.at[1]
    for load in loads:
        load.start()

    odd = col % 2 == 1

    def mutual(dr, dc):
        return jnp.logical_and(row == (0 if dr > 0 else 1), odd if dc > 0 else jnp.logical_not(odd))

    def leads(dr, dc):
        there = exists(dr, dc)
        return there if dr > 0 else jnp.logical_and(there, odd)

    def greets(dr, dc):
        there = exists(dr, dc)
        if dr < 0:
            return jnp.logical_and(there, mutual(dr, dc)) if dc else None
        return leads(dr, dc)

    def greeted_by(dr, dc):
        there = exists(dr, dc)
        if dr > 0:
            return jnp.logical_and(there, mutual(dr, dc)) if dc else None
        return there if dr < 0 else jnp.logical_and(there, jnp.logical_not(odd))

    def alone(test, other):
        return test if other is None else jnp.logical_and(test, jnp.logical_not(other))

    barrier = pltpu.get_barrier_semaphore()
    earlier = 0
    for dr, dc in AROUND:
        test = greets(dr, dc)
        if test is not None:

            @pl.when(test)
            def _():
                pl.semaphore_signal(barrier, inc=1, device_id=device(dr, dc), device_id_type=MESH)

    for dr, dc in AROUND:
        test = greeted_by(dr, dc)
        if test is not None:
            earlier += test.astype(jnp.int32)

    def slot_of(dr, dc):
        up_down, left_right = (dr + 1) // 2, (dc + 1) // 2
        if dr == 0:
            return rims.at[pl.ds(2 * left_right, 2)]
        if dc == 0:
            return rims.at[pl.ds(8 + 2 * up_down, 2)]
        return rims.at[4 + 2 * left_right + up_down]

    def packed(dr, dc):
        up_down, left_right = (dr + 1) // 2, (dc + 1) // 2
        if dr == 0:
            return side_out.at[left_right]
        return vert_out.at[up_down] if dc == 0 else side_out.at[left_right, up_down]

    def copies(k, dr, dc):
        first = pltpu.make_async_remote_copy(
            src_ref=cells.at[4],
            dst_ref=cells.at[(1 - dr) * 3 + 1 - dc],
            send_sem=send1,
            recv_sem=recv1,
            device_id=device(dr, dc),
            device_id_type=MESH,
        )
        second = pltpu.make_async_remote_copy(
            src_ref=packed(dr, dc),
            dst_ref=slot_of(-dr, -dc),
            send_sem=send2,
            recv_sem=recv2,
            device_id=device(dr, dc),
            device_id_type=MESH,
        )
        return first, second

    above_below = (row > 0).astype(jnp.int32) + (row < nr - 1).astype(jnp.int32)
    beside = (col > 0).astype(jnp.int32) + (col < nc - 1).astype(jnp.int32)

    def for_all(wait):
        for v in range(min(nr, 2) - 1, min(nr, 3)):
            for h in range(min(nc, 2) - 1, min(nc, 3)):
                if v + h == 0:
                    continue

                @pl.when(jnp.logical_and(above_below == v, beside == h))
                def _():
                    wait(v + h + v * h, 2 * (v + h) + v * h)

    def batch(ref, n, send, recv):
        part = ref.at[pl.ds(0, n)]
        return pltpu.make_async_remote_copy(
            src_ref=part,
            dst_ref=part,
            send_sem=send,
            recv_sem=recv,
            device_id=device(0, 0),
            device_id_type=MESH,
        )

    for k, (dr, dc) in enumerate(AROUND):

        @pl.when(jnp.logical_not(exists(dr, dc)))
        def _():
            slot = cells.at[(1 + dr) * 3 + 1 + dc]
            slot[...] = jnp.zeros(slot.shape, BF16)
            pixels = slot_of(dr, dc)
            pixels[...] = jnp.zeros(pixels.shape, F32)

    @pl.when(earlier > 0)
    def _():
        pl.semaphore_wait(barrier, earlier)

    for k, (dr, dc) in FAR_FIRST:
        if dr <= 0:
            by = greeted_by(dr, dc)

            @pl.when(alone(by, greets(dr, dc) if dr * dc else None))
            def _():
                pl.semaphore_signal(
                    ready.at[READY[7 - k]], inc=1, device_id=device(dr, dc), device_id_type=MESH
                )

    loads[0].wait()
    for k, (dr, dc) in FAR_FIRST:
        by = greeted_by(dr, dc)
        if by is not None:

            @pl.when(by)
            def _():
                copies(k, dr, dc)[0].start()

    def send_later(entries, when=None):
        for k, (dr, dc) in entries:
            test = alone(leads(dr, dc), greeted_by(dr, dc) if dr else None)

            @pl.when(test if when is None else jnp.logical_and(test, when))
            def _():
                pl.semaphore_wait(ready.at[READY[k]], 1)
                copies(k, dr, dc)[0].start()

    below = [e for e in enumerate(AROUND) if e[1][0] > 0]
    hurry = jnp.logical_or(greeted_by(1, -1), greeted_by(1, 1))
    send_later(below, hurry)
    send_later([e for e in enumerate(AROUND) if e[1][0] == 0])

    tile = lat.shape[1]
    side_cells = tile + 2 * HALO
    margin, inner = 4 * HALO, 4 * tile
    size = inner + 2 * margin
    chans = lat.shape[0]
    span = size * side_cells
    half = span // 2
    wide = chans * side_cells

    loads[1].wait()
    load_out.start()
    wi32[...] = jnp.zeros(wi32.shape, F32)
    wi32[:, 0 : wi.shape[1], :] = wi[...].astype(F32)
    wi72 = wi32[...].reshape(72, wi32.shape[2]).astype(BF16)
    src, dst = iota((384, 72), 0), iota((384, 72), 1)
    pick = (
        (dst // 8 == 3 * (src % 128 // wide) + src // 128)
        & (dst % 8 == (src // side_cells) % chans)
        & (src % 128 < 3 * wide)
    )
    wc[...] = dot(pick.astype(F32).astype(BF16), wi72).astype(BF16)
    pltpu.make_async_copy(tables, tables, local_sem.at[2]).wait()
    pltpu.make_async_copy(limits, limits, local_sem.at[3]).wait()

    spread_r = (iota((size, span), 1) // side_cells == iota((size, span), 0)).astype(F32)
    spread_c = [
        (4 * (iota((size, span), 1) % side_cells) + q == iota((size, span), 0)).astype(F32)
        for q in range(4)
    ]
    spread_c = jnp.concatenate(spread_c, axis=1)
    row_w = dot(table_rows(tables[0].astype(F32), limits.at[0], row, nr, margin, inner), spread_r.astype(BF16))
    col_w = dot(table_rows(tables[1].astype(F32), limits.at[1], col, nc, margin, inner), spread_c.astype(BF16))
    lane = iota((1, span), 1)
    r_of, b_of = lane // side_cells, lane % side_cells
    inside = (
        (r_of >= margin) & (r_of < margin + inner) & (b_of >= HALO) & (b_of < HALO + tile)
    )
    for q in range(4):
        cw = col_w[:, q * span : (q + 1) * span]
        blend[q] = jnp.broadcast_to(row_w[0:1] * cw[0:1], (8, span))
        inverse[q] = jnp.broadcast_to(
            1.0 / jnp.where(inside, row_w[1:2] * cw[1:2], 1.0), (8, span)
        )

    send_later(below, jnp.logical_not(hurry))

    load_out.wait()
    wo32[...] = jnp.zeros(wo32.shape, F32)
    wo32[:, 0 : wo.shape[1], :] = wo[...].astype(F32)
    loads[6].wait()
    out_mid = wm.shape[1]
    for t in range(9):
        wmt[:, out_mid * t : out_mid * (t + 1)] = wm[t].T
    loads[7].wait()
    out_low = wl.shape[1]
    for t in range(9):
        wlt[:, out_low * t : out_low * (t + 1)] = wl[t].T

    for_all(lambda n, m: batch(cells, n, send1, recv1).wait_recv())

    cell = [cells[k].astype(F32) for k in range(9)]
    pieces = [[], [], []]
    for c in range(chans):
        for j, cut in enumerate((slice(tile - HALO, tile), slice(0, tile), slice(0, HALO))):
            upper, middle, lower = (cell[3 * i + j][c][:, cut] for i in range(3))
            zero = jnp.zeros((1, middle.shape[1]), F32)
            upper, lower = upper[tile - HALO :], lower[:HALO]
            pieces[0].append(jnp.concatenate([zero, upper, middle, lower[:-1]], axis=0))
            pieces[1].append(jnp.concatenate([upper, middle, lower], axis=0))
            pieces[2].append(jnp.concatenate([upper[1:], middle, lower, zero], axis=0))
    pieces = pieces[0] + pieces[1] + pieces[2]
    tall = jnp.concatenate(pieces + [jnp.zeros((side_cells, 128 - 3 * wide), F32)], axis=1)
    shape = (side_cells, side_cells, 128)
    spreaded = jnp.broadcast_to(tall[:, None, :], shape)
    gap = iota(shape, 2) % side_cells - iota(shape, 1)
    patches = [jnp.where(gap == dx - 1, spreaded, 0.0) for dx in range(3)]
    patches = jnp.concatenate(patches, axis=2).reshape(-1, 384).astype(BF16)
    first = dot(patches, wc[...]).reshape(side_cells, side_cells, -1)
    (first,) = group_silu([first])
    first = first.reshape(side_cells * side_cells, -1).astype(BF16)

    taps = dot(first, wmt[...])
    taps = [
        taps[:, out_mid * t : out_mid * (t + 1)].reshape(side_cells, side_cells, -1)
        for t in range(9)
    ]
    second = conv_up([[taps]], 1)
    second = group_silu([second[py][px] for py in range(2) for px in range(2)])
    second = jnp.concatenate(second, axis=0)
    second = second.reshape(-1, second.shape[2]).astype(BF16)

    n = side_cells * side_cells
    products = dot(second, wlt[...])
    products = [products[:, out_low * t : out_low * (t + 1)] for t in range(9)]
    taps = [
        [
            [
                p[(2 * py + px) * n : (2 * py + px + 1) * n].reshape(side_cells, side_cells, -1)
                for p in products
            ]
            for px in range(2)
        ]
        for py in range(2)
    ]
    third = conv_up(taps, 2)
    third = group_silu([third[qy][qx] for qy in range(4) for qx in range(4)])

    wo72 = wo32[...].reshape(72, wo32.shape[2]).astype(BF16)
    colour = []
    for qx in range(4):
        rows = jnp.stack([third[4 * qy + qx] for qy in range(4)], axis=1)
        colour.append(nt_dot(wo72, rows.reshape(span, rows.shape[-1]).astype(BF16)))

    def tap(q, t):
        return colour[q][8 * t : 8 * t + 8]

    where_b = iota((4, half), 1) % side_cells
    lower_half = iota((4, half), 1) < half // 2
    sub_b = iota((8, span), 1) % side_cells
    sub_r = iota((8, span), 1) // side_cells
    row_ok = [sub_r > 0, None, sub_r < size - 1]
    col_ok = [sub_b > 0, None, sub_b < side_cells - 1]

    def moved(x, dy, dx):
        shift = (side_cells * (1 - dy) + 1 - dx) % span
        x = pltpu.roll(x, shift, 1) if shift else x
        ok = [m for m in (row_ok[dy], col_ok[dx]) if m is not None]
        return jnp.where(functools.reduce(jnp.logical_and, ok), x, 0.0) if ok else x

    for q in range(4):
        value = None
        for dy in range(3):
            near = tap(q, 3 * dy + 1)
            if q > 0:
                near = near + tap(q - 1, 3 * dy)
            if q < 3:
                near = near + tap(q + 1, 3 * dy + 2)
            term = moved(near, dy, 1)
            if q == 0:
                term = term + moved(tap(3, 3 * dy), dy, 0)
            if q == 3:
                term = term + moved(tap(0, 3 * dy + 2), dy, 2)
            value = term if value is None else value + term
        value = value * blend[q]
        for h in range(2):
            own[h, q] = value[0:4, h * half : (h + 1) * half]

    for h in range(2):
        for k, rim in ((0, 0), (1, side_cells - HALO)):
            dense = pltpu.roll(own[h, 0], (half - rim) % half, 1)
            for q in range(1, 4):
                turned = pltpu.roll(own[h, q], (HALO * q - rim) % half, 1)
                dense = jnp.where(where_b // HALO == q, turned, dense)
            side_out[k, h] = dense
        for pair in range(2):
            even, odds = own[h, 2 * pair], own[h, 2 * pair + 1]
            if h == 0:
                odds = pltpu.roll(odds, half // 2, 1)
            else:
                even = pltpu.roll(even, half // 2, 1)
            vert_out[h, pair] = jnp.where(lower_half, even, odds)

    for k, (dr, dc) in FAR_FIRST:

        @pl.when(exists(dr, dc))
        def _():
            copies(k, dr, dc)[1].start()

    lane_row = iota((8, half), 1) // side_cells
    sublane = iota((8, half), 0)
    keep = [lane_row == sublane + 8, lane_row == sublane]
    beyond_row = [lane_row % 8 == sublane, lane_row % 8 == sublane]

    def spread_rows(piece, c, mask):
        return jnp.where(mask, jnp.broadcast_to(piece[c : c + 1], (8, half)), 0.0)

    def placed(blocks, place):
        tall = jnp.concatenate(blocks, axis=0)
        top = tall.astype(BF16)
        low = (tall - top.astype(F32)).astype(BF16)
        got = dot(jnp.concatenate([top, low], axis=0), place)
        return got[: tall.shape[0]] + got[tall.shape[0] :]

    place_src, place_dst = iota((4 * half, inner), 0), iota((4 * half, inner), 1)
    place = place_dst == 4 * (place_src % side_cells - HALO) + place_src // half
    place = place.astype(F32).astype(BF16)
    blocks = []
    for c in range(3):
        for h in range(2):
            mine = [own[h, q] * inverse[q, 0:4, h * half : (h + 1) * half] for q in range(4)]
            blocks.append(jnp.concatenate([spread_rows(p, c, keep[h]) for p in mine], axis=1))
    mine = placed(blocks, place)

    slot = place_src % side_cells
    from_left = place_dst == 4 * (slot % HALO) + slot // HALO
    from_right = place_dst == 4 * (tile - HALO + slot % HALO) + slot // HALO
    pair_q = 2 * (place_src // half - 2) + place_src % half // (half // 2)
    from_pair = place_dst == 4 * (slot - HALO) + pair_q
    part = place_src // half
    rim_place = jnp.where(
        part == 0, from_left.astype(F32), jnp.where(part == 1, from_right.astype(F32), from_pair.astype(F32))
    ).astype(BF16)
    scales = []
    for h in range(2):
        here = [inverse[q, 0:4, h * half : (h + 1) * half] for q in range(4)]
        sides = []
        for rim in (HALO, tile):
            dense = pltpu.roll(here[0], (half - rim) % half, 1)
            for q in range(1, 4):
                turned = pltpu.roll(here[q], (HALO * q - rim) % half, 1)
                dense = jnp.where(where_b // HALO == q, turned, dense)
            sides.append(dense)
        for pair in range(2):
            even, odds = here[2 * pair], here[2 * pair + 1]
            if h == 0:
                even = pltpu.roll(even, half // 2, 1)
            else:
                odds = pltpu.roll(odds, half // 2, 1)
            sides.append(jnp.where(lower_half, even, odds))
        scales.append(sides)

    for_all(lambda n, m: batch(cells, n, send1, recv1).wait_send())
    for_all(lambda n, m: batch(rims, m, send2, recv2).wait_recv())

    blocks = []
    for c in range(3):
        for h in range(2):
            got = [
                (rims[h] + rims[4 + h]) * scales[h][0],
                (rims[2 + h] + rims[6 + h]) * scales[h][1],
                rims[8 + 2 * h] * scales[h][2],
                rims[9 + 2 * h] * scales[h][3],
            ]
            masks = [keep[h], keep[h], beyond_row[h], beyond_row[h]]
            blocks.append(
                jnp.concatenate([spread_rows(p, c, m) for p, m in zip(got, masks)], axis=1)
            )
    out[...] = (mine + placed(blocks, rim_place)).reshape(3, inner, inner)

    for_all(lambda n, m: batch(rims, m, send2, recv2).wait_send())


def solution(mesh):
    nr, nc = mesh.shape["rows"], mesh.shape["cols"]

    def per_device(lat, w_in, w_mid, w_low, w_out, ramp_r, ramp_c, lim_r, lim_c):
        tile = lat.shape[1]
        inner = 4 * tile
        size = inner + 8 * HALO
        half = size * (tile + 2 * HALO) // 2
        anywhere = pl.BlockSpec(memory_space=pltpu.HBM)
        dma = pltpu.SemaphoreType.DMA
        return pl.pallas_call(
            functools.partial(kernel, nr, nc),
            out_shape=pltpu.VMEM((w_out.shape[1], inner, inner), F32),
            in_specs=[anywhere] * 9,
            out_specs=pl.BlockSpec(memory_space=pltpu.VMEM),
            scratch_shapes=[
                pltpu.VMEM((9,) + lat.shape, BF16),
                pltpu.VMEM(w_in.shape, BF16),
                pltpu.VMEM(w_mid.shape, BF16),
                pltpu.VMEM(w_low.shape, BF16),
                pltpu.VMEM(w_out.shape, BF16),
                pltpu.VMEM((2,) + ramp_r.shape, jnp.int32),
                pltpu.SMEM((2,) + lim_r.shape, jnp.int32),
                pltpu.VMEM((9, 8, w_in.shape[2]), F32),
                pltpu.VMEM((9, 8, w_out.shape[2]), F32),
                pltpu.VMEM((384, w_in.shape[2]), BF16),
                pltpu.VMEM((w_mid.shape[2], 9 * w_mid.shape[1]), BF16),
                pltpu.VMEM((w_low.shape[2], 9 * w_low.shape[1]), BF16),
                pltpu.VMEM((4, 8, 2 * half), F32),
                pltpu.VMEM((4, 8, 2 * half), F32),
                pltpu.VMEM((2, 4, 4, half), F32),
                pltpu.VMEM((2, 2, 4, half), F32),
                pltpu.VMEM((2, 2, 4, half), F32),
                pltpu.VMEM((12, 4, half), F32),
                dma((6,)),
                pltpu.SemaphoreType.REGULAR((5,)),
                dma,
                dma,
            ],
            compiler_params=pltpu.CompilerParams(
                collective_id=0, has_side_effects=True
            ),
            name="decode",
        )(lat, w_in, w_mid, w_low, w_out, ramp_r, ramp_c, lim_r, lim_c)

    return jax.shard_map(
        per_device,
        mesh=mesh,
        in_specs=(P(None, ("groups", "rows"), "cols"), P(), P(), P(), P(), P(), P(), P(), P()),
        out_specs=P(None, ("groups", "rows"), "cols"),
        check_vma=False,
    )
```

```python
import functools

import jax
import jax.numpy as jnp
from jax import lax
from jax.experimental import pallas as pl
from jax.experimental.pallas import tpu as pltpu
from jax.sharding import PartitionSpec as P

MESH = pl.DeviceIdType.MESH
NGROUPS = 32
HALO = 2
F32 = jnp.float32
BF16 = jnp.bfloat16
AROUND = [(dr, dc) for dr in (-1, 0, 1) for dc in (-1, 0, 1) if (dr, dc) != (0, 0)]
FAR_FIRST = sorted(enumerate(AROUND), key=lambda e: -abs(e[1][0]) - abs(e[1][1]))
READY = {k: n for n, k in enumerate((3, 4, 5, 6, 7))}


def iota(shape, dim):
    return lax.broadcasted_iota(jnp.int32, shape, dim)


def nt_dot(a, b):
    return lax.dot_general(a, b, (((1,), (1,)), ((), ())), preferred_element_type=F32)


def dot(a, b):
    return jnp.dot(a, b, preferred_element_type=F32)


def down(x):
    return jnp.concatenate([jnp.zeros_like(x[:1]), x[:-1]], axis=0)


def up(x):
    return jnp.concatenate([x[1:], jnp.zeros_like(x[:1])], axis=0)


def right(x):
    rolled = pltpu.roll(x, 1, 1)
    return jnp.where(iota(x.shape, 1) == 0, 0.0, rolled)


def left(x):
    n = x.shape[1]
    rolled = pltpu.roll(x, n - 1, 1)
    return jnp.where(iota(x.shape, 1) == n - 1, 0.0, rolled)


def expand(products, fine, before, after):
    out = []
    for q in range(fine):
        t0, t1, t2 = products[q]
        prev = products[q - 1][0] if q > 0 else before(products[fine - 1][0])
        nxt = products[q + 1][2] if q < fine - 1 else after(products[0][2])
        out.append(prev + (t1 + t2))
        out.append((t0 + t1) + nxt)
    return out


def conv_up(taps, fine):
    by_col = [
        [
            expand(
                [[taps[py][px][3 * dy + dx] for dy in range(3)] for py in range(fine)],
                fine,
                down,
                up,
            )
            for dx in range(3)
        ]
        for px in range(fine)
    ]
    return [
        expand(
            [[by_col[px][dx][qy] for dx in range(3)] for px in range(fine)],
            fine,
            right,
            left,
        )
        for qy in range(2 * fine)
    ]


def group_sum(x, width):
    lane = iota(x.shape, 1) % width
    parts = [x]
    for k in range(1, width):
        parts.append(jnp.where(lane >= k, pltpu.roll(x, k, 1), 0.0))
        parts.append(jnp.where(lane < width - k, pltpu.roll(x, x.shape[1] - k, 1), 0.0))
    while len(parts) > 1:
        parts = [functools.reduce(jnp.add, parts[k : k + 2]) for k in range(0, len(parts), 2)]
    return parts[0]


def group_silu(phases):
    channels = phases[0].shape[-1]
    width = channels // NGROUPS
    count = channels // 128
    positions = len(phases) * phases[0].shape[0] * phases[0].shape[1]
    scale = 1.0 / (positions * width)
    total = jnp.sum(functools.reduce(jnp.add, phases), axis=(0, 1)).reshape(1, channels)
    squares = functools.reduce(jnp.add, [p * p for p in phases])
    squares = jnp.sum(squares, axis=(0, 1)).reshape(1, channels)
    rows = [x[:, k * 128 : (k + 1) * 128] for x in (total, squares) for k in range(count)]
    rows = jnp.concatenate(rows + [jnp.zeros((1, 128), F32)] * (8 - len(rows)), axis=0)
    got = group_sum(rows, width) * scale
    center = got[:count]
    spread = jnp.maximum(got[count : 2 * count] - center * center, 0.0)
    factor = 0.5 * lax.rsqrt(spread + 1e-06)
    offset = center * factor
    factor = jnp.concatenate([factor[k : k + 1] for k in range(count)], axis=1)[None]
    offset = jnp.concatenate([offset[k : k + 1] for k in range(count)], axis=1)[None]
    result = []
    for p in phases:
        half = p * factor - offset
        result.append(half + half * jnp.tanh(half))
    return result


def table_rows(table, limits, index, count, margin, inner):
    size = table.shape[1]
    pos = iota((1, size), 1)
    far = jnp.maximum(jnp.maximum(margin - pos, pos - (margin + inner) + 1), 0)
    rows = []
    for d in (-1, 0, 1):
        here = index + d
        limit = limits[jnp.clip(here, 0, count - 1)]
        picked = jnp.where(iota(table.shape, 0) == here, table, 0.0)
        row = jnp.sum(picked, axis=0, keepdims=True)
        rows.append(jnp.where(far <= limit, row, 0.0))
    above, own, below = rows
    other = jnp.where(pos < inner, jnp.roll(above, inner, 1), jnp.roll(below, inner, 1))
    pair = jnp.concatenate([own, own + other, jnp.zeros((6, size), F32)], axis=0)
    return pair.astype(BF16)


def kernel(
    nr, nc, lat, w_in, w_mid, w_low, w_out, ramp_r, ramp_c, lim_r, lim_c, out,
    cells, wi, wm, wl, wo, tables, limits, wi32, wo32, wc, wmt, wlt,
    blend, inverse, own, side_out, vert_out, rims,
    local_sem, ready, recv1, recv2,
):
    row, col = lax.axis_index("rows"), lax.axis_index("cols")

    def exists(dr, dc):
        ok = None
        for d, here, n in ((dr, row, nr), (dc, col, nc)):
            test = None if d == 0 else (here > 0 if d < 0 else here < n - 1)
            if test is not None:
                ok = test if ok is None else jnp.logical_and(ok, test)
        return ok

    def device(dr, dc):
        return {"rows": row + dr, "cols": col + dc}

    loads = [
        pltpu.make_async_copy(src, dst, local_sem.at[k])
        for k, src, dst in [
            (0, lat, cells.at[4]),
            (1, w_in, wi),
            (2, ramp_r, tables.at[0]),
            (2, ramp_c, tables.at[1]),
            (3, lim_r, limits.at[0]),
            (3, lim_c, limits.at[1]),
            (4, w_mid, wm),
            (5, w_low, wl),
        ]
    ]
    load_out = pltpu.make_async_copy(w_out, wo, local_sem.at[1])
    send1, send2 = local_sem.at[0], local_sem.at[1]
    for load in loads:
        load.start()

    odd = col % 2 == 1

    def mutual(dr, dc):
        return jnp.logical_and(row == (0 if dr > 0 else 1), odd if dc > 0 else jnp.logical_not(odd))

    def leads(dr, dc):
        there = exists(dr, dc)
        return there if dr > 0 else jnp.logical_and(there, odd)

    def greets(dr, dc):
        there = exists(dr, dc)
        if dr < 0:
            return jnp.logical_and(there, mutual(dr, dc)) if dc else None
        return leads(dr, dc)

    def greeted_by(dr, dc):
        there = exists(dr, dc)
        if dr > 0:
            return jnp.logical_and(there, mutual(dr, dc)) if dc else None
        return there if dr < 0 else jnp.logical_and(there, jnp.logical_not(odd))

    def alone(test, other):
        return test if other is None else jnp.logical_and(test, jnp.logical_not(other))

    barrier = pltpu.get_barrier_semaphore()
    earlier = 0
    for dr, dc in AROUND:
        test = greets(dr, dc)
        if test is not None:

            @pl.when(test)
            def _():
                pl.semaphore_signal(barrier, inc=1, device_id=device(dr, dc), device_id_type=MESH)

    for dr, dc in AROUND:
        test = greeted_by(dr, dc)
        if test is not None:
            earlier += test.astype(jnp.int32)

    def slot_of(dr, dc):
        up_down, left_right = (dr + 1) // 2, (dc + 1) // 2
        if dr == 0:
            return rims.at[pl.ds(2 * left_right, 2)]
        if dc == 0:
            return rims.at[pl.ds(8 + 2 * up_down, 2)]
        return rims.at[4 + 2 * left_right + up_down]

    def packed(dr, dc):
        up_down, left_right = (dr + 1) // 2, (dc + 1) // 2
        if dr == 0:
            return side_out.at[left_right]
        return vert_out.at[up_down] if dc == 0 else side_out.at[left_right, up_down]

    def copies(k, dr, dc):
        first = pltpu.make_async_remote_copy(
            src_ref=cells.at[4],
            dst_ref=cells.at[(1 - dr) * 3 + 1 - dc],
            send_sem=send1,
            recv_sem=recv1,
            device_id=device(dr, dc),
            device_id_type=MESH,
        )
        second = pltpu.make_async_remote_copy(
            src_ref=packed(dr, dc),
            dst_ref=slot_of(-dr, -dc),
            send_sem=send2,
            recv_sem=recv2,
            device_id=device(dr, dc),
            device_id_type=MESH,
        )
        return first, second

    above_below = (row > 0).astype(jnp.int32) + (row < nr - 1).astype(jnp.int32)
    beside = (col > 0).astype(jnp.int32) + (col < nc - 1).astype(jnp.int32)

    def for_all(wait):
        for v in range(min(nr, 2) - 1, min(nr, 3)):
            for h in range(min(nc, 2) - 1, min(nc, 3)):
                if v + h == 0:
                    continue

                @pl.when(jnp.logical_and(above_below == v, beside == h))
                def _():
                    wait(v + h + v * h, 2 * (v + h) + v * h)

    def batch(ref, n, send, recv):
        part = ref.at[pl.ds(0, n)]
        return pltpu.make_async_remote_copy(
            src_ref=part,
            dst_ref=part,
            send_sem=send,
            recv_sem=recv,
            device_id=device(0, 0),
            device_id_type=MESH,
        )

    for k, (dr, dc) in enumerate(AROUND):

        @pl.when(jnp.logical_not(exists(dr, dc)))
        def _():
            slot = cells.at[(1 + dr) * 3 + 1 + dc]
            slot[...] = jnp.zeros(slot.shape, BF16)
            pixels = slot_of(dr, dc)
            pixels[...] = jnp.zeros(pixels.shape, F32)

    @pl.when(earlier > 0)
    def _():
        pl.semaphore_wait(barrier, earlier)

    for k, (dr, dc) in FAR_FIRST:
        if dr <= 0:
            by = greeted_by(dr, dc)

            @pl.when(alone(by, greets(dr, dc) if dr * dc else None))
            def _():
                pl.semaphore_signal(
                    ready.at[READY[7 - k]], inc=1, device_id=device(dr, dc), device_id_type=MESH
                )

    loads[0].wait()
    for k, (dr, dc) in FAR_FIRST:
        by = greeted_by(dr, dc)
        if by is not None:

            @pl.when(by)
            def _():
                copies(k, dr, dc)[0].start()

    def send_later(entries, when=None):
        for k, (dr, dc) in entries:
            test = alone(leads(dr, dc), greeted_by(dr, dc) if dr else None)

            @pl.when(test if when is None else jnp.logical_and(test, when))
            def _():
                pl.semaphore_wait(ready.at[READY[k]], 1)
                copies(k, dr, dc)[0].start()

    below = [e for e in enumerate(AROUND) if e[1][0] > 0]
    hurry = jnp.logical_or(greeted_by(1, -1), greeted_by(1, 1))
    send_later(below, hurry)
    send_later([e for e in enumerate(AROUND) if e[1][0] == 0])

    tile = lat.shape[1]
    side_cells = tile + 2 * HALO
    margin, inner = 4 * HALO, 4 * tile
    size = inner + 2 * margin
    chans = lat.shape[0]
    span = size * side_cells
    half = span // 2
    wide = chans * side_cells

    loads[1].wait()
    load_out.start()
    wi32[...] = jnp.zeros(wi32.shape, F32)
    wi32[:, 0 : wi.shape[1], :] = wi[...].astype(F32)
    wi72 = wi32[...].reshape(72, wi32.shape[2]).astype(BF16)
    src, dst = iota((384, 72), 0), iota((384, 72), 1)
    pick = (
        (dst // 8 == 3 * (src % 128 // wide) + src // 128)
        & (dst % 8 == (src // side_cells) % chans)
        & (src % 128 < 3 * wide)
    )
    wc[...] = dot(pick.astype(F32).astype(BF16), wi72).astype(BF16)
    pltpu.make_async_copy(tables, tables, local_sem.at[2]).wait()
    pltpu.make_async_copy(limits, limits, local_sem.at[3]).wait()

    spread_r = (iota((size, span), 1) // side_cells == iota((size, span), 0)).astype(F32)
    spread_c = [
        (4 * (iota((size, span), 1) % side_cells) + q == iota((size, span), 0)).astype(F32)
        for q in range(4)
    ]
    spread_c = jnp.concatenate(spread_c, axis=1)
    row_w = dot(table_rows(tables[0].astype(F32), limits.at[0], row, nr, margin, inner), spread_r.astype(BF16))
    col_w = dot(table_rows(tables[1].astype(F32), limits.at[1], col, nc, margin, inner), spread_c.astype(BF16))
    lane = iota((1, span), 1)
    r_of, b_of = lane // side_cells, lane % side_cells
    inside = (
        (r_of >= margin) & (r_of < margin + inner) & (b_of >= HALO) & (b_of < HALO + tile)
    )
    for q in range(4):
        cw = col_w[:, q * span : (q + 1) * span]
        blend[q] = jnp.broadcast_to(row_w[0:1] * cw[0:1], (8, span))
        inverse[q] = jnp.broadcast_to(
            1.0 / jnp.where(inside, row_w[1:2] * cw[1:2], 1.0), (8, span)
        )

    send_later(below, jnp.logical_not(hurry))

    load_out.wait()
    wo32[...] = jnp.zeros(wo32.shape, F32)
    wo32[:, 0 : wo.shape[1], :] = wo[...].astype(F32)
    loads[6].wait()
    out_mid = wm.shape[1]
    for t in range(9):
        wmt[:, out_mid * t : out_mid * (t + 1)] = wm[t].T
    loads[7].wait()
    out_low = wl.shape[1]
    for t in range(9):
        wlt[:, out_low * t : out_low * (t + 1)] = wl[t].T

    for_all(lambda n, m: batch(cells, n, send1, recv1).wait_recv())

    cell = [cells[k].astype(F32) for k in range(9)]
    pieces = [[], [], []]
    for c in range(chans):
        for j, cut in enumerate((slice(tile - HALO, tile), slice(0, tile), slice(0, HALO))):
            upper, middle, lower = (cell[3 * i + j][c][:, cut] for i in range(3))
            zero = jnp.zeros((1, middle.shape[1]), F32)
            upper, lower = upper[tile - HALO :], lower[:HALO]
            pieces[0].append(jnp.concatenate([zero, upper, middle, lower[:-1]], axis=0))
            pieces[1].append(jnp.concatenate([upper, middle, lower], axis=0))
            pieces[2].append(jnp.concatenate([upper[1:], middle, lower, zero], axis=0))
    pieces = pieces[0] + pieces[1] + pieces[2]
    tall = jnp.concatenate(pieces + [jnp.zeros((side_cells, 128 - 3 * wide), F32)], axis=1)
    shape = (side_cells, side_cells, 128)
    spreaded = jnp.broadcast_to(tall[:, None, :], shape)
    gap = iota(shape, 2) % side_cells - iota(shape, 1)
    patches = [jnp.where(gap == dx - 1, spreaded, 0.0) for dx in range(3)]
    patches = jnp.concatenate(patches, axis=2).reshape(-1, 384).astype(BF16)
    first = dot(patches, wc[...]).reshape(side_cells, side_cells, -1)
    (first,) = group_silu([first])
    first = first.reshape(side_cells * side_cells, -1).astype(BF16)

    taps = dot(first, wmt[...])
    taps = [
        taps[:, out_mid * t : out_mid * (t + 1)].reshape(side_cells, side_cells, -1)
        for t in range(9)
    ]
    second = conv_up([[taps]], 1)
    second = group_silu([second[py][px] for py in range(2) for px in range(2)])
    second = jnp.concatenate(second, axis=0)
    second = second.reshape(-1, second.shape[2]).astype(BF16)

    n = side_cells * side_cells
    products = dot(second, wlt[...])
    products = [products[:, out_low * t : out_low * (t + 1)] for t in range(9)]
    taps = [
        [
            [
                p[(2 * py + px) * n : (2 * py + px + 1) * n].reshape(side_cells, side_cells, -1)
                for p in products
            ]
            for px in range(2)
        ]
        for py in range(2)
    ]
    third = conv_up(taps, 2)
    third = group_silu([third[qy][qx] for qy in range(4) for qx in range(4)])

    wo72 = wo32[...].reshape(72, wo32.shape[2]).astype(BF16)
    colour = []
    for qx in range(4):
        rows = jnp.stack([third[4 * qy + qx] for qy in range(4)], axis=1)
        colour.append(nt_dot(wo72, rows.reshape(span, rows.shape[-1]).astype(BF16)))

    def tap(q, t):
        return colour[q][8 * t : 8 * t + 8]

    where_b = iota((4, half), 1) % side_cells
    lower_half = iota((4, half), 1) < half // 2
    sub_b = iota((8, span), 1) % side_cells
    sub_r = iota((8, span), 1) // side_cells
    row_ok = [sub_r > 0, None, sub_r < size - 1]
    col_ok = [sub_b > 0, None, sub_b < side_cells - 1]

    def moved(x, dy, dx):
        shift = (side_cells * (1 - dy) + 1 - dx) % span
        x = pltpu.roll(x, shift, 1) if shift else x
        ok = [m for m in (row_ok[dy], col_ok[dx]) if m is not None]
        return jnp.where(functools.reduce(jnp.logical_and, ok), x, 0.0) if ok else x

    for q in range(4):
        value = None
        for dy in range(3):
            near = tap(q, 3 * dy + 1)
            if q > 0:
                near = near + tap(q - 1, 3 * dy)
            if q < 3:
                near = near + tap(q + 1, 3 * dy + 2)
            term = moved(near, dy, 1)
            if q == 0:
                term = term + moved(tap(3, 3 * dy), dy, 0)
            if q == 3:
                term = term + moved(tap(0, 3 * dy + 2), dy, 2)
            value = term if value is None else value + term
        value = value * blend[q]
        for h in range(2):
            own[h, q] = value[0:4, h * half : (h + 1) * half]

    for h in range(2):
        for k, rim in ((0, 0), (1, side_cells - HALO)):
            dense = pltpu.roll(own[h, 0], (half - rim) % half, 1)
            for q in range(1, 4):
                turned = pltpu.roll(own[h, q], (HALO * q - rim) % half, 1)
                dense = jnp.where(where_b // HALO == q, turned, dense)
            side_out[k, h] = dense
        for pair in range(2):
            even, odds = own[h, 2 * pair], own[h, 2 * pair + 1]
            if h == 0:
                odds = pltpu.roll(odds, half // 2, 1)
            else:
                even = pltpu.roll(even, half // 2, 1)
            vert_out[h, pair] = jnp.where(lower_half, even, odds)

    for k, (dr, dc) in FAR_FIRST:

        @pl.when(exists(dr, dc))
        def _():
            copies(k, dr, dc)[1].start()

    lane_row = iota((8, half), 1) // side_cells
    sublane = iota((8, half), 0)
    keep = [lane_row == sublane + 8, lane_row == sublane]
    beyond_row = [lane_row % 8 == sublane, lane_row % 8 == sublane]

    def spread_rows(piece, c, mask):
        return jnp.where(mask, jnp.broadcast_to(piece[c : c + 1], (8, half)), 0.0)

    def placed(blocks, place):
        tall = jnp.concatenate(blocks, axis=0)
        top = tall.astype(BF16)
        low = (tall - top.astype(F32)).astype(BF16)
        got = dot(jnp.concatenate([top, low], axis=0), place)
        return got[: tall.shape[0]] + got[tall.shape[0] :]

    place_src, place_dst = iota((4 * half, inner), 0), iota((4 * half, inner), 1)
    place = place_dst == 4 * (place_src % side_cells - HALO) + place_src // half
    place = place.astype(F32).astype(BF16)
    blocks = []
    for c in range(3):
        for h in range(2):
            mine = [own[h, q] * inverse[q, 0:4, h * half : (h + 1) * half] for q in range(4)]
            blocks.append(jnp.concatenate([spread_rows(p, c, keep[h]) for p in mine], axis=1))
    mine = placed(blocks, place)

    slot = place_src % side_cells
    from_left = place_dst == 4 * (slot % HALO) + slot // HALO
    from_right = place_dst == 4 * (tile - HALO + slot % HALO) + slot // HALO
    pair_q = 2 * (place_src // half - 2) + place_src % half // (half // 2)
    from_pair = place_dst == 4 * (slot - HALO) + pair_q
    part = place_src // half
    rim_place = jnp.where(
        part == 0, from_left.astype(F32), jnp.where(part == 1, from_right.astype(F32), from_pair.astype(F32))
    ).astype(BF16)
    scales = []
    for h in range(2):
        here = [inverse[q, 0:4, h * half : (h + 1) * half] for q in range(4)]
        sides = []
        for rim in (HALO, tile):
            dense = pltpu.roll(here[0], (half - rim) % half, 1)
            for q in range(1, 4):
                turned = pltpu.roll(here[q], (HALO * q - rim) % half, 1)
                dense = jnp.where(where_b // HALO == q, turned, dense)
            sides.append(dense)
        for pair in range(2):
            even, odds = here[2 * pair], here[2 * pair + 1]
            if h == 0:
                even = pltpu.roll(even, half // 2, 1)
            else:
                odds = pltpu.roll(odds, half // 2, 1)
            sides.append(jnp.where(lower_half, even, odds))
        scales.append(sides)

    for_all(lambda n, m: batch(cells, n, send1, recv1).wait_send())
    for_all(lambda n, m: batch(rims, m, send2, recv2).wait_recv())

    blocks = []
    for c in range(3):
        for h in range(2):
            got = [
                (rims[h] + rims[4 + h]) * scales[h][0],
                (rims[2 + h] + rims[6 + h]) * scales[h][1],
                rims[8 + 2 * h] * scales[h][2],
                rims[9 + 2 * h] * scales[h][3],
            ]
            masks = [keep[h], keep[h], beyond_row[h], beyond_row[h]]
            blocks.append(
                jnp.concatenate([spread_rows(p, c, m) for p, m in zip(got, masks)], axis=1)
            )
    out[...] = (mine + placed(blocks, rim_place)).reshape(3, inner, inner)

    for_all(lambda n, m: batch(rims, m, send2, recv2).wait_send())


def solution(mesh):
    nr, nc = mesh.shape["rows"], mesh.shape["cols"]

    def per_device(lat, w_in, w_mid, w_low, w_out, ramp_r, ramp_c, lim_r, lim_c):
        tile = lat.shape[1]
        inner = 4 * tile
        size = inner + 8 * HALO
        half = size * (tile + 2 * HALO) // 2
        anywhere = pl.BlockSpec(memory_space=pltpu.HBM)
        dma = pltpu.SemaphoreType.DMA
        return pl.pallas_call(
            functools.partial(kernel, nr, nc),
            out_shape=pltpu.VMEM((w_out.shape[1], inner, inner), F32),
            in_specs=[anywhere] * 9,
            out_specs=pl.BlockSpec(memory_space=pltpu.VMEM),
            scratch_shapes=[
                pltpu.VMEM((9,) + lat.shape, BF16),
                pltpu.VMEM(w_in.shape, BF16),
                pltpu.VMEM(w_mid.shape, BF16),
                pltpu.VMEM(w_low.shape, BF16),
                pltpu.VMEM(w_out.shape, BF16),
                pltpu.VMEM((2,) + ramp_r.shape, jnp.int32),
                pltpu.SMEM((2,) + lim_r.shape, jnp.int32),
                pltpu.VMEM((9, 8, w_in.shape[2]), F32),
                pltpu.VMEM((9, 8, w_out.shape[2]), F32),
                pltpu.VMEM((384, w_in.shape[2]), BF16),
                pltpu.VMEM((w_mid.shape[2], 9 * w_mid.shape[1]), BF16),
                pltpu.VMEM((w_low.shape[2], 9 * w_low.shape[1]), BF16),
                pltpu.VMEM((4, 8, 2 * half), F32),
                pltpu.VMEM((4, 8, 2 * half), F32),
                pltpu.VMEM((2, 4, 4, half), F32),
                pltpu.VMEM((2, 2, 4, half), F32),
                pltpu.VMEM((2, 2, 4, half), F32),
                pltpu.VMEM((12, 4, half), F32),
                dma((6,)),
                pltpu.SemaphoreType.REGULAR((5,)),
                dma,
                dma,
            ],
            compiler_params=pltpu.CompilerParams(
                collective_id=0, has_side_effects=True
            ),
            name="decode",
        )(lat, w_in, w_mid, w_low, w_out, ramp_r, ramp_c, lim_r, lim_c)

    return jax.shard_map(
        per_device,
        mesh=mesh,
        in_specs=(P(None, ("groups", "rows"), "cols"), P(), P(), P(), P(), P(), P(), P(), P()),
        out_specs=P(None, ("groups", "rows"), "cols"),
        check_vma=False,
    )
```

```python
import functools

import jax
import jax.numpy as jnp
from jax import lax
from jax.experimental import pallas as pl
from jax.experimental.pallas import tpu as pltpu
from jax.sharding import PartitionSpec as P

MESH = pl.DeviceIdType.MESH
NGROUPS = 32
HALO = 2
F32 = jnp.float32
BF16 = jnp.bfloat16
AROUND = [(dr, dc) for dr in (-1, 0, 1) for dc in (-1, 0, 1) if (dr, dc) != (0, 0)]
FAR_FIRST = sorted(enumerate(AROUND), key=lambda e: -abs(e[1][0]) - abs(e[1][1]))
BY_COLUMN = [3 * (t % 3) + t // 3 for t in range(9)]
READY = {k: n for n, k in enumerate((3, 4, 5, 6, 7))}


def iota(shape, dim):
    return lax.broadcasted_iota(jnp.int32, shape, dim)


def nt_dot(a, b):
    return lax.dot_general(a, b, (((1,), (1,)), ((), ())), preferred_element_type=F32)


def dot(a, b):
    return jnp.dot(a, b, preferred_element_type=F32)


def down(x):
    return jnp.concatenate([jnp.zeros_like(x[:1]), x[:-1]], axis=0)


def up(x):
    return jnp.concatenate([x[1:], jnp.zeros_like(x[:1])], axis=0)


def right(x):
    rolled = pltpu.roll(x, 1, 1)
    return jnp.where(iota(x.shape, 1) == 0, 0.0, rolled)


def left(x):
    n = x.shape[1]
    rolled = pltpu.roll(x, n - 1, 1)
    return jnp.where(iota(x.shape, 1) == n - 1, 0.0, rolled)


def expand(products, fine, before, after):
    out = []
    for q in range(fine):
        t0, t1, t2 = products[q]
        prev = products[q - 1][0] if q > 0 else before(products[fine - 1][0])
        nxt = products[q + 1][2] if q < fine - 1 else after(products[0][2])
        out.append(prev + (t1 + t2))
        out.append((t0 + t1) + nxt)
    return out


def conv_up(taps, fine):
    by_col = [
        [
            expand(
                [[taps[py][px][3 * dy + dx] for dy in range(3)] for py in range(fine)],
                fine,
                down,
                up,
            )
            for dx in range(3)
        ]
        for px in range(fine)
    ]
    return [
        expand(
            [[by_col[px][dx][qy] for dx in range(3)] for px in range(fine)],
            fine,
            right,
            left,
        )
        for qy in range(2 * fine)
    ]


def group_sum(x, width):
    lane = iota(x.shape, 1) % width
    parts = [x]
    for k in range(1, width):
        parts.append(jnp.where(lane >= k, pltpu.roll(x, k, 1), 0.0))
        parts.append(jnp.where(lane < width - k, pltpu.roll(x, x.shape[1] - k, 1), 0.0))
    while len(parts) > 1:
        parts = [functools.reduce(jnp.add, parts[k : k + 2]) for k in range(0, len(parts), 2)]
    return parts[0]


def group_silu(phases):
    channels = phases[0].shape[-1]
    width = channels // NGROUPS
    count = channels // 128
    positions = len(phases) * phases[0].shape[0] * phases[0].shape[1]
    scale = 1.0 / (positions * width)
    total = jnp.sum(functools.reduce(jnp.add, phases), axis=(0, 1)).reshape(1, channels)
    squares = functools.reduce(jnp.add, [p * p for p in phases])
    squares = jnp.sum(squares, axis=(0, 1)).reshape(1, channels)
    rows = [x[:, k * 128 : (k + 1) * 128] for x in (total, squares) for k in range(count)]
    rows = jnp.concatenate(rows + [jnp.zeros((1, 128), F32)] * (8 - len(rows)), axis=0)
    got = group_sum(rows, width) * scale
    center = got[:count]
    spread = jnp.maximum(got[count : 2 * count] - center * center, 0.0)
    factor = 0.5 * lax.rsqrt(spread + 1e-06)
    offset = center * factor
    factor = jnp.concatenate([factor[k : k + 1] for k in range(count)], axis=1)[None]
    offset = jnp.concatenate([offset[k : k + 1] for k in range(count)], axis=1)[None]
    result = []
    for p in phases:
        half = p * factor - offset
        result.append(half + half * jnp.tanh(half))
    return result


def table_rows(table, limits, index, count, margin, inner):
    size = table.shape[1]
    pos = iota((1, size), 1)
    far = jnp.maximum(jnp.maximum(margin - pos, pos - (margin + inner) + 1), 0)
    rows = []
    for d in (-1, 0, 1):
        here = index + d
        limit = limits[jnp.clip(here, 0, count - 1)]
        picked = jnp.where(iota(table.shape, 0) == here, table, 0.0)
        row = jnp.sum(picked, axis=0, keepdims=True)
        rows.append(jnp.where(far <= limit, row, 0.0))
    above, own, below = rows
    other = jnp.where(pos < inner, jnp.roll(above, inner, 1), jnp.roll(below, inner, 1))
    pair = jnp.concatenate([own, own + other, jnp.zeros((6, size), F32)], axis=0)
    return pair.astype(BF16)


def kernel(
    nr, nc, lat, w_in, w_mid, w_low, w_out, ramp_r, ramp_c, lim_r, lim_c, out,
    cells, wi, wm, wl, wo, tables, limits, wi32, wo32, wc, wmt, wlt,
    blend, inverse, places, scales, own, side_out, vert_out, rims,
    local_sem, ready, recv1, recv2,
):
    row, col = lax.axis_index("rows"), lax.axis_index("cols")

    def exists(dr, dc):
        ok = None
        for d, here, n in ((dr, row, nr), (dc, col, nc)):
            test = None if d == 0 else (here > 0 if d < 0 else here < n - 1)
            if test is not None:
                ok = test if ok is None else jnp.logical_and(ok, test)
        return ok

    def device(dr, dc):
        return {"rows": row + dr, "cols": col + dc}

    loads = [
        pltpu.make_async_copy(src, dst, local_sem.at[k])
        for k, src, dst in [
            (0, lat, cells.at[4]),
            (1, w_in, wi),
            (2, ramp_r, tables.at[0]),
            (2, ramp_c, tables.at[1]),
            (3, lim_r, limits.at[0]),
            (3, lim_c, limits.at[1]),
            (4, w_mid, wm),
            (5, w_low, wl),
        ]
    ]
    load_out = pltpu.make_async_copy(w_out, wo, local_sem.at[1])
    send1, send2 = local_sem.at[0], local_sem.at[1]
    for load in loads:
        load.start()

    odd = col % 2 == 1

    def mutual(dr, dc):
        return jnp.logical_and(row == (0 if dr > 0 else 1), odd if dc > 0 else jnp.logical_not(odd))

    def leads(dr, dc):
        there = exists(dr, dc)
        return there if dr > 0 else jnp.logical_and(there, odd)

    def greets(dr, dc):
        there = exists(dr, dc)
        if dr < 0:
            return jnp.logical_and(there, mutual(dr, dc)) if dc else None
        return leads(dr, dc)

    def greeted_by(dr, dc):
        there = exists(dr, dc)
        if dr > 0:
            return jnp.logical_and(there, mutual(dr, dc)) if dc else None
        return there if dr < 0 else jnp.logical_and(there, jnp.logical_not(odd))

    def alone(test, other):
        return test if other is None else jnp.logical_and(test, jnp.logical_not(other))

    barrier = pltpu.get_barrier_semaphore()
    earlier = 0
    for dr, dc in AROUND:
        test = greets(dr, dc)
        if test is not None:

            @pl.when(test)
            def _():
                pl.semaphore_signal(barrier, inc=1, device_id=device(dr, dc), device_id_type=MESH)

    for dr, dc in AROUND:
        test = greeted_by(dr, dc)
        if test is not None:
            earlier += test.astype(jnp.int32)

    def slot_of(dr, dc):
        up_down, left_right = (dr + 1) // 2, (dc + 1) // 2
        if dr == 0:
            return rims.at[pl.ds(2 * left_right, 2)]
        if dc == 0:
            return rims.at[pl.ds(8 + 2 * up_down, 2)]
        return rims.at[4 + 2 * left_right + up_down]

    def packed(dr, dc):
        up_down, left_right = (dr + 1) // 2, (dc + 1) // 2
        if dr == 0:
            return side_out.at[left_right]
        return vert_out.at[up_down] if dc == 0 else side_out.at[left_right, up_down]

    def rows_of(slot, dr):
        if dr == 0:
            return cells.at[slot]
        return cells.at[slot, :, pl.ds(0 if dr < 0 else lat.shape[1] - HALO, HALO)]

    def copies(k, dr, dc):
        first = pltpu.make_async_remote_copy(
            src_ref=rows_of(4, dr),
            dst_ref=rows_of((1 - dr) * 3 + 1 - dc, dr),
            send_sem=send1,
            recv_sem=recv1,
            device_id=device(dr, dc),
            device_id_type=MESH,
        )
        second = pltpu.make_async_remote_copy(
            src_ref=packed(dr, dc),
            dst_ref=slot_of(-dr, -dc),
            send_sem=send2,
            recv_sem=recv2,
            device_id=device(dr, dc),
            device_id_type=MESH,
        )
        return first, second

    above_below = (row > 0).astype(jnp.int32) + (row < nr - 1).astype(jnp.int32)
    beside = (col > 0).astype(jnp.int32) + (col < nc - 1).astype(jnp.int32)

    def for_all(wait):
        for v in range(min(nr, 2) - 1, min(nr, 3)):
            for h in range(min(nc, 2) - 1, min(nc, 3)):
                if v + h == 0:
                    continue

                @pl.when(jnp.logical_and(above_below == v, beside == h))
                def _():
                    wait(v + v * h + lat.shape[1] // HALO * h, 2 * (v + h) + v * h)

    def batch(ref, n, send, recv):
        part = ref.at[pl.ds(0, n), :, pl.ds(0, HALO)] if ref is cells else ref.at[pl.ds(0, n)]
        return pltpu.make_async_remote_copy(
            src_ref=part,
            dst_ref=part,
            send_sem=send,
            recv_sem=recv,
            device_id=device(0, 0),
            device_id_type=MESH,
        )

    for k, (dr, dc) in enumerate(AROUND):

        @pl.when(jnp.logical_not(exists(dr, dc)))
        def _():
            slot = cells.at[(1 + dr) * 3 + 1 + dc]
            slot[...] = jnp.zeros(slot.shape, BF16)
            pixels = slot_of(dr, dc)
            pixels[...] = jnp.zeros(pixels.shape, F32)

    @pl.when(earlier > 0)
    def _():
        pl.semaphore_wait(barrier, earlier)

    for k, (dr, dc) in FAR_FIRST:
        if dr <= 0:
            by = greeted_by(dr, dc)

            @pl.when(alone(by, greets(dr, dc) if dr * dc else None))
            def _():
                pl.semaphore_signal(
                    ready.at[READY[7 - k]], inc=1, device_id=device(dr, dc), device_id_type=MESH
                )

    loads[0].wait()
    for k, (dr, dc) in FAR_FIRST:
        by = greeted_by(dr, dc)
        if by is not None:

            @pl.when(by)
            def _():
                copies(k, dr, dc)[0].start()

    def send_later(entries, when=None):
        for k, (dr, dc) in entries:
            test = alone(leads(dr, dc), greeted_by(dr, dc) if dr else None)

            @pl.when(test if when is None else jnp.logical_and(test, when))
            def _():
                pl.semaphore_wait(ready.at[READY[k]], 1)
                copies(k, dr, dc)[0].start()

    below = [e for e in enumerate(AROUND) if e[1][0] > 0]
    hurry = jnp.logical_or(greeted_by(1, -1), greeted_by(1, 1))
    send_later(below, hurry)
    send_later([e for e in enumerate(AROUND) if e[1][0] == 0])

    tile = lat.shape[1]
    side_cells = tile + 2 * HALO
    margin, inner = 4 * HALO, 4 * tile
    size = inner + 2 * margin
    chans = lat.shape[0]
    span = size * side_cells
    half = span // 2
    wide = chans * side_cells

    loads[1].wait()
    load_out.start()
    wi32[...] = jnp.zeros(wi32.shape, F32)
    wi32[:, 0 : wi.shape[1], :] = wi[...].astype(F32)
    wi72 = wi32[...].reshape(72, wi32.shape[2]).astype(BF16)
    src, dst = iota((384, 72), 0), iota((384, 72), 1)
    pick = (
        (dst // 8 == 3 * (src % 128 // wide) + src // 128)
        & (dst % 8 == (src // side_cells) % chans)
        & (src % 128 < 3 * wide)
    )
    wc[...] = dot(pick.astype(F32).astype(BF16), wi72).astype(BF16)
    pltpu.make_async_copy(tables, tables, local_sem.at[2]).wait()
    pltpu.make_async_copy(limits, limits, local_sem.at[3]).wait()

    spread_r = (iota((size, span), 1) // side_cells == iota((size, span), 0)).astype(F32)
    spread_c = [
        (4 * (iota((size, span), 1) % side_cells) + q == iota((size, span), 0)).astype(F32)
        for q in range(4)
    ]
    spread_c = jnp.concatenate(spread_c, axis=1)
    row_w = dot(table_rows(tables[0].astype(F32), limits.at[0], row, nr, margin, inner), spread_r.astype(BF16))
    col_w = dot(table_rows(tables[1].astype(F32), limits.at[1], col, nc, margin, inner), spread_c.astype(BF16))
    lane = iota((1, span), 1)
    r_of, b_of = lane // side_cells, lane % side_cells
    inside = (
        (r_of >= margin) & (r_of < margin + inner) & (b_of >= HALO) & (b_of < HALO + tile)
    )
    for q in range(4):
        cw = col_w[:, q * span : (q + 1) * span]
        blend[q] = jnp.broadcast_to(row_w[0:1] * cw[0:1], (8, span))
        inverse[q] = jnp.broadcast_to(
            1.0 / jnp.where(inside, row_w[1:2] * cw[1:2], 1.0), (8, span)
        )

    send_later(below, jnp.logical_not(hurry))

    load_out.wait()
    wo32[...] = jnp.zeros(wo32.shape, F32)
    wo32[:, 0 : wo.shape[1], :] = wo[...].astype(F32)
    loads[6].wait()
    out_mid = wm.shape[1]
    for t in range(9):
        wmt[:, out_mid * t : out_mid * (t + 1)] = wm[BY_COLUMN[t]].T
    loads[7].wait()
    out_low = wl.shape[1]
    for t in range(9):
        wlt[:, out_low * t : out_low * (t + 1)] = wl[BY_COLUMN[t]].T

    where_b = iota((4, half), 1) % side_cells
    lower_half = iota((4, half), 1) < half // 2
    place_src, place_dst = iota((4 * half, inner), 0), iota((4 * half, inner), 1)
    place = place_dst == 4 * (place_src % side_cells - HALO) + place_src // half
    places[0] = place.astype(F32).astype(BF16)
    slot = place_src % side_cells
    from_left = place_dst == 4 * (slot % HALO) + slot // HALO
    from_right = place_dst == 4 * (tile - HALO + slot % HALO) + slot // HALO
    pair_q = 2 * (place_src // half - 2) + place_src % half // (half // 2)
    from_pair = place_dst == 4 * (slot - HALO) + pair_q
    part = place_src // half
    places[1] = jnp.where(
        part == 0, from_left.astype(F32), jnp.where(part == 1, from_right.astype(F32), from_pair.astype(F32))
    ).astype(BF16)
    for h in range(2):
        here = [inverse[q, 0:4, h * half : (h + 1) * half] for q in range(4)]
        sides = []
        for rim in (HALO, tile):
            dense = pltpu.roll(here[0], (half - rim) % half, 1)
            for q in range(1, 4):
                turned = pltpu.roll(here[q], (HALO * q - rim) % half, 1)
                dense = jnp.where(where_b // HALO == q, turned, dense)
            sides.append(dense)
        for pair in range(2):
            even, odds = here[2 * pair], here[2 * pair + 1]
            if h == 0:
                even = pltpu.roll(even, half // 2, 1)
            else:
                odds = pltpu.roll(odds, half // 2, 1)
            sides.append(jnp.where(lower_half, even, odds))
        for n, side in enumerate(sides):
            scales[h, n] = side

    for_all(lambda n, m: batch(cells, n, send1, recv1).wait_recv())

    cell = [cells[k].astype(F32) for k in range(9)]
    pieces = [[], [], []]
    for c in range(chans):
        for j, cut in enumerate((slice(tile - HALO, tile), slice(0, tile), slice(0, HALO))):
            upper, middle, lower = (cell[3 * i + j][c][:, cut] for i in range(3))
            zero = jnp.zeros((1, middle.shape[1]), F32)
            upper, lower = upper[tile - HALO :], lower[:HALO]
            pieces[0].append(jnp.concatenate([zero, upper, middle, lower[:-1]], axis=0))
            pieces[1].append(jnp.concatenate([upper, middle, lower], axis=0))
            pieces[2].append(jnp.concatenate([upper[1:], middle, lower, zero], axis=0))
    pieces = pieces[0] + pieces[1] + pieces[2]
    tall = jnp.concatenate(pieces + [jnp.zeros((side_cells, 128 - 3 * wide), F32)], axis=1)
    shape = (side_cells, side_cells, 128)
    spreaded = jnp.broadcast_to(tall[:, None, :], shape)
    gap = iota(shape, 2) % side_cells - iota(shape, 1)
    patches = [jnp.where(gap == dx - 1, spreaded, 0.0) for dx in range(3)]
    patches = jnp.concatenate(patches, axis=2).reshape(-1, 384).astype(BF16)
    first = dot(patches, wc[...]).reshape(side_cells, side_cells, -1)
    (first,) = group_silu([first])
    first = first.reshape(side_cells * side_cells, -1).astype(BF16)

    taps = dot(first, wmt[...])
    taps = [
        taps[:, out_mid * t : out_mid * (t + 1)].reshape(side_cells, side_cells, -1)
        for t in BY_COLUMN
    ]
    second = conv_up([[taps]], 1)
    second = group_silu([second[py][px] for py in range(2) for px in range(2)])
    second = jnp.concatenate(second, axis=0)
    second = second.reshape(-1, second.shape[2]).astype(BF16)

    n = side_cells * side_cells
    products = dot(second, wlt[...])
    products = [products[:, out_low * t : out_low * (t + 1)] for t in BY_COLUMN]
    taps = [
        [
            [
                p[(2 * py + px) * n : (2 * py + px + 1) * n].reshape(side_cells, side_cells, -1)
                for p in products
            ]
            for px in range(2)
        ]
        for py in range(2)
    ]
    third = conv_up(taps, 2)
    third = group_silu([third[qy][qx] for qy in range(4) for qx in range(4)])

    wo72 = wo32[...].reshape(72, wo32.shape[2]).astype(BF16)
    colour = []
    for qx in range(4):
        rows = jnp.stack([third[4 * qy + qx] for qy in range(4)], axis=1)
        colour.append(nt_dot(wo72, rows.reshape(span, rows.shape[-1]).astype(BF16)))

    def tap(q, t):
        return colour[q][8 * t : 8 * t + 8]

    sub_b = iota((8, span), 1) % side_cells
    sub_r = iota((8, span), 1) // side_cells
    row_ok = [sub_r > 0, None, sub_r < size - 1]
    col_ok = [sub_b > 0, None, sub_b < side_cells - 1]

    def moved(x, dy, dx):
        shift = (side_cells * (1 - dy) + 1 - dx) % span
        x = pltpu.roll(x, shift, 1) if shift else x
        ok = [m for m in (row_ok[dy], col_ok[dx]) if m is not None]
        return jnp.where(functools.reduce(jnp.logical_and, ok), x, 0.0) if ok else x

    for q in range(4):
        value = None
        for dy in range(3):
            near = tap(q, 3 * dy + 1)
            if q > 0:
                near = near + tap(q - 1, 3 * dy)
            if q < 3:
                near = near + tap(q + 1, 3 * dy + 2)
            term = moved(near, dy, 1)
            if q == 0:
                term = term + moved(tap(3, 3 * dy), dy, 0)
            if q == 3:
                term = term + moved(tap(0, 3 * dy + 2), dy, 2)
            value = term if value is None else value + term
        value = value * blend[q]
        for h in range(2):
            own[h, q] = value[0:4, h * half : (h + 1) * half]

    for h in range(2):
        for k, rim in ((0, 0), (1, side_cells - HALO)):
            dense = pltpu.roll(own[h, 0], (half - rim) % half, 1)
            for q in range(1, 4):
                turned = pltpu.roll(own[h, q], (HALO * q - rim) % half, 1)
                dense = jnp.where(where_b // HALO == q, turned, dense)
            side_out[k, h] = dense
        for pair in range(2):
            even, odds = own[h, 2 * pair], own[h, 2 * pair + 1]
            if h == 0:
                odds = pltpu.roll(odds, half // 2, 1)
            else:
                even = pltpu.roll(even, half // 2, 1)
            vert_out[h, pair] = jnp.where(lower_half, even, odds)

    for k, (dr, dc) in FAR_FIRST:

        @pl.when(exists(dr, dc))
        def _():
            copies(k, dr, dc)[1].start()

    lane_row = iota((8, half), 1) // side_cells
    sublane = iota((8, half), 0)
    keep = [lane_row == sublane + 8, lane_row == sublane]
    beyond_row = [lane_row % 8 == sublane, lane_row % 8 == sublane]

    def spread_rows(piece, c, mask):
        return jnp.where(mask, jnp.broadcast_to(piece[c : c + 1], (8, half)), 0.0)

    def placed(blocks, place):
        tall = jnp.concatenate(blocks, axis=0)
        top = tall.astype(BF16)
        low = (tall - top.astype(F32)).astype(BF16)
        got = dot(jnp.concatenate([top, low], axis=0), place)
        return got[: tall.shape[0]] + got[tall.shape[0] :]

    blocks = []
    for c in range(3):
        for h in range(2):
            mine = [own[h, q] * inverse[q, 0:4, h * half : (h + 1) * half] for q in range(4)]
            blocks.append(jnp.concatenate([spread_rows(p, c, keep[h]) for p in mine], axis=1))
    mine = placed(blocks, places[0])

    for_all(lambda n, m: batch(cells, n, send1, recv1).wait_send())
    for_all(lambda n, m: batch(rims, m, send2, recv2).wait_recv())

    blocks = []
    for c in range(3):
        for h in range(2):
            got = [
                (rims[h] + rims[4 + h]) * scales[h, 0],
                (rims[2 + h] + rims[6 + h]) * scales[h, 1],
                rims[8 + 2 * h] * scales[h, 2],
                rims[9 + 2 * h] * scales[h, 3],
            ]
            masks = [keep[h], keep[h], beyond_row[h], beyond_row[h]]
            blocks.append(
                jnp.concatenate([spread_rows(p, c, m) for p, m in zip(got, masks)], axis=1)
            )
    out[...] = (mine + placed(blocks, places[1])).reshape(3, inner, inner)

    for_all(lambda n, m: batch(rims, m, send2, recv2).wait_send())


def solution(mesh):
    nr, nc = mesh.shape["rows"], mesh.shape["cols"]

    def per_device(lat, w_in, w_mid, w_low, w_out, ramp_r, ramp_c, lim_r, lim_c):
        tile = lat.shape[1]
        inner = 4 * tile
        size = inner + 8 * HALO
        half = size * (tile + 2 * HALO) // 2
        anywhere = pl.BlockSpec(memory_space=pltpu.HBM)
        dma = pltpu.SemaphoreType.DMA
        return pl.pallas_call(
            functools.partial(kernel, nr, nc),
            out_shape=pltpu.VMEM((w_out.shape[1], inner, inner), F32),
            in_specs=[anywhere] * 9,
            out_specs=pl.BlockSpec(memory_space=pltpu.VMEM),
            scratch_shapes=[
                pltpu.VMEM((max(9, 6 + 2 * (lat.shape[1] // HALO)),) + lat.shape, BF16),
                pltpu.VMEM(w_in.shape, BF16),
                pltpu.VMEM(w_mid.shape, BF16),
                pltpu.VMEM(w_low.shape, BF16),
                pltpu.VMEM(w_out.shape, BF16),
                pltpu.VMEM((2,) + ramp_r.shape, jnp.int32),
                pltpu.SMEM((2,) + lim_r.shape, jnp.int32),
                pltpu.VMEM((9, 8, w_in.shape[2]), F32),
                pltpu.VMEM((9, 8, w_out.shape[2]), F32),
                pltpu.VMEM((384, w_in.shape[2]), BF16),
                pltpu.VMEM((w_mid.shape[2], 9 * w_mid.shape[1]), BF16),
                pltpu.VMEM((w_low.shape[2], 9 * w_low.shape[1]), BF16),
                pltpu.VMEM((4, 8, 2 * half), F32),
                pltpu.VMEM((4, 8, 2 * half), F32),
                pltpu.VMEM((2, 4 * half, inner), BF16),
                pltpu.VMEM((2, 4, 4, half), F32),
                pltpu.VMEM((2, 4, 4, half), F32),
                pltpu.VMEM((2, 2, 4, half), F32),
                pltpu.VMEM((2, 2, 4, half), F32),
                pltpu.VMEM((12, 4, half), F32),
                dma((6,)),
                pltpu.SemaphoreType.REGULAR((5,)),
                dma,
                dma,
            ],
            compiler_params=pltpu.CompilerParams(
                collective_id=0, has_side_effects=True
            ),
            name="decode",
        )(lat, w_in, w_mid, w_low, w_out, ramp_r, ramp_c, lim_r, lim_c)

    return jax.shard_map(
        per_device,
        mesh=mesh,
        in_specs=(P(None, ("groups", "rows"), "cols"), P(), P(), P(), P(), P(), P(), P(), P()),
        out_specs=P(None, ("groups", "rows"), "cols"),
        check_vma=False,
    )
```

```python
import functools

import jax
import jax.numpy as jnp
from jax import lax
from jax.experimental import pallas as pl
from jax.experimental.pallas import tpu as pltpu
from jax.sharding import PartitionSpec as P

MESH = pl.DeviceIdType.MESH
NGROUPS = 32
HALO = 2
F32 = jnp.float32
BF16 = jnp.bfloat16
AROUND = [(dr, dc) for dr in (-1, 0, 1) for dc in (-1, 0, 1) if (dr, dc) != (0, 0)]
FAR_FIRST = sorted(enumerate(AROUND), key=lambda e: -abs(e[1][0]) - abs(e[1][1]))
BY_COLUMN = [3 * (t % 3) + t // 3 for t in range(9)]
READY = {k: n for n, k in enumerate((3, 4, 5, 6, 7))}


def iota(shape, dim):
    return lax.broadcasted_iota(jnp.int32, shape, dim)


def nt_dot(a, b):
    return lax.dot_general(a, b, (((1,), (1,)), ((), ())), preferred_element_type=F32)


def dot(a, b):
    return jnp.dot(a, b, preferred_element_type=F32)


def down(x):
    return jnp.concatenate([jnp.zeros_like(x[:1]), x[:-1]], axis=0)


def up(x):
    return jnp.concatenate([x[1:], jnp.zeros_like(x[:1])], axis=0)


def right(x):
    rolled = pltpu.roll(x, 1, 1)
    return jnp.where(iota(x.shape, 1) == 0, 0.0, rolled)


def left(x):
    n = x.shape[1]
    rolled = pltpu.roll(x, n - 1, 1)
    return jnp.where(iota(x.shape, 1) == n - 1, 0.0, rolled)


def expand(products, fine, before, after):
    out = []
    for q in range(fine):
        t0, t1, t2 = products[q]
        prev = products[q - 1][0] if q > 0 else before(products[fine - 1][0])
        nxt = products[q + 1][2] if q < fine - 1 else after(products[0][2])
        out.append(prev + (t1 + t2))
        out.append((t0 + t1) + nxt)
    return out


def conv_up(taps, fine):
    by_col = [
        [
            expand(
                [[taps[py][px][3 * dy + dx] for dy in range(3)] for py in range(fine)],
                fine,
                down,
                up,
            )
            for dx in range(3)
        ]
        for px in range(fine)
    ]
    return [
        expand(
            [[by_col[px][dx][qy] for dx in range(3)] for px in range(fine)],
            fine,
            right,
            left,
        )
        for qy in range(2 * fine)
    ]


def group_sum(x, width):
    lane = iota(x.shape, 1) % width
    parts = [x]
    for k in range(1, width):
        parts.append(jnp.where(lane >= k, pltpu.roll(x, k, 1), 0.0))
        parts.append(jnp.where(lane < width - k, pltpu.roll(x, x.shape[1] - k, 1), 0.0))
    while len(parts) > 1:
        parts = [functools.reduce(jnp.add, parts[k : k + 2]) for k in range(0, len(parts), 2)]
    return parts[0]


def group_silu(phases, width):
    channels = phases[0].shape[-1]
    count = channels // 128
    positions = len(phases) * phases[0].shape[0] * phases[0].shape[1]
    scale = 1.0 / (positions * width)
    total = jnp.sum(functools.reduce(jnp.add, phases), axis=(0, 1)).reshape(1, channels)
    squares = functools.reduce(jnp.add, [p * p for p in phases])
    squares = jnp.sum(squares, axis=(0, 1)).reshape(1, channels)
    rows = [x[:, k * 128 : (k + 1) * 128] for x in (total, squares) for k in range(count)]
    rows = jnp.concatenate(rows + [jnp.zeros((1, 128), F32)] * (8 - len(rows)), axis=0)
    got = group_sum(rows, width) * scale
    center = got[:count]
    spread = jnp.maximum(got[count : 2 * count] - center * center, 0.0)
    factor = 0.5 * lax.rsqrt(spread + 1e-06)
    offset = center * factor
    factor = jnp.concatenate([factor[k : k + 1] for k in range(count)], axis=1)[None]
    offset = jnp.concatenate([offset[k : k + 1] for k in range(count)], axis=1)[None]
    result = []
    for p in phases:
        half = p * factor - offset
        result.append(half + half * jnp.tanh(half))
    return result


def table_rows(table, limits, index, count, margin, inner):
    size = table.shape[1]
    pos = iota((1, size), 1)
    far = jnp.maximum(jnp.maximum(margin - pos, pos - (margin + inner) + 1), 0)
    rows = []
    for d in (-1, 0, 1):
        here = index + d
        limit = limits[jnp.clip(here, 0, count - 1)]
        picked = jnp.where(iota(table.shape, 0) == here, table, 0.0)
        row = jnp.sum(picked, axis=0, keepdims=True)
        rows.append(jnp.where(far <= limit, row, 0.0))
    above, own, below = rows
    other = jnp.where(pos < inner, jnp.roll(above, inner, 1), jnp.roll(below, inner, 1))
    pair = jnp.concatenate([own, own + other, jnp.zeros((6, size), F32)], axis=0)
    return pair.astype(BF16)


def body(
    nr, nc, lat, w_in, w_mid, w_low, w_out, ramp_r, ramp_c, lim_r, lim_c, out,
    cells, wi, wm, wl, wo, tables, limits, wi32, wo32, wc, wmt, wlt,
    blend, inverse, places, scales, own, side_out, vert_out, rims,
    ready, recv1, recv2, local_sem,
):
    row, col = lax.axis_index("rows"), lax.axis_index("cols")

    def exists(dr, dc):
        ok = None
        for d, here, n in ((dr, row, nr), (dc, col, nc)):
            test = None if d == 0 else (here > 0 if d < 0 else here < n - 1)
            if test is not None:
                ok = test if ok is None else jnp.logical_and(ok, test)
        return ok

    def device(dr, dc):
        return {"rows": row + dr, "cols": col + dc}

    loads = [
        pltpu.make_async_copy(src, dst, local_sem.at[k])
        for k, src, dst in [
            (0, lat, cells.at[4]),
            (1, w_in, wi),
            (2, ramp_r, tables.at[0]),
            (2, ramp_c, tables.at[1]),
            (3, lim_r, limits.at[0]),
            (3, lim_c, limits.at[1]),
            (4, w_mid, wm),
            (5, w_low, wl),
        ]
    ]
    load_out = pltpu.make_async_copy(w_out, wo, local_sem.at[1])
    send1, send2 = local_sem.at[0], local_sem.at[1]
    odd = col % 2 == 1

    def mutual(dr, dc):
        return jnp.logical_and(row == (0 if dr > 0 else 1), odd if dc > 0 else jnp.logical_not(odd))

    def leads(dr, dc):
        there = exists(dr, dc)
        return there if dr > 0 else jnp.logical_and(there, odd)

    def greets(dr, dc):
        there = exists(dr, dc)
        if dr < 0:
            return jnp.logical_and(there, mutual(dr, dc)) if dc else None
        return leads(dr, dc)

    def greeted_by(dr, dc):
        there = exists(dr, dc)
        if dr > 0:
            return jnp.logical_and(there, mutual(dr, dc)) if dc else None
        return there if dr < 0 else jnp.logical_and(there, jnp.logical_not(odd))

    def alone(test, other):
        return test if other is None else jnp.logical_and(test, jnp.logical_not(other))

    barrier = pltpu.get_barrier_semaphore()
    earlier = 0

    def greet(entries):
        for dr, dc in entries:
            test = greets(dr, dc)
            if test is not None:

                @pl.when(test)
                def _():
                    pl.semaphore_signal(
                        barrier, inc=1, device_id=device(dr, dc), device_id_type=MESH
                    )

    loads[0].start()
    greet([e for e in AROUND if e[0] < 0])
    for load in loads[1:]:
        load.start()
    greet([e for e in AROUND if e[0] >= 0])
    for dr, dc in AROUND:
        test = greeted_by(dr, dc)
        if test is not None:
            earlier += test.astype(jnp.int32)

    def slot_of(dr, dc):
        up_down, left_right = (dr + 1) // 2, (dc + 1) // 2
        if dr == 0:
            return rims.at[pl.ds(2 * left_right, 2)]
        if dc == 0:
            return rims.at[pl.ds(8 + 2 * up_down, 2)]
        return rims.at[4 + 2 * left_right + up_down]

    def packed(dr, dc):
        up_down, left_right = (dr + 1) // 2, (dc + 1) // 2
        if dr == 0:
            return side_out.at[left_right]
        return vert_out.at[up_down] if dc == 0 else side_out.at[left_right, up_down]

    def rows_of(slot, dr):
        if dr == 0:
            return cells.at[slot]
        return cells.at[slot, :, pl.ds(0 if dr < 0 else lat.shape[1] - HALO, HALO)]

    def copies(k, dr, dc):
        first = pltpu.make_async_remote_copy(
            src_ref=rows_of(4, dr),
            dst_ref=rows_of((1 - dr) * 3 + 1 - dc, dr),
            send_sem=send1,
            recv_sem=recv1,
            device_id=device(dr, dc),
            device_id_type=MESH,
        )
        second = pltpu.make_async_remote_copy(
            src_ref=packed(dr, dc),
            dst_ref=slot_of(-dr, -dc),
            send_sem=send2,
            recv_sem=recv2,
            device_id=device(dr, dc),
            device_id_type=MESH,
        )
        return first, second

    above_below = (row > 0).astype(jnp.int32) + (row < nr - 1).astype(jnp.int32)
    beside = (col > 0).astype(jnp.int32) + (col < nc - 1).astype(jnp.int32)

    def for_all(wait):
        for v in range(min(nr, 2) - 1, min(nr, 3)):
            for h in range(min(nc, 2) - 1, min(nc, 3)):
                if v + h == 0:
                    continue

                @pl.when(jnp.logical_and(above_below == v, beside == h))
                def _():
                    wait(v + v * h + lat.shape[1] // HALO * h, 2 * (v + h) + v * h)

    def batch(ref, n, send, recv):
        part = ref.at[pl.ds(0, n), :, pl.ds(0, HALO)] if ref is cells else ref.at[pl.ds(0, n)]
        return pltpu.make_async_remote_copy(
            src_ref=part,
            dst_ref=part,
            send_sem=send,
            recv_sem=recv,
            device_id=device(0, 0),
            device_id_type=MESH,
        )

    for k, (dr, dc) in enumerate(AROUND):

        @pl.when(jnp.logical_not(exists(dr, dc)))
        def _():
            slot = cells.at[(1 + dr) * 3 + 1 + dc]
            slot[...] = jnp.zeros(slot.shape, BF16)
            pixels = slot_of(dr, dc)
            pixels[...] = jnp.zeros(pixels.shape, F32)

    @pl.when(earlier > 0)
    def _():
        pl.semaphore_wait(barrier, earlier)

    for k, (dr, dc) in FAR_FIRST:
        if dr <= 0:
            by = greeted_by(dr, dc)

            @pl.when(alone(by, greets(dr, dc) if dr * dc else None))
            def _():
                pl.semaphore_signal(
                    ready.at[READY[7 - k]], inc=1, device_id=device(dr, dc), device_id_type=MESH
                )

    loads[0].wait()
    for k, (dr, dc) in FAR_FIRST:
        by = greeted_by(dr, dc)
        if by is not None:

            @pl.when(by)
            def _():
                copies(k, dr, dc)[0].start()

    def send_later(entries, when=None):
        for k, (dr, dc) in entries:
            test = alone(leads(dr, dc), greeted_by(dr, dc) if dr else None)

            @pl.when(test if when is None else jnp.logical_and(test, when))
            def _():
                pl.semaphore_wait(ready.at[READY[k]], 1)
                copies(k, dr, dc)[0].start()

    below = [e for e in enumerate(AROUND) if e[1][0] > 0]
    hurry = jnp.logical_or(greeted_by(1, -1), greeted_by(1, 1))
    send_later(below, hurry)
    send_later([e for e in enumerate(AROUND) if e[1][0] == 0])

    tile = lat.shape[1]
    side_cells = tile + 2 * HALO
    margin, inner = 4 * HALO, 4 * tile
    size = inner + 2 * margin
    chans = lat.shape[0]
    span = size * side_cells
    half = span // 2
    wide = chans * side_cells

    loads[1].wait()
    load_out.start()
    wi32[...] = jnp.zeros(wi32.shape, F32)
    wi32[:, 0 : wi.shape[1], :] = wi[...].astype(F32)
    wi72 = wi32[...].reshape(72, wi32.shape[2]).astype(BF16)
    src, dst = iota((384, 72), 0), iota((384, 72), 1)
    pick = (
        (dst // 8 == 3 * (src % 128 // wide) + src // 128)
        & (dst % 8 == (src // side_cells) % chans)
        & (src % 128 < 3 * wide)
    )
    wc[...] = dot(pick.astype(F32).astype(BF16), wi72).astype(BF16)
    pltpu.make_async_copy(tables, tables, local_sem.at[2]).wait()
    pltpu.make_async_copy(limits, limits, local_sem.at[3]).wait()

    spread_r = (iota((size, span), 1) // side_cells == iota((size, span), 0)).astype(F32)
    spread_c = [
        (4 * (iota((size, span), 1) % side_cells) + q == iota((size, span), 0)).astype(F32)
        for q in range(4)
    ]
    spread_c = jnp.concatenate(spread_c, axis=1)
    row_w = dot(table_rows(tables[0].astype(F32), limits.at[0], row, nr, margin, inner), spread_r.astype(BF16))
    col_w = dot(table_rows(tables[1].astype(F32), limits.at[1], col, nc, margin, inner), spread_c.astype(BF16))
    lane = iota((1, span), 1)
    r_of, b_of = lane // side_cells, lane % side_cells
    inside = (
        (r_of >= margin) & (r_of < margin + inner) & (b_of >= HALO) & (b_of < HALO + tile)
    )
    for q in range(4):
        cw = col_w[:, q * span : (q + 1) * span]
        blend[q] = jnp.broadcast_to(row_w[0:1] * cw[0:1], (8, span))
        inverse[q] = jnp.broadcast_to(
            1.0 / jnp.where(inside, row_w[1:2] * cw[1:2], 1.0), (8, span)
        )

    send_later(below, jnp.logical_not(hurry))

    load_out.wait()
    wo32[...] = jnp.zeros(wo32.shape, F32)
    wo32[:, 0 : wo.shape[1], :] = wo[...].astype(F32)
    loads[6].wait()
    out_mid = wm.shape[1]
    for t in range(9):
        turned = wm[BY_COLUMN[t]].T
        for n in range(out_mid // 128):
            at = 128 * (9 * n + t)
            wmt[:, at : at + 128] = turned[:, 128 * n : 128 * (n + 1)]
    loads[7].wait()
    out_low = wl.shape[1]
    for t in range(9):
        wlt[:, out_low * t : out_low * (t + 1)] = wl[BY_COLUMN[t]].T

    where_b = iota((4, half), 1) % side_cells
    lower_half = iota((4, half), 1) < half // 2
    place_src, place_dst = iota((4 * half, inner), 0), iota((4 * half, inner), 1)
    place = place_dst == 4 * (place_src % side_cells - HALO) + place_src // half
    places[0] = place.astype(F32).astype(BF16)
    slot = place_src % side_cells
    from_left = place_dst == 4 * (slot % HALO) + slot // HALO
    from_right = place_dst == 4 * (tile - HALO + slot % HALO) + slot // HALO
    pair_q = 2 * (place_src // half - 2) + place_src % half // (half // 2)
    from_pair = place_dst == 4 * (slot - HALO) + pair_q
    part = place_src // half
    places[1] = jnp.where(
        part == 0, from_left.astype(F32), jnp.where(part == 1, from_right.astype(F32), from_pair.astype(F32))
    ).astype(BF16)
    for h in range(2):
        here = [inverse[q, 0:4, h * half : (h + 1) * half] for q in range(4)]
        sides = []
        for rim in (HALO, tile):
            dense = pltpu.roll(here[0], (half - rim) % half, 1)
            for q in range(1, 4):
                turned = pltpu.roll(here[q], (HALO * q - rim) % half, 1)
                dense = jnp.where(where_b // HALO == q, turned, dense)
            sides.append(dense)
        for pair in range(2):
            even, odds = here[2 * pair], here[2 * pair + 1]
            if h == 0:
                even = pltpu.roll(even, half // 2, 1)
            else:
                odds = pltpu.roll(odds, half // 2, 1)
            sides.append(jnp.where(lower_half, even, odds))
        for n, side in enumerate(sides):
            scales[h, n] = side

    for_all(lambda n, m: batch(cells, n, send1, recv1).wait_recv())

    cell = [cells[k].astype(F32) for k in range(9)]
    pieces = [[], [], []]
    for c in range(chans):
        for j, cut in enumerate((slice(tile - HALO, tile), slice(0, tile), slice(0, HALO))):
            upper, middle, lower = (cell[3 * i + j][c][:, cut] for i in range(3))
            zero = jnp.zeros((1, middle.shape[1]), F32)
            upper, lower = upper[tile - HALO :], lower[:HALO]
            pieces[0].append(jnp.concatenate([zero, upper, middle, lower[:-1]], axis=0))
            pieces[1].append(jnp.concatenate([upper, middle, lower], axis=0))
            pieces[2].append(jnp.concatenate([upper[1:], middle, lower, zero], axis=0))
    pieces = pieces[0] + pieces[1] + pieces[2]
    tall = jnp.concatenate(pieces + [jnp.zeros((side_cells, 128 - 3 * wide), F32)], axis=1)
    shape = (side_cells, side_cells, 128)
    spreaded = jnp.broadcast_to(tall[:, None, :], shape)
    gap = iota(shape, 2) % side_cells - iota(shape, 1)
    patches = [jnp.where(gap == dx - 1, spreaded, 0.0) for dx in range(3)]
    patches = jnp.concatenate(patches, axis=2).reshape(-1, 384).astype(BF16)
    first = dot(patches, wc[...]).reshape(side_cells, side_cells, -1)
    (first,) = group_silu([first], first.shape[2] // NGROUPS)
    first = first.reshape(side_cells * side_cells, -1).astype(BF16)

    taps = dot(first, wmt[...])
    chunks = []
    for n in range(out_mid // 128):
        part = [
            taps[:, 128 * (9 * n + t) : 128 * (9 * n + t + 1)].reshape(side_cells, side_cells, -1)
            for t in BY_COLUMN
        ]
        part = conv_up([[part]], 1)
        part = [part[py][px] for py in range(2) for px in range(2)]
        chunks.append(group_silu(part, out_mid // NGROUPS))
    second = [jnp.concatenate(parts, axis=2) for parts in zip(*chunks)]
    second = jnp.concatenate(second, axis=0)
    second = second.reshape(-1, second.shape[2]).astype(BF16)

    n = side_cells * side_cells
    products = dot(second, wlt[...])
    products = [products[:, out_low * t : out_low * (t + 1)] for t in BY_COLUMN]
    taps = [
        [
            [
                p[(2 * py + px) * n : (2 * py + px + 1) * n].reshape(side_cells, side_cells, -1)
                for p in products
            ]
            for px in range(2)
        ]
        for py in range(2)
    ]
    third = conv_up(taps, 2)
    third = [third[qy][qx] for qy in range(4) for qx in range(4)]
    third = group_silu(third, out_low // NGROUPS)

    wo72 = wo32[...].reshape(72, wo32.shape[2]).astype(BF16)
    colour = []
    for qx in range(4):
        rows = jnp.stack([third[4 * qy + qx] for qy in range(4)], axis=1)
        colour.append(nt_dot(wo72, rows.reshape(span, rows.shape[-1]).astype(BF16)))

    def tap(q, t):
        return colour[q][8 * t : 8 * t + 8]

    sub_b = iota((8, span), 1) % side_cells
    sub_r = iota((8, span), 1) // side_cells
    row_ok = [sub_r > 0, None, sub_r < size - 1]
    col_ok = [sub_b > 0, None, sub_b < side_cells - 1]

    def moved(x, dy, dx):
        shift = (side_cells * (1 - dy) + 1 - dx) % span
        x = pltpu.roll(x, shift, 1) if shift else x
        ok = [m for m in (row_ok[dy], col_ok[dx]) if m is not None]
        return jnp.where(functools.reduce(jnp.logical_and, ok), x, 0.0) if ok else x

    for q in range(4):
        value = None
        for dy in range(3):
            near = tap(q, 3 * dy + 1)
            if q > 0:
                near = near + tap(q - 1, 3 * dy)
            if q < 3:
                near = near + tap(q + 1, 3 * dy + 2)
            term = moved(near, dy, 1)
            if q == 0:
                term = term + moved(tap(3, 3 * dy), dy, 0)
            if q == 3:
                term = term + moved(tap(0, 3 * dy + 2), dy, 2)
            value = term if value is None else value + term
        value = value * blend[q]
        for h in range(2):
            own[h, q] = value[0:4, h * half : (h + 1) * half]

    for h in range(2):
        for k, rim in ((0, 0), (1, side_cells - HALO)):
            dense = pltpu.roll(own[h, 0], (half - rim) % half, 1)
            for q in range(1, 4):
                turned = pltpu.roll(own[h, q], (HALO * q - rim) % half, 1)
                dense = jnp.where(where_b // HALO == q, turned, dense)
            side_out[k, h] = dense
        for pair in range(2):
            even, odds = own[h, 2 * pair], own[h, 2 * pair + 1]
            if h == 0:
                odds = pltpu.roll(odds, half // 2, 1)
            else:
                even = pltpu.roll(even, half // 2, 1)
            vert_out[h, pair] = jnp.where(lower_half, even, odds)

    for k, (dr, dc) in FAR_FIRST:

        @pl.when(exists(dr, dc))
        def _():
            copies(k, dr, dc)[1].start()

    lane_row = iota((8, half), 1) // side_cells
    sublane = iota((8, half), 0)
    keep = [lane_row == sublane + 8, lane_row == sublane]
    beyond_row = [lane_row % 8 == sublane, lane_row % 8 == sublane]

    def spread_rows(piece, c, mask):
        return jnp.where(mask, jnp.broadcast_to(piece[c : c + 1], (8, half)), 0.0)

    def placed(blocks, place):
        tall = jnp.concatenate(blocks, axis=0)
        top = tall.astype(BF16)
        low = (tall - top.astype(F32)).astype(BF16)
        got = dot(jnp.concatenate([top, low], axis=0), place)
        return got[: tall.shape[0]] + got[tall.shape[0] :]

    blocks = []
    for c in range(3):
        for h in range(2):
            mine = [own[h, q] * inverse[q, 0:4, h * half : (h + 1) * half] for q in range(4)]
            blocks.append(jnp.concatenate([spread_rows(p, c, keep[h]) for p in mine], axis=1))
    mine = placed(blocks, places[0])

    for_all(lambda n, m: batch(cells, n, send1, recv1).wait_send())
    for_all(lambda n, m: batch(rims, m, send2, recv2).wait_recv())

    blocks = []
    for c in range(3):
        for h in range(2):
            got = [
                (rims[h] + rims[4 + h]) * scales[h, 0],
                (rims[2 + h] + rims[6 + h]) * scales[h, 1],
                rims[8 + 2 * h] * scales[h, 2],
                rims[9 + 2 * h] * scales[h, 3],
            ]
            masks = [keep[h], keep[h], beyond_row[h], beyond_row[h]]
            blocks.append(
                jnp.concatenate([spread_rows(p, c, m) for p, m in zip(got, masks)], axis=1)
            )
    out[...] = (mine + placed(blocks, places[1])).reshape(3, inner, inner)

    for_all(lambda n, m: batch(rims, m, send2, recv2).wait_send())


def kernel(nr, nc, *refs):
    def scoped(local_sem):
        body(nr, nc, *refs, local_sem)

    pl.run_scoped(scoped, pltpu.SemaphoreType.DMA((6,)))


def solution(mesh):
    nr, nc = mesh.shape["rows"], mesh.shape["cols"]

    def per_device(lat, w_in, w_mid, w_low, w_out, ramp_r, ramp_c, lim_r, lim_c):
        tile = lat.shape[1]
        inner = 4 * tile
        size = inner + 8 * HALO
        half = size * (tile + 2 * HALO) // 2
        anywhere = pl.BlockSpec(memory_space=pltpu.HBM)
        dma = pltpu.SemaphoreType.DMA
        return pl.pallas_call(
            functools.partial(kernel, nr, nc),
            out_shape=pltpu.VMEM((w_out.shape[1], inner, inner), F32),
            in_specs=[anywhere] * 9,
            out_specs=pl.BlockSpec(memory_space=pltpu.VMEM),
            scratch_shapes=[
                pltpu.VMEM((max(9, 6 + 2 * (lat.shape[1] // HALO)),) + lat.shape, BF16),
                pltpu.VMEM(w_in.shape, BF16),
                pltpu.VMEM(w_mid.shape, BF16),
                pltpu.VMEM(w_low.shape, BF16),
                pltpu.VMEM(w_out.shape, BF16),
                pltpu.VMEM((2,) + ramp_r.shape, jnp.int32),
                pltpu.SMEM((2,) + lim_r.shape, jnp.int32),
                pltpu.VMEM((9, 8, w_in.shape[2]), F32),
                pltpu.VMEM((9, 8, w_out.shape[2]), F32),
                pltpu.VMEM((384, w_in.shape[2]), BF16),
                pltpu.VMEM((w_mid.shape[2], 9 * w_mid.shape[1]), BF16),
                pltpu.VMEM((w_low.shape[2], 9 * w_low.shape[1]), BF16),
                pltpu.VMEM((4, 8, 2 * half), F32),
                pltpu.VMEM((4, 8, 2 * half), F32),
                pltpu.VMEM((2, 4 * half, inner), BF16),
                pltpu.VMEM((2, 4, 4, half), F32),
                pltpu.VMEM((2, 4, 4, half), F32),
                pltpu.VMEM((2, 2, 4, half), F32),
                pltpu.VMEM((2, 2, 4, half), F32),
                pltpu.VMEM((12, 4, half), F32),
                pltpu.SemaphoreType.REGULAR((5,)),
                dma,
                dma,
            ],
            compiler_params=pltpu.CompilerParams(
                collective_id=0, has_side_effects=True
            ),
            name="decode",
        )(lat, w_in, w_mid, w_low, w_out, ramp_r, ramp_c, lim_r, lim_c)

    return jax.shard_map(
        per_device,
        mesh=mesh,
        in_specs=(P(None, ("groups", "rows"), "cols"), P(), P(), P(), P(), P(), P(), P(), P()),
        out_specs=P(None, ("groups", "rows"), "cols"),
        check_vma=False,
    )
```

```python
import functools

import jax
import jax.numpy as jnp
from jax import lax
from jax.experimental import pallas as pl
from jax.experimental.pallas import tpu as pltpu
from jax.sharding import PartitionSpec as P

MESH = pl.DeviceIdType.MESH
NGROUPS = 32
HALO = 2
F32 = jnp.float32
BF16 = jnp.bfloat16
AROUND = [(dr, dc) for dr in (-1, 0, 1) for dc in (-1, 0, 1) if (dr, dc) != (0, 0)]
FAR_FIRST = sorted(enumerate(AROUND), key=lambda e: -abs(e[1][0]) - abs(e[1][1]))
BY_COLUMN = [3 * (t % 3) + t // 3 for t in range(9)]
READY = {k: n for n, k in enumerate((3, 4, 5, 6, 7))}


def iota(shape, dim):
    return lax.broadcasted_iota(jnp.int32, shape, dim)


def nt_dot(a, b):
    return lax.dot_general(a, b, (((1,), (1,)), ((), ())), preferred_element_type=F32)


def dot(a, b):
    return jnp.dot(a, b, preferred_element_type=F32)


def down(x):
    return jnp.concatenate([jnp.zeros_like(x[:1]), x[:-1]], axis=0)


def up(x):
    return jnp.concatenate([x[1:], jnp.zeros_like(x[:1])], axis=0)


def right(x):
    rolled = pltpu.roll(x, 1, 1)
    return jnp.where(iota(x.shape, 1) == 0, 0.0, rolled)


def left(x):
    n = x.shape[1]
    rolled = pltpu.roll(x, n - 1, 1)
    return jnp.where(iota(x.shape, 1) == n - 1, 0.0, rolled)


def expand(products, fine, before, after):
    out = []
    for q in range(fine):
        t0, t1, t2 = products[q]
        prev = products[q - 1][0] if q > 0 else before(products[fine - 1][0])
        nxt = products[q + 1][2] if q < fine - 1 else after(products[0][2])
        out.append(prev + (t1 + t2))
        out.append((t0 + t1) + nxt)
    return out


def conv_up(taps, fine):
    by_col = [
        [
            expand(
                [[taps[py][px][3 * dy + dx] for dy in range(3)] for py in range(fine)],
                fine,
                down,
                up,
            )
            for dx in range(3)
        ]
        for px in range(fine)
    ]
    return [
        expand(
            [[by_col[px][dx][qy] for dx in range(3)] for px in range(fine)],
            fine,
            right,
            left,
        )
        for qy in range(2 * fine)
    ]


def group_sum(x, width):
    lane = iota(x.shape, 1) % width
    parts = [x]
    for k in range(1, width):
        parts.append(jnp.where(lane >= k, pltpu.roll(x, k, 1), 0.0))
        parts.append(jnp.where(lane < width - k, pltpu.roll(x, x.shape[1] - k, 1), 0.0))
    while len(parts) > 1:
        parts = [functools.reduce(jnp.add, parts[k : k + 2]) for k in range(0, len(parts), 2)]
    return parts[0]


def group_terms(phases, width):
    channels = phases[0].shape[-1]
    count = channels // 128
    positions = len(phases) * phases[0].shape[0] * phases[0].shape[1]
    scale = 1.0 / (positions * width)
    total = jnp.sum(functools.reduce(jnp.add, phases), axis=(0, 1)).reshape(1, channels)
    squares = functools.reduce(jnp.add, [p * p for p in phases])
    squares = jnp.sum(squares, axis=(0, 1)).reshape(1, channels)
    rows = [x[:, k * 128 : (k + 1) * 128] for x in (total, squares) for k in range(count)]
    rows = jnp.concatenate(rows + [jnp.zeros((1, 128), F32)] * (8 - len(rows)), axis=0)
    got = group_sum(rows, width) * scale
    center = got[:count]
    spread = jnp.maximum(got[count : 2 * count] - center * center, 0.0)
    factor = 0.5 * lax.rsqrt(spread + 1e-06)
    offset = center * factor
    factor = jnp.concatenate([factor[k : k + 1] for k in range(count)], axis=1)[None]
    offset = jnp.concatenate([offset[k : k + 1] for k in range(count)], axis=1)[None]
    return factor, offset


def silu(p, terms):
    half = p * terms[0] - terms[1]
    return half + half * jnp.tanh(half)


def group_silu(phases, width):
    terms = group_terms(phases, width)
    return [silu(p, terms) for p in phases]


def table_rows(table, limits, index, count, margin, inner):
    size = table.shape[1]
    pos = iota((1, size), 1)
    far = jnp.maximum(jnp.maximum(margin - pos, pos - (margin + inner) + 1), 0)
    rows = []
    for d in (-1, 0, 1):
        here = index + d
        limit = limits[jnp.clip(here, 0, count - 1)]
        picked = jnp.where(iota(table.shape, 0) == here, table, 0.0)
        row = jnp.sum(picked, axis=0, keepdims=True)
        rows.append(jnp.where(far <= limit, row, 0.0))
    above, own, below = rows
    other = jnp.where(pos < inner, jnp.roll(above, inner, 1), jnp.roll(below, inner, 1))
    pair = jnp.concatenate([own, own + other, jnp.zeros((6, size), F32)], axis=0)
    return pair.astype(BF16)


def body(
    nr, nc, lat, w_in, w_mid, w_low, w_out, ramp_r, ramp_c, lim_r, lim_c, out,
    cells, wi, wm, wl, wo, tables, limits, wi32, wo32, wc, wmt, wlt,
    blend, inverse, places, scales, own, up_out, side_out, vert_out, rims,
    ready, recv1, recv2, local_sem,
):
    row, col = lax.axis_index("rows"), lax.axis_index("cols")

    def exists(dr, dc):
        ok = None
        for d, here, n in ((dr, row, nr), (dc, col, nc)):
            test = None if d == 0 else (here > 0 if d < 0 else here < n - 1)
            if test is not None:
                ok = test if ok is None else jnp.logical_and(ok, test)
        return ok

    def device(dr, dc):
        return {"rows": row + dr, "cols": col + dc}

    loads = [
        pltpu.make_async_copy(src, dst, local_sem.at[k])
        for k, src, dst in [
            (0, lat, cells.at[4]),
            (1, w_in, wi),
            (2, ramp_r, tables.at[0]),
            (2, ramp_c, tables.at[1]),
            (3, lim_r, limits.at[0]),
            (3, lim_c, limits.at[1]),
            (4, w_mid, wm),
            (5, w_low, wl),
        ]
    ]
    load_out = pltpu.make_async_copy(w_out, wo, local_sem.at[1])
    send1, send2 = local_sem.at[0], local_sem.at[1]
    odd = col % 2 == 1

    def mutual(dr, dc):
        return jnp.logical_and(row == (0 if dr > 0 else 1), odd if dc > 0 else jnp.logical_not(odd))

    def leads(dr, dc):
        there = exists(dr, dc)
        return there if dr > 0 else jnp.logical_and(there, odd)

    def greets(dr, dc):
        there = exists(dr, dc)
        if dr < 0:
            return jnp.logical_and(there, mutual(dr, dc)) if dc else None
        return leads(dr, dc)

    def greeted_by(dr, dc):
        there = exists(dr, dc)
        if dr > 0:
            return jnp.logical_and(there, mutual(dr, dc)) if dc else None
        return there if dr < 0 else jnp.logical_and(there, jnp.logical_not(odd))

    def alone(test, other):
        return test if other is None else jnp.logical_and(test, jnp.logical_not(other))

    barrier = pltpu.get_barrier_semaphore()
    earlier = 0

    def greet(entries):
        for dr, dc in entries:
            test = greets(dr, dc)
            if test is not None:

                @pl.when(test)
                def _():
                    pl.semaphore_signal(
                        barrier, inc=1, device_id=device(dr, dc), device_id_type=MESH
                    )

    loads[0].start()
    greet([e for e in AROUND if e[0] < 0])
    for load in loads[1:]:
        load.start()
    greet([e for e in AROUND if e[0] >= 0])
    for dr, dc in AROUND:
        test = greeted_by(dr, dc)
        if test is not None:
            earlier += test.astype(jnp.int32)

    def slot_of(dr, dc):
        up_down, left_right = (dr + 1) // 2, (dc + 1) // 2
        if dr == 0:
            return rims.at[pl.ds(2 * left_right, 2)]
        if dc == 0:
            return rims.at[pl.ds(8 + 2 * up_down, 2)]
        return rims.at[4 + 2 * left_right + up_down]

    def packed(dr, dc):
        up_down, left_right = (dr + 1) // 2, (dc + 1) // 2
        if dr == 0:
            return side_out.at[left_right]
        if dc == 0:
            return vert_out.at[up_down]
        return up_out.at[left_right] if dr < 0 else side_out.at[left_right, 1]

    def rows_of(slot, dr):
        if dr == 0:
            return cells.at[slot]
        return cells.at[slot, :, pl.ds(0 if dr < 0 else lat.shape[1] - HALO, HALO)]

    def copies(k, dr, dc):
        first = pltpu.make_async_remote_copy(
            src_ref=rows_of(4, dr),
            dst_ref=rows_of((1 - dr) * 3 + 1 - dc, dr),
            send_sem=send1,
            recv_sem=recv1,
            device_id=device(dr, dc),
            device_id_type=MESH,
        )
        second = pltpu.make_async_remote_copy(
            src_ref=packed(dr, dc),
            dst_ref=slot_of(-dr, -dc),
            send_sem=send2,
            recv_sem=recv2,
            device_id=device(dr, dc),
            device_id_type=MESH,
        )
        return first, second

    above_below = (row > 0).astype(jnp.int32) + (row < nr - 1).astype(jnp.int32)
    beside = (col > 0).astype(jnp.int32) + (col < nc - 1).astype(jnp.int32)

    def for_all(wait):
        for v in range(min(nr, 2) - 1, min(nr, 3)):
            for h in range(min(nc, 2) - 1, min(nc, 3)):
                if v + h == 0:
                    continue

                @pl.when(jnp.logical_and(above_below == v, beside == h))
                def _():
                    wait(v + v * h + lat.shape[1] // HALO * h, 2 * (v + h) + v * h)

    def batch(ref, n, send, recv):
        part = ref.at[pl.ds(0, n), :, pl.ds(0, HALO)] if ref is cells else ref.at[pl.ds(0, n)]
        return pltpu.make_async_remote_copy(
            src_ref=part,
            dst_ref=part,
            send_sem=send,
            recv_sem=recv,
            device_id=device(0, 0),
            device_id_type=MESH,
        )

    for k, (dr, dc) in enumerate(AROUND):

        @pl.when(jnp.logical_not(exists(dr, dc)))
        def _():
            slot = cells.at[(1 + dr) * 3 + 1 + dc]
            slot[...] = jnp.zeros(slot.shape, BF16)
            pixels = slot_of(dr, dc)
            pixels[...] = jnp.zeros(pixels.shape, F32)

    @pl.when(earlier > 0)
    def _():
        pl.semaphore_wait(barrier, earlier)

    for k, (dr, dc) in FAR_FIRST:
        if dr <= 0:
            by = greeted_by(dr, dc)

            @pl.when(alone(by, greets(dr, dc) if dr * dc else None))
            def _():
                pl.semaphore_signal(
                    ready.at[READY[7 - k]], inc=1, device_id=device(dr, dc), device_id_type=MESH
                )

    loads[0].wait()
    for k, (dr, dc) in FAR_FIRST:
        by = greeted_by(dr, dc)
        if by is not None:

            @pl.when(by)
            def _():
                copies(k, dr, dc)[0].start()

    def send_later(entries, when=None):
        for k, (dr, dc) in entries:
            test = alone(leads(dr, dc), greeted_by(dr, dc) if dr else None)

            @pl.when(test if when is None else jnp.logical_and(test, when))
            def _():
                pl.semaphore_wait(ready.at[READY[k]], 1)
                copies(k, dr, dc)[0].start()

    below = [e for e in enumerate(AROUND) if e[1][0] > 0]
    hurry = jnp.logical_or(greeted_by(1, -1), greeted_by(1, 1))
    send_later(below, hurry)
    send_later([e for e in enumerate(AROUND) if e[1][0] == 0])

    tile = lat.shape[1]
    side_cells = tile + 2 * HALO
    margin, inner = 4 * HALO, 4 * tile
    size = inner + 2 * margin
    chans = lat.shape[0]
    span = size * side_cells
    half = span // 2
    wide = chans * side_cells

    loads[1].wait()
    load_out.start()
    wi32[...] = jnp.zeros(wi32.shape, F32)
    wi32[:, 0 : wi.shape[1], :] = wi[...].astype(F32)
    wi72 = wi32[...].reshape(72, wi32.shape[2]).astype(BF16)
    src, dst = iota((384, 72), 0), iota((384, 72), 1)
    pick = (
        (dst // 8 == 3 * (src % 128 // wide) + src // 128)
        & (dst % 8 == (src // side_cells) % chans)
        & (src % 128 < 3 * wide)
    )
    wc[...] = dot(pick.astype(F32).astype(BF16), wi72).astype(BF16)
    pltpu.make_async_copy(tables, tables, local_sem.at[2]).wait()
    pltpu.make_async_copy(limits, limits, local_sem.at[3]).wait()

    spread_r = (iota((size, span), 1) // side_cells == iota((size, span), 0)).astype(F32)
    spread_c = [
        (4 * (iota((size, span), 1) % side_cells) + q == iota((size, span), 0)).astype(F32)
        for q in range(4)
    ]
    spread_c = jnp.concatenate(spread_c, axis=1)
    row_w = dot(table_rows(tables[0].astype(F32), limits.at[0], row, nr, margin, inner), spread_r.astype(BF16))
    col_w = dot(table_rows(tables[1].astype(F32), limits.at[1], col, nc, margin, inner), spread_c.astype(BF16))
    lane = iota((1, span), 1)
    r_of, b_of = lane // side_cells, lane % side_cells
    inside = (
        (r_of >= margin) & (r_of < margin + inner) & (b_of >= HALO) & (b_of < HALO + tile)
    )
    for q in range(4):
        cw = col_w[:, q * span : (q + 1) * span]
        blend[q] = jnp.broadcast_to(row_w[0:1] * cw[0:1], (8, span))
        inverse[q] = jnp.broadcast_to(
            1.0 / jnp.where(inside, row_w[1:2] * cw[1:2], 1.0), (8, span)
        )

    send_later(below, jnp.logical_not(hurry))

    load_out.wait()
    wo32[...] = jnp.zeros(wo32.shape, F32)
    wo32[:, 0 : wo.shape[1], :] = wo[...].astype(F32)
    loads[6].wait()
    out_mid = wm.shape[1]
    for t in range(9):
        turned = wm[BY_COLUMN[t]].T
        for n in range(out_mid // 128):
            at = 128 * (9 * n + t)
            wmt[:, at : at + 128] = turned[:, 128 * n : 128 * (n + 1)]
    loads[7].wait()
    out_low = wl.shape[1]
    for t in range(9):
        wlt[:, out_low * t : out_low * (t + 1)] = wl[BY_COLUMN[t]].T

    where_b = iota((4, half), 1) % side_cells
    lower_half = iota((4, half), 1) < half // 2
    place_src, place_dst = iota((4 * half, inner), 0), iota((4 * half, inner), 1)
    place = place_dst == 4 * (place_src % side_cells - HALO) + place_src // half
    places[0] = place.astype(F32).astype(BF16)
    slot = place_src % side_cells
    from_left = place_dst == 4 * (slot % HALO) + slot // HALO
    from_right = place_dst == 4 * (tile - HALO + slot % HALO) + slot // HALO
    pair_q = 2 * (place_src // half - 2) + place_src % half // (half // 2)
    from_pair = place_dst == 4 * (slot - HALO) + pair_q
    part = place_src // half
    places[1] = jnp.where(
        part == 0, from_left.astype(F32), jnp.where(part == 1, from_right.astype(F32), from_pair.astype(F32))
    ).astype(BF16)
    for h in range(2):
        here = [inverse[q, 0:4, h * half : (h + 1) * half] for q in range(4)]
        sides = []
        for rim in (HALO, tile):
            dense = pltpu.roll(here[0], (half - rim) % half, 1)
            for q in range(1, 4):
                turned = pltpu.roll(here[q], (HALO * q - rim) % half, 1)
                dense = jnp.where(where_b // HALO == q, turned, dense)
            sides.append(dense)
        for pair in range(2):
            even, odds = here[2 * pair], here[2 * pair + 1]
            if h == 0:
                even = pltpu.roll(even, half // 2, 1)
            else:
                odds = pltpu.roll(odds, half // 2, 1)
            sides.append(jnp.where(lower_half, even, odds))
        for n, side in enumerate(sides):
            scales[h, n] = side

    for_all(lambda n, m: batch(cells, n, send1, recv1).wait_recv())

    cell = [cells[k].astype(F32) for k in range(9)]
    pieces = [[], [], []]
    for c in range(chans):
        for j, cut in enumerate((slice(tile - HALO, tile), slice(0, tile), slice(0, HALO))):
            upper, middle, lower = (cell[3 * i + j][c][:, cut] for i in range(3))
            zero = jnp.zeros((1, middle.shape[1]), F32)
            upper, lower = upper[tile - HALO :], lower[:HALO]
            pieces[0].append(jnp.concatenate([zero, upper, middle, lower[:-1]], axis=0))
            pieces[1].append(jnp.concatenate([upper, middle, lower], axis=0))
            pieces[2].append(jnp.concatenate([upper[1:], middle, lower, zero], axis=0))
    pieces = pieces[0] + pieces[1] + pieces[2]
    tall = jnp.concatenate(pieces + [jnp.zeros((side_cells, 128 - 3 * wide), F32)], axis=1)
    shape = (side_cells, side_cells, 128)
    spreaded = jnp.broadcast_to(tall[:, None, :], shape)
    gap = iota(shape, 2) % side_cells - iota(shape, 1)
    patches = [jnp.where(gap == dx - 1, spreaded, 0.0) for dx in range(3)]
    patches = jnp.concatenate(patches, axis=2).reshape(-1, 384).astype(BF16)
    first = dot(patches, wc[...]).reshape(side_cells, side_cells, -1)
    (first,) = group_silu([first], first.shape[2] // NGROUPS)
    first = first.reshape(side_cells * side_cells, -1).astype(BF16)

    taps = dot(first, wmt[...])
    chunks = []
    for n in range(out_mid // 128):
        part = [
            taps[:, 128 * (9 * n + t) : 128 * (9 * n + t + 1)].reshape(side_cells, side_cells, -1)
            for t in BY_COLUMN
        ]
        part = conv_up([[part]], 1)
        part = [part[py][px] for py in range(2) for px in range(2)]
        chunks.append(group_silu(part, out_mid // NGROUPS))
    second = [jnp.concatenate(parts, axis=2) for parts in zip(*chunks)]
    second = jnp.concatenate(second, axis=0)
    second = second.reshape(-1, second.shape[2]).astype(BF16)

    n = side_cells * side_cells
    products = dot(second, wlt[...])
    products = [products[:, out_low * t : out_low * (t + 1)] for t in BY_COLUMN]
    taps = [
        [
            [
                p[(2 * py + px) * n : (2 * py + px + 1) * n].reshape(side_cells, side_cells, -1)
                for p in products
            ]
            for px in range(2)
        ]
        for py in range(2)
    ]
    third = conv_up(taps, 2)
    third = [third[qy][qx] for qy in range(4) for qx in range(4)]
    terms = group_terms(third, out_low // NGROUPS)

    wo72 = wo32[...].reshape(72, wo32.shape[2]).astype(BF16)
    def colours(lo, hi):
        got = []
        for pair in range(2):
            rows = [
                jnp.stack([silu(third[4 * qy + qx][lo:hi], terms) for qy in range(4)], axis=1)
                for qx in (2 * pair, 2 * pair + 1)
            ]
            rows = jnp.concatenate([r.reshape(-1, r.shape[-1]) for r in rows], axis=0)
            both = nt_dot(wo72, rows.astype(BF16))
            got += [both[:, :half], both[:, half:]]
        return got

    def blended(colour, at):
        lanes = colour[0].shape[1]
        sub_b = iota((8, lanes), 1) % side_cells
        sub_r = iota((8, lanes), 1) // side_cells
        row_ok = [sub_r > 0, None, sub_r < lanes // side_cells - 1]
        col_ok = [sub_b > 0, None, sub_b < side_cells - 1]

        def tap(q, t):
            return colour[q][8 * t : 8 * t + 8]

        def moved(x, dy, dx):
            shift = (side_cells * (1 - dy) + 1 - dx) % lanes
            x = pltpu.roll(x, shift, 1) if shift else x
            ok = [m for m in (row_ok[dy], col_ok[dx]) if m is not None]
            return jnp.where(functools.reduce(jnp.logical_and, ok), x, 0.0) if ok else x

        values = []
        for q in range(4):
            value = None
            for dy in range(3):
                near = tap(q, 3 * dy + 1)
                if q > 0:
                    near = near + tap(q - 1, 3 * dy)
                if q < 3:
                    near = near + tap(q + 1, 3 * dy + 2)
                term = moved(near, dy, 1)
                if q == 0:
                    term = term + moved(tap(3, 3 * dy), dy, 0)
                if q == 3:
                    term = term + moved(tap(0, 3 * dy + 2), dy, 2)
                value = term if value is None else value + term
            values.append(value * blend[q, :, at : at + lanes])
        return values

    def pack_side(x, rim):
        dense = pltpu.roll(x[0], (half - rim) % half, 1)
        for q in range(1, 4):
            turned = pltpu.roll(x[q], (HALO * q - rim) % half, 1)
            dense = jnp.where(where_b // HALO == q, turned, dense)
        return dense

    def pack_pair(x, pair, h):
        even, odds = x[2 * pair], x[2 * pair + 1]
        if h == 0:
            odds = pltpu.roll(odds, half // 2, 1)
        else:
            even = pltpu.roll(even, half // 2, 1)
        return jnp.where(lower_half, even, odds)

    def send_rims(wanted):
        for k, (dr, dc) in FAR_FIRST:
            if wanted(dr):

                @pl.when(exists(dr, dc))
                def _():
                    copies(k, dr, dc)[1].start()

    middle = side_cells // 2
    upper = colours(0, middle)
    up_rows = [v[0:4] for v in blended(upper, 0)]
    for k, rim in ((0, 0), (1, side_cells - HALO)):
        up_out[k] = pack_side(up_rows, rim)
    for pair in range(2):
        vert_out[0, pair] = pack_pair(up_rows, pair, 0)
    send_rims(lambda dr: dr < 0)
    for_all(lambda n, m: batch(cells, n, send1, recv1).wait_send())

    lower = colours(middle, side_cells)
    both = [jnp.concatenate([a, b], axis=1) for a, b in zip(upper, lower)]
    values = blended(both, 0)
    for h in range(2):
        here = [v[0:4, h * half : (h + 1) * half] for v in values]
        for q in range(4):
            own[h, q] = here[q]
        for k, rim in ((0, 0), (1, side_cells - HALO)):
            side_out[k, h] = pack_side(here, rim)
        if h == 1:
            for pair in range(2):
                vert_out[h, pair] = pack_pair(here, pair, h)
    send_rims(lambda dr: dr >= 0)

    lane_row = iota((8, half), 1) // side_cells
    sublane = iota((8, half), 0)
    keep = [lane_row == sublane + 8, lane_row == sublane]
    beyond_row = [lane_row % 8 == sublane, lane_row % 8 == sublane]

    def spread_rows(piece, c, mask):
        return jnp.where(mask, jnp.broadcast_to(piece[c : c + 1], (8, half)), 0.0)

    def placed(blocks, place):
        tall = jnp.concatenate(blocks, axis=0)
        top = tall.astype(BF16)
        low = (tall - top.astype(F32)).astype(BF16)
        got = dot(jnp.concatenate([top, low], axis=0), place)
        return got[: tall.shape[0]] + got[tall.shape[0] :]

    blocks = []
    for c in range(3):
        for h in range(2):
            mine = [own[h, q] * inverse[q, 0:4, h * half : (h + 1) * half] for q in range(4)]
            blocks.append(jnp.concatenate([spread_rows(p, c, keep[h]) for p in mine], axis=1))
    mine = placed(blocks, places[0])

    for_all(lambda n, m: batch(rims, m, send2, recv2).wait_recv())

    blocks = []
    for c in range(3):
        for h in range(2):
            got = [
                (rims[h] + rims[4 + h]) * scales[h, 0],
                (rims[2 + h] + rims[6 + h]) * scales[h, 1],
                rims[8 + 2 * h] * scales[h, 2],
                rims[9 + 2 * h] * scales[h, 3],
            ]
            masks = [keep[h], keep[h], beyond_row[h], beyond_row[h]]
            blocks.append(
                jnp.concatenate([spread_rows(p, c, m) for p, m in zip(got, masks)], axis=1)
            )
    out[...] = (mine + placed(blocks, places[1])).reshape(3, inner, inner)

    for_all(lambda n, m: batch(rims, m, send2, recv2).wait_send())


def kernel(nr, nc, *refs):
    def scoped(local_sem):
        body(nr, nc, *refs, local_sem)

    pl.run_scoped(scoped, pltpu.SemaphoreType.DMA((6,)))


def solution(mesh):
    nr, nc = mesh.shape["rows"], mesh.shape["cols"]

    def per_device(lat, w_in, w_mid, w_low, w_out, ramp_r, ramp_c, lim_r, lim_c):
        tile = lat.shape[1]
        inner = 4 * tile
        size = inner + 8 * HALO
        half = size * (tile + 2 * HALO) // 2
        anywhere = pl.BlockSpec(memory_space=pltpu.HBM)
        dma = pltpu.SemaphoreType.DMA
        return pl.pallas_call(
            functools.partial(kernel, nr, nc),
            out_shape=pltpu.VMEM((w_out.shape[1], inner, inner), F32),
            in_specs=[anywhere] * 9,
            out_specs=pl.BlockSpec(memory_space=pltpu.VMEM),
            scratch_shapes=[
                pltpu.VMEM((max(9, 6 + 2 * (lat.shape[1] // HALO)),) + lat.shape, BF16),
                pltpu.VMEM(w_in.shape, BF16),
                pltpu.VMEM(w_mid.shape, BF16),
                pltpu.VMEM(w_low.shape, BF16),
                pltpu.VMEM(w_out.shape, BF16),
                pltpu.VMEM((2,) + ramp_r.shape, jnp.int32),
                pltpu.SMEM((2,) + lim_r.shape, jnp.int32),
                pltpu.VMEM((9, 8, w_in.shape[2]), F32),
                pltpu.VMEM((9, 8, w_out.shape[2]), F32),
                pltpu.VMEM((384, w_in.shape[2]), BF16),
                pltpu.VMEM((w_mid.shape[2], 9 * w_mid.shape[1]), BF16),
                pltpu.VMEM((w_low.shape[2], 9 * w_low.shape[1]), BF16),
                pltpu.VMEM((4, 8, 2 * half), F32),
                pltpu.VMEM((4, 8, 2 * half), F32),
                pltpu.VMEM((2, 4 * half, inner), BF16),
                pltpu.VMEM((2, 4, 4, half), F32),
                pltpu.VMEM((2, 4, 4, half), F32),
                pltpu.VMEM((2, 4, half), F32),
                pltpu.VMEM((2, 2, 4, half), F32),
                pltpu.VMEM((2, 2, 4, half), F32),
                pltpu.VMEM((12, 4, half), F32),
                pltpu.SemaphoreType.REGULAR((5,)),
                dma,
                dma,
            ],
            compiler_params=pltpu.CompilerParams(
                collective_id=0, has_side_effects=True
            ),
            name="decode",
        )(lat, w_in, w_mid, w_low, w_out, ramp_r, ramp_c, lim_r, lim_c)

    return jax.shard_map(
        per_device,
        mesh=mesh,
        in_specs=(P(None, ("groups", "rows"), "cols"), P(), P(), P(), P(), P(), P(), P(), P()),
        out_specs=P(None, ("groups", "rows"), "cols"),
        check_vma=False,
    )
```

```python
import functools

import jax
import jax.numpy as jnp
from jax import lax
from jax.experimental import pallas as pl
from jax.experimental.pallas import tpu as pltpu
from jax.sharding import PartitionSpec as P

MESH = pl.DeviceIdType.MESH
NGROUPS = 32
HALO = 2
F32 = jnp.float32
BF16 = jnp.bfloat16
AROUND = [(dr, dc) for dr in (-1, 0, 1) for dc in (-1, 0, 1) if (dr, dc) != (0, 0)]
FAR_FIRST = sorted(enumerate(AROUND), key=lambda e: -abs(e[1][0]) - abs(e[1][1]))
BY_COLUMN = [3 * (t % 3) + t // 3 for t in range(9)]
READY = {k: n for n, k in enumerate((3, 4, 5, 6, 7))}


def iota(shape, dim):
    return lax.broadcasted_iota(jnp.int32, shape, dim)


def nt_dot(a, b):
    return lax.dot_general(a, b, (((1,), (1,)), ((), ())), preferred_element_type=F32)


def dot(a, b):
    return jnp.dot(a, b, preferred_element_type=F32)


def down(x):
    return jnp.concatenate([jnp.zeros_like(x[:1]), x[:-1]], axis=0)


def up(x):
    return jnp.concatenate([x[1:], jnp.zeros_like(x[:1])], axis=0)


def right(x):
    rolled = pltpu.roll(x, 1, 1)
    return jnp.where(iota(x.shape, 1) == 0, 0.0, rolled)


def left(x):
    n = x.shape[1]
    rolled = pltpu.roll(x, n - 1, 1)
    return jnp.where(iota(x.shape, 1) == n - 1, 0.0, rolled)


def expand(products, fine, before, after):
    out = []
    for q in range(fine):
        t0, t1, t2 = products[q]
        prev = products[q - 1][0] if q > 0 else before(products[fine - 1][0])
        nxt = products[q + 1][2] if q < fine - 1 else after(products[0][2])
        out.append(prev + (t1 + t2))
        out.append((t0 + t1) + nxt)
    return out


def conv_up(taps, fine):
    by_col = [
        [
            expand(
                [[taps[py][px][3 * dy + dx] for dy in range(3)] for py in range(fine)],
                fine,
                down,
                up,
            )
            for dx in range(3)
        ]
        for px in range(fine)
    ]
    return [
        expand(
            [[by_col[px][dx][qy] for dx in range(3)] for px in range(fine)],
            fine,
            right,
            left,
        )
        for qy in range(2 * fine)
    ]


def group_sum(x, width):
    lane = iota(x.shape, 1) % width
    parts = [x]
    for k in range(1, width):
        parts.append(jnp.where(lane >= k, pltpu.roll(x, k, 1), 0.0))
        parts.append(jnp.where(lane < width - k, pltpu.roll(x, x.shape[1] - k, 1), 0.0))
    while len(parts) > 1:
        parts = [functools.reduce(jnp.add, parts[k : k + 2]) for k in range(0, len(parts), 2)]
    return parts[0]


def group_terms(phases, width):
    channels = phases[0].shape[-1]
    count = channels // 128
    positions = len(phases) * phases[0].shape[0] * phases[0].shape[1]
    scale = 1.0 / (positions * width)
    total = jnp.sum(functools.reduce(jnp.add, phases), axis=(0, 1)).reshape(1, channels)
    squares = functools.reduce(jnp.add, [p * p for p in phases])
    squares = jnp.sum(squares, axis=(0, 1)).reshape(1, channels)
    rows = [x[:, k * 128 : (k + 1) * 128] for x in (total, squares) for k in range(count)]
    rows = jnp.concatenate(rows + [jnp.zeros((1, 128), F32)] * (8 - len(rows)), axis=0)
    got = group_sum(rows, width) * scale
    center = got[:count]
    spread = jnp.maximum(got[count : 2 * count] - center * center, 0.0)
    factor = 0.5 * lax.rsqrt(spread + 1e-06)
    offset = center * factor
    factor = jnp.concatenate([factor[k : k + 1] for k in range(count)], axis=1)[None]
    offset = jnp.concatenate([offset[k : k + 1] for k in range(count)], axis=1)[None]
    return factor, offset


def silu(p, terms):
    half = p * terms[0] - terms[1]
    return half + half * jnp.tanh(half)


def group_silu(phases, width):
    terms = group_terms(phases, width)
    return [silu(p, terms) for p in phases]


def table_rows(table, limits, index, count, margin, inner):
    size = table.shape[1]
    pos = iota((1, size), 1)
    far = jnp.maximum(jnp.maximum(margin - pos, pos - (margin + inner) + 1), 0)
    rows = []
    for d in (-1, 0, 1):
        here = index + d
        limit = limits[jnp.clip(here, 0, count - 1)]
        picked = jnp.where(iota(table.shape, 0) == here, table, 0.0)
        row = jnp.sum(picked, axis=0, keepdims=True)
        rows.append(jnp.where(far <= limit, row, 0.0))
    above, own, below = rows
    other = jnp.where(pos < inner, jnp.roll(above, inner, 1), jnp.roll(below, inner, 1))
    pair = jnp.concatenate([own, own + other, jnp.zeros((6, size), F32)], axis=0)
    return pair.astype(BF16)


def body(
    nr, nc, lat, w_in, w_mid, w_low, w_out, ramp_r, ramp_c, lim_r, lim_c, out,
    cells, lined, wi, wm, wl, wo, tables, limits, wi32, wo32, wc, wmt, wlt,
    blend, inverse, places, scales, own, up_out, side_out, vert_out, rims,
    ready, recv1, recv2, local_sem,
):
    row, col = lax.axis_index("rows"), lax.axis_index("cols")

    def exists(dr, dc):
        ok = None
        for d, here, n in ((dr, row, nr), (dc, col, nc)):
            test = None if d == 0 else (here > 0 if d < 0 else here < n - 1)
            if test is not None:
                ok = test if ok is None else jnp.logical_and(ok, test)
        return ok

    def device(dr, dc):
        return {"rows": row + dr, "cols": col + dc}

    loads = [
        pltpu.make_async_copy(src, dst, local_sem.at[k])
        for k, src, dst in [
            (0, lat, cells.at[4]),
            (1, w_in, wi),
            (2, ramp_r, tables.at[0]),
            (2, ramp_c, tables.at[1]),
            (3, lim_r, limits.at[0]),
            (3, lim_c, limits.at[1]),
            (4, w_mid, wm),
            (5, w_low, wl),
        ]
    ]
    load_out = pltpu.make_async_copy(w_out, wo, local_sem.at[1])
    send1, send2 = local_sem.at[0], local_sem.at[1]
    odd = col % 2 == 1

    def mutual(dr, dc):
        return jnp.logical_and(row == (0 if dr > 0 else 1), odd if dc > 0 else jnp.logical_not(odd))

    def leads(dr, dc):
        there = exists(dr, dc)
        return there if dr > 0 else jnp.logical_and(there, odd)

    def greets(dr, dc):
        there = exists(dr, dc)
        if dr < 0:
            return jnp.logical_and(there, mutual(dr, dc)) if dc else None
        return leads(dr, dc)

    def greeted_by(dr, dc):
        there = exists(dr, dc)
        if dr > 0:
            return jnp.logical_and(there, mutual(dr, dc)) if dc else None
        return there if dr < 0 else jnp.logical_and(there, jnp.logical_not(odd))

    def alone(test, other):
        return test if other is None else jnp.logical_and(test, jnp.logical_not(other))

    barrier = pltpu.get_barrier_semaphore()
    earlier = 0

    def greet(entries):
        for dr, dc in entries:
            test = greets(dr, dc)
            if test is not None:

                @pl.when(test)
                def _():
                    pl.semaphore_signal(
                        barrier, inc=1, device_id=device(dr, dc), device_id_type=MESH
                    )

    loads[0].start()
    greet([e for e in AROUND if e[0] < 0])
    for load in loads[1:]:
        load.start()
    greet([e for e in AROUND if e[0] >= 0])
    for dr, dc in AROUND:
        test = greeted_by(dr, dc)
        if test is not None:
            earlier += test.astype(jnp.int32)

    def slot_of(dr, dc):
        up_down, left_right = (dr + 1) // 2, (dc + 1) // 2
        if dr == 0:
            return rims.at[pl.ds(2 * left_right, 2)]
        if dc == 0:
            return rims.at[pl.ds(8 + 2 * up_down, 2)]
        return rims.at[4 + 2 * left_right + up_down]

    def packed(dr, dc):
        up_down, left_right = (dr + 1) // 2, (dc + 1) // 2
        if dr == 0:
            return side_out.at[left_right]
        if dc == 0:
            return vert_out.at[up_down]
        return up_out.at[left_right] if dr < 0 else side_out.at[left_right, 1]

    def rows_of(slot, dr):
        if dr == 0:
            return cells.at[slot]
        return cells.at[slot, :, pl.ds(0 if dr < 0 else lat.shape[1] - HALO, HALO)]

    def copies(k, dr, dc):
        first = pltpu.make_async_remote_copy(
            src_ref=rows_of(4, dr),
            dst_ref=rows_of((1 - dr) * 3 + 1 - dc, dr),
            send_sem=send1,
            recv_sem=recv1,
            device_id=device(dr, dc),
            device_id_type=MESH,
        )
        second = pltpu.make_async_remote_copy(
            src_ref=packed(dr, dc),
            dst_ref=slot_of(-dr, -dc),
            send_sem=send2,
            recv_sem=recv2,
            device_id=device(dr, dc),
            device_id_type=MESH,
        )
        return first, second

    above_below = (row > 0).astype(jnp.int32) + (row < nr - 1).astype(jnp.int32)
    beside = (col > 0).astype(jnp.int32) + (col < nc - 1).astype(jnp.int32)

    def for_all(wait):
        for v in range(min(nr, 2) - 1, min(nr, 3)):
            for h in range(min(nc, 2) - 1, min(nc, 3)):
                if v + h == 0:
                    continue

                @pl.when(jnp.logical_and(above_below == v, beside == h))
                def _():
                    wait(v + v * h + lat.shape[1] // HALO * h, 2 * (v + h) + v * h)

    def batch(ref, n, send, recv):
        part = ref.at[pl.ds(0, n), :, pl.ds(0, HALO)] if ref is cells else ref.at[pl.ds(0, n)]
        return pltpu.make_async_remote_copy(
            src_ref=part,
            dst_ref=part,
            send_sem=send,
            recv_sem=recv,
            device_id=device(0, 0),
            device_id_type=MESH,
        )

    for k, (dr, dc) in enumerate(AROUND):

        @pl.when(jnp.logical_not(exists(dr, dc)))
        def _():
            slot = cells.at[(1 + dr) * 3 + 1 + dc]
            slot[...] = jnp.zeros(slot.shape, BF16)
            pixels = slot_of(dr, dc)
            pixels[...] = jnp.zeros(pixels.shape, F32)

    @pl.when(earlier > 0)
    def _():
        pl.semaphore_wait(barrier, earlier)

    for k, (dr, dc) in FAR_FIRST:
        if dr <= 0:
            by = greeted_by(dr, dc)

            @pl.when(alone(by, greets(dr, dc) if dr * dc else None))
            def _():
                pl.semaphore_signal(
                    ready.at[READY[7 - k]], inc=1, device_id=device(dr, dc), device_id_type=MESH
                )

    loads[0].wait()
    for k, (dr, dc) in FAR_FIRST:
        by = greeted_by(dr, dc)
        if by is not None:

            @pl.when(by)
            def _():
                copies(k, dr, dc)[0].start()

    def send_later(entries, when=None):
        for k, (dr, dc) in entries:
            test = alone(leads(dr, dc), greeted_by(dr, dc) if dr else None)

            @pl.when(test if when is None else jnp.logical_and(test, when))
            def _():
                pl.semaphore_wait(ready.at[READY[k]], 1)
                copies(k, dr, dc)[0].start()

    below = [e for e in enumerate(AROUND) if e[1][0] > 0]
    hurry = jnp.logical_or(greeted_by(1, -1), greeted_by(1, 1))
    send_later(below, hurry)
    send_later([e for e in enumerate(AROUND) if e[1][0] == 0])

    tile = lat.shape[1]
    side_cells = tile + 2 * HALO
    margin, inner = 4 * HALO, 4 * tile
    size = inner + 2 * margin
    chans = lat.shape[0]
    span = size * side_cells
    half = span // 2
    wide = chans * side_cells

    loads[1].wait()
    load_out.start()
    wi32[...] = jnp.zeros(wi32.shape, F32)
    wi32[:, 0 : wi.shape[1], :] = wi[...].astype(F32)
    wi72 = wi32[...].reshape(72, wi32.shape[2]).astype(BF16)
    src, dst = iota((384, 72), 0), iota((384, 72), 1)
    pick = (
        (dst // 8 == 3 * (src % 128 // wide) + src // 128)
        & (dst % 8 == (src // side_cells) % chans)
        & (src % 128 < 3 * wide)
    )
    wc[...] = dot(pick.astype(F32).astype(BF16), wi72).astype(BF16)
    pltpu.make_async_copy(tables, tables, local_sem.at[2]).wait()
    pltpu.make_async_copy(limits, limits, local_sem.at[3]).wait()

    spread_r = (iota((size, span), 1) // side_cells == iota((size, span), 0)).astype(F32)
    spread_c = [
        (4 * (iota((size, span), 1) % side_cells) + q == iota((size, span), 0)).astype(F32)
        for q in range(4)
    ]
    spread_c = jnp.concatenate(spread_c, axis=1)
    row_w = dot(table_rows(tables[0].astype(F32), limits.at[0], row, nr, margin, inner), spread_r.astype(BF16))
    col_w = dot(table_rows(tables[1].astype(F32), limits.at[1], col, nc, margin, inner), spread_c.astype(BF16))
    lane = iota((1, span), 1)
    r_of, b_of = lane // side_cells, lane % side_cells
    inside = (
        (r_of >= margin) & (r_of < margin + inner) & (b_of >= HALO) & (b_of < HALO + tile)
    )
    for q in range(4):
        cw = col_w[:, q * span : (q + 1) * span]
        blend[q] = jnp.broadcast_to(row_w[0:1] * cw[0:1], (8, span))
        inverse[q] = jnp.broadcast_to(
            1.0 / jnp.where(inside, row_w[1:2] * cw[1:2], 1.0), (8, span)
        )

    send_later(below, jnp.logical_not(hurry))

    load_out.wait()
    wo32[...] = jnp.zeros(wo32.shape, F32)
    wo32[:, 0 : wo.shape[1], :] = wo[...].astype(F32)
    loads[6].wait()
    out_mid = wm.shape[1]
    for t in range(9):
        turned = wm[BY_COLUMN[t]].T
        for n in range(out_mid // 128):
            at = 128 * (9 * n + t)
            wmt[:, at : at + 128] = turned[:, 128 * n : 128 * (n + 1)]
    loads[7].wait()
    out_low = wl.shape[1]
    for t in range(9):
        wlt[:, out_low * t : out_low * (t + 1)] = wl[BY_COLUMN[t]].T

    where_b = iota((4, half), 1) % side_cells
    lower_half = iota((4, half), 1) < half // 2
    place_src, place_dst = iota((4 * half, inner), 0), iota((4 * half, inner), 1)
    place = place_dst == 4 * (place_src % side_cells - HALO) + place_src // half
    places[0] = place.astype(F32).astype(BF16)
    slot = place_src % side_cells
    from_left = place_dst == 4 * (slot % HALO) + slot // HALO
    from_right = place_dst == 4 * (tile - HALO + slot % HALO) + slot // HALO
    pair_q = 2 * (place_src // half - 2) + place_src % half // (half // 2)
    from_pair = place_dst == 4 * (slot - HALO) + pair_q
    part = place_src // half
    places[1] = jnp.where(
        part == 0, from_left.astype(F32), jnp.where(part == 1, from_right.astype(F32), from_pair.astype(F32))
    ).astype(BF16)
    for h in range(2):
        here = [inverse[q, 0:4, h * half : (h + 1) * half] for q in range(4)]
        sides = []
        for rim in (HALO, tile):
            dense = pltpu.roll(here[0], (half - rim) % half, 1)
            for q in range(1, 4):
                turned = pltpu.roll(here[q], (HALO * q - rim) % half, 1)
                dense = jnp.where(where_b // HALO == q, turned, dense)
            sides.append(dense)
        for pair in range(2):
            even, odds = here[2 * pair], here[2 * pair + 1]
            if h == 0:
                even = pltpu.roll(even, half // 2, 1)
            else:
                odds = pltpu.roll(odds, half // 2, 1)
            sides.append(jnp.where(lower_half, even, odds))
        for n, side in enumerate(sides):
            scales[h, n] = side

    lined[...] = jnp.zeros(lined.shape, F32)
    for_all(lambda n, m: batch(cells, n, send1, recv1).wait_recv())

    pieces = [[], [], []]
    cuts = (slice(tile - HALO, tile), slice(0, tile), slice(0, HALO))
    for c in range(chans):
        for j, cut in enumerate(cuts):
            at = 1
            for i in range(3):
                block = cells[3 * i + j, c].astype(F32)[cuts[i], :]
                lined[c, j, at : at + block.shape[0], 0:tile] = block
                at += block.shape[0]
            for dy in range(3):
                pieces[dy].append(lined[c, j, dy : dy + side_cells, cut])
    pieces = pieces[0] + pieces[1] + pieces[2]
    tall = jnp.concatenate(pieces + [jnp.zeros((side_cells, 128 - 3 * wide), F32)], axis=1)
    shape = (side_cells, side_cells, 128)
    spreaded = jnp.broadcast_to(tall[:, None, :], shape)
    gap = iota(shape, 2) % side_cells - iota(shape, 1)
    patches = [jnp.where(gap == dx - 1, spreaded, 0.0) for dx in range(3)]
    patches = jnp.concatenate(patches, axis=2).reshape(-1, 384).astype(BF16)
    first = dot(patches, wc[...]).reshape(side_cells, side_cells, -1)
    (first,) = group_silu([first], first.shape[2] // NGROUPS)
    first = first.reshape(side_cells * side_cells, -1).astype(BF16)

    taps = dot(first, wmt[...])
    chunks = []
    for n in range(out_mid // 128):
        part = [
            taps[:, 128 * (9 * n + t) : 128 * (9 * n + t + 1)].reshape(side_cells, side_cells, -1)
            for t in BY_COLUMN
        ]
        part = conv_up([[part]], 1)
        part = [part[py][px] for py in range(2) for px in range(2)]
        chunks.append(group_silu(part, out_mid // NGROUPS))
    second = [jnp.concatenate(parts, axis=2) for parts in zip(*chunks)]
    second = jnp.concatenate(second, axis=0)
    second = second.reshape(-1, second.shape[2]).astype(BF16)

    n = side_cells * side_cells
    products = dot(second, wlt[...])
    products = [products[:, out_low * t : out_low * (t + 1)] for t in BY_COLUMN]
    taps = [
        [
            [
                p[(2 * py + px) * n : (2 * py + px + 1) * n].reshape(side_cells, side_cells, -1)
                for p in products
            ]
            for px in range(2)
        ]
        for py in range(2)
    ]
    third = conv_up(taps, 2)
    third = [third[qy][qx] for qy in range(4) for qx in range(4)]
    terms = group_terms(third, out_low // NGROUPS)

    wo72 = wo32[...].reshape(72, wo32.shape[2]).astype(BF16)
    def colours(lo, hi):
        got = []
        for pair in range(2):
            rows = [
                jnp.stack([silu(third[4 * qy + qx][lo:hi], terms) for qy in range(4)], axis=1)
                for qx in (2 * pair, 2 * pair + 1)
            ]
            rows = jnp.concatenate([r.reshape(-1, r.shape[-1]) for r in rows], axis=0)
            both = nt_dot(wo72, rows.astype(BF16))
            got += [both[:, :half], both[:, half:]]
        return got

    def blended(colour, at):
        lanes = colour[0].shape[1]
        sub_b = iota((8, lanes), 1) % side_cells
        sub_r = iota((8, lanes), 1) // side_cells
        row_ok = [sub_r > 0, None, sub_r < lanes // side_cells - 1]
        col_ok = [sub_b > 0, None, sub_b < side_cells - 1]

        def tap(q, t):
            return colour[q][8 * t : 8 * t + 8]

        def moved(x, dy, dx):
            shift = (side_cells * (1 - dy) + 1 - dx) % lanes
            x = pltpu.roll(x, shift, 1) if shift else x
            ok = [m for m in (row_ok[dy], col_ok[dx]) if m is not None]
            return jnp.where(functools.reduce(jnp.logical_and, ok), x, 0.0) if ok else x

        values = []
        for q in range(4):
            value = None
            for dy in range(3):
                near = tap(q, 3 * dy + 1)
                if q > 0:
                    near = near + tap(q - 1, 3 * dy)
                if q < 3:
                    near = near + tap(q + 1, 3 * dy + 2)
                term = moved(near, dy, 1)
                if q == 0:
                    term = term + moved(tap(3, 3 * dy), dy, 0)
                if q == 3:
                    term = term + moved(tap(0, 3 * dy + 2), dy, 2)
                value = term if value is None else value + term
            values.append(value * blend[q, :, at : at + lanes])
        return values

    def pack_side(x, rim):
        dense = pltpu.roll(x[0], (half - rim) % half, 1)
        for q in range(1, 4):
            turned = pltpu.roll(x[q], (HALO * q - rim) % half, 1)
            dense = jnp.where(where_b // HALO == q, turned, dense)
        return dense

    def pack_pair(x, pair, h):
        even, odds = x[2 * pair], x[2 * pair + 1]
        if h == 0:
            odds = pltpu.roll(odds, half // 2, 1)
        else:
            even = pltpu.roll(even, half // 2, 1)
        return jnp.where(lower_half, even, odds)

    def send_rims(wanted):
        for k, (dr, dc) in FAR_FIRST:
            if wanted(dr):

                @pl.when(exists(dr, dc))
                def _():
                    copies(k, dr, dc)[1].start()

    middle = side_cells // 2
    upper = colours(0, middle)
    up_rows = [v[0:4] for v in blended(upper, 0)]
    for k, rim in ((0, 0), (1, side_cells - HALO)):
        up_out[k] = pack_side(up_rows, rim)
    for pair in range(2):
        vert_out[0, pair] = pack_pair(up_rows, pair, 0)
    send_rims(lambda dr: dr < 0)
    for_all(lambda n, m: batch(cells, n, send1, recv1).wait_send())

    lower = colours(middle, side_cells)
    both = [jnp.concatenate([a, b], axis=1) for a, b in zip(upper, lower)]
    values = blended(both, 0)
    for h in range(2):
        here = [v[0:4, h * half : (h + 1) * half] for v in values]
        for q in range(4):
            own[h, q] = here[q]
        for k, rim in ((0, 0), (1, side_cells - HALO)):
            side_out[k, h] = pack_side(here, rim)
        if h == 1:
            for pair in range(2):
                vert_out[h, pair] = pack_pair(here, pair, h)
    send_rims(lambda dr: dr >= 0)

    lane_row = iota((8, half), 1) // side_cells
    sublane = iota((8, half), 0)
    keep = [lane_row == sublane + 8, lane_row == sublane]
    beyond_row = [lane_row % 8 == sublane, lane_row % 8 == sublane]

    def spread_rows(piece, c, mask):
        return jnp.where(mask, jnp.broadcast_to(piece[c : c + 1], (8, half)), 0.0)

    def placed(blocks, place):
        tall = jnp.concatenate(blocks, axis=0)
        top = tall.astype(BF16)
        low = (tall - top.astype(F32)).astype(BF16)
        got = dot(jnp.concatenate([top, low], axis=0), place)
        return got[: tall.shape[0]] + got[tall.shape[0] :]

    blocks = []
    for c in range(3):
        for h in range(2):
            mine = [own[h, q] * inverse[q, 0:4, h * half : (h + 1) * half] for q in range(4)]
            blocks.append(jnp.concatenate([spread_rows(p, c, keep[h]) for p in mine], axis=1))
    mine = placed(blocks, places[0])

    for_all(lambda n, m: batch(rims, m, send2, recv2).wait_recv())

    blocks = []
    for c in range(3):
        for h in range(2):
            got = [
                (rims[h] + rims[4 + h]) * scales[h, 0],
                (rims[2 + h] + rims[6 + h]) * scales[h, 1],
                rims[8 + 2 * h] * scales[h, 2],
                rims[9 + 2 * h] * scales[h, 3],
            ]
            masks = [keep[h], keep[h], beyond_row[h], beyond_row[h]]
            blocks.append(
                jnp.concatenate([spread_rows(p, c, m) for p, m in zip(got, masks)], axis=1)
            )
    rest = dot(jnp.concatenate(blocks, axis=0).astype(BF16), places[1])
    out[...] = (mine + rest).reshape(3, inner, inner)

    for_all(lambda n, m: batch(rims, m, send2, recv2).wait_send())


def kernel(nr, nc, *refs):
    def scoped(local_sem):
        body(nr, nc, *refs, local_sem)

    pl.run_scoped(scoped, pltpu.SemaphoreType.DMA((6,)))


def solution(mesh):
    nr, nc = mesh.shape["rows"], mesh.shape["cols"]

    def per_device(lat, w_in, w_mid, w_low, w_out, ramp_r, ramp_c, lim_r, lim_c):
        tile = lat.shape[1]
        inner = 4 * tile
        size = inner + 8 * HALO
        half = size * (tile + 2 * HALO) // 2
        anywhere = pl.BlockSpec(memory_space=pltpu.HBM)
        dma = pltpu.SemaphoreType.DMA
        return pl.pallas_call(
            functools.partial(kernel, nr, nc),
            out_shape=pltpu.VMEM((w_out.shape[1], inner, inner), F32),
            in_specs=[anywhere] * 9,
            out_specs=pl.BlockSpec(memory_space=pltpu.VMEM),
            scratch_shapes=[
                pltpu.VMEM((max(9, 6 + 2 * (lat.shape[1] // HALO)),) + lat.shape, BF16),
                pltpu.VMEM((lat.shape[0], 3, 16, 128), F32),
                pltpu.VMEM(w_in.shape, BF16),
                pltpu.VMEM(w_mid.shape, BF16),
                pltpu.VMEM(w_low.shape, BF16),
                pltpu.VMEM(w_out.shape, BF16),
                pltpu.VMEM((2,) + ramp_r.shape, jnp.int32),
                pltpu.SMEM((2,) + lim_r.shape, jnp.int32),
                pltpu.VMEM((9, 8, w_in.shape[2]), F32),
                pltpu.VMEM((9, 8, w_out.shape[2]), F32),
                pltpu.VMEM((384, w_in.shape[2]), BF16),
                pltpu.VMEM((w_mid.shape[2], 9 * w_mid.shape[1]), BF16),
                pltpu.VMEM((w_low.shape[2], 9 * w_low.shape[1]), BF16),
                pltpu.VMEM((4, 8, 2 * half), F32),
                pltpu.VMEM((4, 8, 2 * half), F32),
                pltpu.VMEM((2, 4 * half, inner), BF16),
                pltpu.VMEM((2, 4, 4, half), F32),
                pltpu.VMEM((2, 4, 4, half), F32),
                pltpu.VMEM((2, 4, half), F32),
                pltpu.VMEM((2, 2, 4, half), F32),
                pltpu.VMEM((2, 2, 4, half), F32),
                pltpu.VMEM((12, 4, half), F32),
                pltpu.SemaphoreType.REGULAR((5,)),
                dma,
                dma,
            ],
            compiler_params=pltpu.CompilerParams(
                collective_id=0, has_side_effects=True
            ),
            name="decode",
        )(lat, w_in, w_mid, w_low, w_out, ramp_r, ramp_c, lim_r, lim_c)

    return jax.shard_map(
        per_device,
        mesh=mesh,
        in_specs=(P(None, ("groups", "rows"), "cols"), P(), P(), P(), P(), P(), P(), P(), P()),
        out_specs=P(None, ("groups", "rows"), "cols"),
        check_vma=False,
    )
```

```python
import functools

import jax
import jax.numpy as jnp
from jax import lax
from jax.experimental import pallas as pl
from jax.experimental.pallas import tpu as pltpu
from jax.sharding import PartitionSpec as P

MESH = pl.DeviceIdType.MESH
NGROUPS = 32
HALO = 2
F32 = jnp.float32
BF16 = jnp.bfloat16
AROUND = [(dr, dc) for dr in (-1, 0, 1) for dc in (-1, 0, 1) if (dr, dc) != (0, 0)]
FAR_FIRST = sorted(enumerate(AROUND), key=lambda e: -abs(e[1][0]) - abs(e[1][1]))
BY_COLUMN = [3 * (t % 3) + t // 3 for t in range(9)]
READY = {k: n for n, k in enumerate((3, 4, 5, 6, 7))}


def iota(shape, dim):
    return lax.broadcasted_iota(jnp.int32, shape, dim)


def nt_dot(a, b):
    return lax.dot_general(a, b, (((1,), (1,)), ((), ())), preferred_element_type=F32)


def dot(a, b):
    return jnp.dot(a, b, preferred_element_type=F32)


def down(x):
    return jnp.concatenate([jnp.zeros_like(x[:1]), x[:-1]], axis=0)


def up(x):
    return jnp.concatenate([x[1:], jnp.zeros_like(x[:1])], axis=0)


def right(x):
    rolled = pltpu.roll(x, 1, 1)
    return jnp.where(iota(x.shape, 1) == 0, 0.0, rolled)


def left(x):
    n = x.shape[1]
    rolled = pltpu.roll(x, n - 1, 1)
    return jnp.where(iota(x.shape, 1) == n - 1, 0.0, rolled)


def expand(products, fine, before, after):
    out = []
    for q in range(fine):
        t0, t1, t2 = products[q]
        prev = products[q - 1][0] if q > 0 else before(products[fine - 1][0])
        nxt = products[q + 1][2] if q < fine - 1 else after(products[0][2])
        out.append(prev + (t1 + t2))
        out.append((t0 + t1) + nxt)
    return out


def conv_up(taps, fine):
    by_col = [
        [
            expand(
                [[taps[py][px][3 * dy + dx] for dy in range(3)] for py in range(fine)],
                fine,
                down,
                up,
            )
            for dx in range(3)
        ]
        for px in range(fine)
    ]
    return [
        expand(
            [[by_col[px][dx][qy] for dx in range(3)] for px in range(fine)],
            fine,
            right,
            left,
        )
        for qy in range(2 * fine)
    ]


def group_sum(x, width):
    lane = iota(x.shape, 1) % width
    parts = [x]
    for k in range(1, width):
        parts.append(jnp.where(lane >= k, pltpu.roll(x, k, 1), 0.0))
        parts.append(jnp.where(lane < width - k, pltpu.roll(x, x.shape[1] - k, 1), 0.0))
    while len(parts) > 1:
        parts = [functools.reduce(jnp.add, parts[k : k + 2]) for k in range(0, len(parts), 2)]
    return parts[0]


def group_terms(phases, width):
    channels = phases[0].shape[-1]
    count = channels // 128
    positions = len(phases) * phases[0].shape[0] * phases[0].shape[1]
    scale = 1.0 / (positions * width)
    total = jnp.sum(functools.reduce(jnp.add, phases), axis=(0, 1)).reshape(1, channels)
    squares = functools.reduce(jnp.add, [p * p for p in phases])
    squares = jnp.sum(squares, axis=(0, 1)).reshape(1, channels)
    rows = [x[:, k * 128 : (k + 1) * 128] for x in (total, squares) for k in range(count)]
    rows = jnp.concatenate(rows + [jnp.zeros((1, 128), F32)] * (8 - len(rows)), axis=0)
    got = group_sum(rows, width) * scale
    center = got[:count]
    spread = jnp.maximum(got[count : 2 * count] - center * center, 0.0)
    factor = 0.5 * lax.rsqrt(spread + 1e-06)
    offset = center * factor
    factor = jnp.concatenate([factor[k : k + 1] for k in range(count)], axis=1)[None]
    offset = jnp.concatenate([offset[k : k + 1] for k in range(count)], axis=1)[None]
    return factor, offset


def silu(p, terms):
    half = p * terms[0] - terms[1]
    return half + half * jnp.tanh(half)


def group_silu(phases, width):
    terms = group_terms(phases, width)
    return [silu(p, terms) for p in phases]


def table_rows(table, limits, index, count, margin, inner):
    size = table.shape[1]
    pos = iota((1, size), 1)
    far = jnp.maximum(jnp.maximum(margin - pos, pos - (margin + inner) + 1), 0)
    rows = []
    for d in (-1, 0, 1):
        here = index + d
        limit = limits[jnp.clip(here, 0, count - 1)]
        picked = jnp.where(iota(table.shape, 0) == here, table, 0.0)
        row = jnp.sum(picked, axis=0, keepdims=True)
        rows.append(jnp.where(far <= limit, row, 0.0))
    above, own, below = rows
    other = jnp.where(pos < inner, jnp.roll(above, inner, 1), jnp.roll(below, inner, 1))
    pair = jnp.concatenate([own, own + other, jnp.zeros((6, size), F32)], axis=0)
    return pair.astype(BF16)


def body(
    nr, nc, lat, w_in, w_mid, w_low, w_out, ramp_r, ramp_c, lim_r, lim_c, out,
    cells, lined, wi, wm, wl, wo, tables, limits, wi32, wo32, wc, wmt, wlt,
    blend, inverse, places, blend_up, scales, own, side_out, vert_out, rims,
    ready, recv1, recv2, local_sem,
):
    row, col = lax.axis_index("rows"), lax.axis_index("cols")

    def exists(dr, dc):
        ok = None
        for d, here, n in ((dr, row, nr), (dc, col, nc)):
            test = None if d == 0 else (here > 0 if d < 0 else here < n - 1)
            if test is not None:
                ok = test if ok is None else jnp.logical_and(ok, test)
        return ok

    def device(dr, dc):
        return {"rows": row + dr, "cols": col + dc}

    loads = [
        pltpu.make_async_copy(src, dst, local_sem.at[k])
        for k, src, dst in [
            (0, lat, cells.at[4]),
            (1, w_in, wi),
            (2, ramp_r, tables.at[0]),
            (2, ramp_c, tables.at[1]),
            (3, lim_r, limits.at[0]),
            (3, lim_c, limits.at[1]),
            (4, w_mid, wm),
            (5, w_low, wl),
        ]
    ]
    load_out = pltpu.make_async_copy(w_out, wo, local_sem.at[1])
    send1, send2 = local_sem.at[0], local_sem.at[1]
    odd = col % 2 == 1

    def mutual(dr, dc):
        return jnp.logical_and(row == (0 if dr > 0 else 1), odd if dc > 0 else jnp.logical_not(odd))

    def leads(dr, dc):
        there = exists(dr, dc)
        return there if dr > 0 else jnp.logical_and(there, odd)

    def greets(dr, dc):
        there = exists(dr, dc)
        if dr < 0:
            return jnp.logical_and(there, mutual(dr, dc)) if dc else None
        return leads(dr, dc)

    def greeted_by(dr, dc):
        there = exists(dr, dc)
        if dr > 0:
            return jnp.logical_and(there, mutual(dr, dc)) if dc else None
        return there if dr < 0 else jnp.logical_and(there, jnp.logical_not(odd))

    def alone(test, other):
        return test if other is None else jnp.logical_and(test, jnp.logical_not(other))

    barrier = pltpu.get_barrier_semaphore()
    earlier = 0

    def greet(entries):
        for dr, dc in entries:
            test = greets(dr, dc)
            if test is not None:

                @pl.when(test)
                def _():
                    pl.semaphore_signal(
                        barrier, inc=1, device_id=device(dr, dc), device_id_type=MESH
                    )

    loads[0].start()
    greet([e for e in AROUND if e[0] < 0])
    for load in loads[1:]:
        load.start()
    greet([e for e in AROUND if e[0] >= 0])
    for dr, dc in AROUND:
        test = greeted_by(dr, dc)
        if test is not None:
            earlier += test.astype(jnp.int32)

    def slot_of(dr, dc):
        up_down, left_right = (dr + 1) // 2, (dc + 1) // 2
        if dr == 0:
            return rims.at[pl.ds(2 * left_right, 2)]
        if dc == 0:
            return rims.at[pl.ds(12 + 2 * up_down, 2)]
        return rims.at[pl.ds(4 + 4 * left_right + 2 * up_down, 2)]

    def packed(dr, dc):
        return side_out.at[(dc + 1) // 2] if dr == 0 else vert_out.at[(dr + 1) // 2]

    def rows_of(slot, dr):
        if dr == 0:
            return cells.at[slot]
        return cells.at[slot, :, pl.ds(0 if dr < 0 else lat.shape[1] - HALO, HALO)]

    def copies(k, dr, dc):
        first = pltpu.make_async_remote_copy(
            src_ref=rows_of(4, dr),
            dst_ref=rows_of((1 - dr) * 3 + 1 - dc, dr),
            send_sem=send1,
            recv_sem=recv1,
            device_id=device(dr, dc),
            device_id_type=MESH,
        )
        second = pltpu.make_async_remote_copy(
            src_ref=packed(dr, dc),
            dst_ref=slot_of(-dr, -dc),
            send_sem=send2,
            recv_sem=recv2,
            device_id=device(dr, dc),
            device_id_type=MESH,
        )
        return first, second

    above_below = (row > 0).astype(jnp.int32) + (row < nr - 1).astype(jnp.int32)
    beside = (col > 0).astype(jnp.int32) + (col < nc - 1).astype(jnp.int32)

    def for_all(wait):
        for v in range(min(nr, 2) - 1, min(nr, 3)):
            for h in range(min(nc, 2) - 1, min(nc, 3)):
                if v + h == 0:
                    continue

                @pl.when(jnp.logical_and(above_below == v, beside == h))
                def _():
                    wait(v + v * h + lat.shape[1] // HALO * h, 2 * (v + h + v * h))

    def batch(ref, n, send, recv):
        part = ref.at[pl.ds(0, n), :, pl.ds(0, HALO)] if ref is cells else ref.at[pl.ds(0, n)]
        return pltpu.make_async_remote_copy(
            src_ref=part,
            dst_ref=part,
            send_sem=send,
            recv_sem=recv,
            device_id=device(0, 0),
            device_id_type=MESH,
        )

    for k, (dr, dc) in enumerate(AROUND):

        @pl.when(jnp.logical_not(exists(dr, dc)))
        def _():
            slot = cells.at[(1 + dr) * 3 + 1 + dc]
            slot[...] = jnp.zeros(slot.shape, BF16)
            pixels = slot_of(dr, dc)
            pixels[...] = jnp.zeros(pixels.shape, BF16)

    @pl.when(earlier > 0)
    def _():
        pl.semaphore_wait(barrier, earlier)

    for k, (dr, dc) in FAR_FIRST:
        if dr <= 0:
            by = greeted_by(dr, dc)

            @pl.when(alone(by, greets(dr, dc) if dr * dc else None))
            def _():
                pl.semaphore_signal(
                    ready.at[READY[7 - k]], inc=1, device_id=device(dr, dc), device_id_type=MESH
                )

    loads[0].wait()
    for k, (dr, dc) in FAR_FIRST:
        by = greeted_by(dr, dc)
        if by is not None:

            @pl.when(by)
            def _():
                copies(k, dr, dc)[0].start()

    def send_later(entries, when=None):
        for k, (dr, dc) in entries:
            test = alone(leads(dr, dc), greeted_by(dr, dc) if dr else None)

            @pl.when(test if when is None else jnp.logical_and(test, when))
            def _():
                pl.semaphore_wait(ready.at[READY[k]], 1)
                copies(k, dr, dc)[0].start()

    below = [e for e in enumerate(AROUND) if e[1][0] > 0]
    hurry = jnp.logical_or(greeted_by(1, -1), greeted_by(1, 1))
    send_later(below, hurry)
    send_later([e for e in enumerate(AROUND) if e[1][0] == 0])

    tile = lat.shape[1]
    side_cells = tile + 2 * HALO
    margin, inner = 4 * HALO, 4 * tile
    size = inner + 2 * margin
    chans = lat.shape[0]
    span = size * side_cells
    half = span // 2
    wide = chans * side_cells

    loads[1].wait()
    load_out.start()
    wi32[...] = jnp.zeros(wi32.shape, F32)
    wi32[:, 0 : wi.shape[1], :] = wi[...].astype(F32)
    wi72 = wi32[...].reshape(72, wi32.shape[2]).astype(BF16)
    src, dst = iota((384, 72), 0), iota((384, 72), 1)
    pick = (
        (dst // 8 == 3 * (src % 128 // wide) + src // 128)
        & (dst % 8 == (src // side_cells) % chans)
        & (src % 128 < 3 * wide)
    )
    wc[...] = dot(pick.astype(F32).astype(BF16), wi72).astype(BF16)
    pltpu.make_async_copy(tables, tables, local_sem.at[2]).wait()
    pltpu.make_async_copy(limits, limits, local_sem.at[3]).wait()

    spread_r = (iota((size, span), 1) // side_cells == iota((size, span), 0)).astype(F32)
    spread_c = [
        (4 * (iota((size, span), 1) % side_cells) + q == iota((size, span), 0)).astype(F32)
        for q in range(4)
    ]
    spread_c = jnp.concatenate(spread_c, axis=1)
    row_w = dot(table_rows(tables[0].astype(F32), limits.at[0], row, nr, margin, inner), spread_r.astype(BF16))
    col_w = dot(table_rows(tables[1].astype(F32), limits.at[1], col, nc, margin, inner), spread_c.astype(BF16))
    lane = iota((1, span), 1)
    r_of, b_of = lane // side_cells, lane % side_cells
    inside = (
        (r_of >= margin) & (r_of < margin + inner) & (b_of >= HALO) & (b_of < HALO + tile)
    )
    for q in range(4):
        cw = col_w[:, q * span : (q + 1) * span]
        blend[q] = jnp.broadcast_to(row_w[0:1] * cw[0:1], (8, span))
        upper = jnp.broadcast_to((row_w[0:1] * cw[0:1])[:, :half], (8, half))
        blend_up[q] = pltpu.roll(upper, half // 2, 1) if q % 2 else upper
        inverse[q] = jnp.broadcast_to(
            1.0 / jnp.where(inside, row_w[1:2] * cw[1:2], 1.0), (8, span)
        )

    send_later(below, jnp.logical_not(hurry))

    load_out.wait()
    wo32[...] = jnp.zeros(wo32.shape, F32)
    wo32[:, 0 : wo.shape[1], :] = wo[...].astype(F32)
    loads[6].wait()
    out_mid = wm.shape[1]
    for t in range(9):
        turned = wm[BY_COLUMN[t]].T
        for n in range(out_mid // 128):
            at = 128 * (9 * n + t)
            wmt[:, at : at + 128] = turned[:, 128 * n : 128 * (n + 1)]
    loads[7].wait()
    out_low = wl.shape[1]
    for t in range(9):
        wlt[:, out_low * t : out_low * (t + 1)] = wl[BY_COLUMN[t]].T

    where_b = iota((4, half), 1) % side_cells
    lower_half = iota((4, half), 1) < half // 2
    place_src, place_dst = iota((4 * half, inner), 0), iota((4 * half, inner), 1)
    place = place_dst == 4 * (place_src % side_cells - HALO) + place_src // half
    places[0] = place.astype(F32).astype(BF16)
    slot = place_src % side_cells
    from_left = place_dst == 4 * (slot % HALO) + slot // HALO
    from_right = place_dst == 4 * (tile - HALO + slot % HALO) + slot // HALO
    pair_q = 2 * (place_src // half - 2) + place_src % half // (half // 2)
    beside_by = jnp.where(slot < HALO, tile, jnp.where(slot < HALO + tile, 0, -tile))
    from_pair = place_dst == 4 * (slot - HALO + beside_by) + pair_q
    part = place_src // half
    places[1] = jnp.where(
        part == 0, from_left.astype(F32), jnp.where(part == 1, from_right.astype(F32), from_pair.astype(F32))
    ).astype(BF16)
    for h in range(2):
        here = [inverse[q, 0:4, h * half : (h + 1) * half] for q in range(4)]
        sides = []
        for rim in (HALO, tile):
            dense = pltpu.roll(here[0], (half - rim) % half, 1)
            for q in range(1, 4):
                turned = pltpu.roll(here[q], (HALO * q - rim) % half, 1)
                dense = jnp.where(where_b // HALO == q, turned, dense)
            sides.append(dense)
        for pair in range(2):
            even, odds = here[2 * pair], here[2 * pair + 1]
            if h == 0:
                even = pltpu.roll(even, half // 2, 1)
            else:
                odds = pltpu.roll(odds, half // 2, 1)
            inner_scale = jnp.where(lower_half, even, odds)
            onward = pltpu.roll(inner_scale, half - tile, 1)
            back = pltpu.roll(inner_scale, tile, 1)
            outer_scale = jnp.where(where_b < HALO, onward, back)
            within = jnp.logical_and(where_b >= HALO, where_b < HALO + tile)
            sides.append(jnp.where(within, inner_scale, outer_scale))
        for n, side in enumerate(sides):
            scales[h, n] = side

    lined[...] = jnp.zeros(lined.shape, F32)
    for_all(lambda n, m: batch(cells, n, send1, recv1).wait_recv())

    pieces = [[], [], []]
    cuts = (slice(tile - HALO, tile), slice(0, tile), slice(0, HALO))
    for c in range(chans):
        for j, cut in enumerate(cuts):
            at = 1
            for i in range(3):
                block = cells[3 * i + j, c].astype(F32)[cuts[i], :]
                lined[c, j, at : at + block.shape[0], 0:tile] = block
                at += block.shape[0]
            for dy in range(3):
                pieces[dy].append(lined[c, j, dy : dy + side_cells, cut])
    pieces = pieces[0] + pieces[1] + pieces[2]
    tall = jnp.concatenate(pieces + [jnp.zeros((side_cells, 128 - 3 * wide), F32)], axis=1)
    shape = (side_cells, side_cells, 128)
    spreaded = jnp.broadcast_to(tall[:, None, :], shape)
    gap = iota(shape, 2) % side_cells - iota(shape, 1)
    patches = [jnp.where(gap == dx - 1, spreaded, 0.0) for dx in range(3)]
    patches = jnp.concatenate(patches, axis=2).reshape(-1, 384).astype(BF16)
    first = dot(patches, wc[...]).reshape(side_cells, side_cells, -1)
    (first,) = group_silu([first], first.shape[2] // NGROUPS)
    first = first.reshape(side_cells * side_cells, -1).astype(BF16)

    taps = dot(first, wmt[...])
    chunks = []
    for n in range(out_mid // 128):
        part = [
            taps[:, 128 * (9 * n + t) : 128 * (9 * n + t + 1)].reshape(side_cells, side_cells, -1)
            for t in BY_COLUMN
        ]
        part = conv_up([[part]], 1)
        part = [part[py][px] for py in range(2) for px in range(2)]
        chunks.append(group_silu(part, out_mid // NGROUPS))
    second = [jnp.concatenate(parts, axis=2) for parts in zip(*chunks)]
    second = jnp.concatenate(second, axis=0)
    second = second.reshape(-1, second.shape[2]).astype(BF16)

    n = side_cells * side_cells
    products = dot(second, wlt[...])
    products = [products[:, out_low * t : out_low * (t + 1)] for t in BY_COLUMN]
    taps = [
        [
            [
                p[(2 * py + px) * n : (2 * py + px + 1) * n].reshape(side_cells, side_cells, -1)
                for p in products
            ]
            for px in range(2)
        ]
        for py in range(2)
    ]
    third = conv_up(taps, 2)
    third = [third[qy][qx] for qy in range(4) for qx in range(4)]
    terms = group_terms(third, out_low // NGROUPS)

    wo72 = wo32[...].reshape(72, wo32.shape[2]).astype(BF16)
    def colours(lo, hi):
        got = []
        for pair in range(2):
            rows = [
                jnp.stack([silu(third[4 * qy + qx][lo:hi], terms) for qy in range(4)], axis=1)
                for qx in (2 * pair, 2 * pair + 1)
            ]
            rows = jnp.concatenate([r.reshape(-1, r.shape[-1]) for r in rows], axis=0)
            both = nt_dot(wo72, rows.astype(BF16))
            got += [both[:, :half], both[:, half:]]
        return got

    def blended(colour, weight, turn):
        lanes = colour[0].shape[1]
        def tap(q, t):
            return colour[q][8 * t : 8 * t + 8]

        def moved(x, dy, dx, by):
            at = (iota((8, lanes), 1) + lanes - by) % lanes
            sub_b, sub_r = at % side_cells, at // side_cells
            row_ok = [sub_r > 0, None, sub_r < lanes // side_cells - 1]
            col_ok = [sub_b > 0, None, sub_b < side_cells - 1]
            shift = (side_cells * (1 - dy) + 1 - dx + by) % lanes
            x = pltpu.roll(x, shift, 1) if shift else x
            ok = [m for m in (row_ok[dy], col_ok[dx]) if m is not None]
            return jnp.where(functools.reduce(jnp.logical_and, ok), x, 0.0) if ok else x

        values = []
        for q in range(4):
            value, by = None, turn * (q % 2)
            for dy in range(3):
                near = tap(q, 3 * dy + 1)
                if q > 0:
                    near = near + tap(q - 1, 3 * dy)
                if q < 3:
                    near = near + tap(q + 1, 3 * dy + 2)
                term = moved(near, dy, 1, by)
                if q == 0:
                    term = term + moved(tap(3, 3 * dy), dy, 0, by)
                if q == 3:
                    term = term + moved(tap(0, 3 * dy + 2), dy, 2, by)
                value = term if value is None else value + term
            values.append(value * weight[q])
        return values

    def pack_side(x, rim):
        dense = pltpu.roll(x[0], (half - rim) % half, 1)
        for q in range(1, 4):
            turned = pltpu.roll(x[q], (HALO * q - rim) % half, 1)
            dense = jnp.where(where_b // HALO == q, turned, dense)
        return dense

    def pack_pair(x, pair):
        even = pltpu.roll(x[2 * pair], half // 2, 1)
        return jnp.where(lower_half, even, x[2 * pair + 1])

    def send_rims(wanted):
        for k, (dr, dc) in FAR_FIRST:
            if wanted(dr):

                @pl.when(exists(dr, dc))
                def _():
                    copies(k, dr, dc)[1].start()

    middle = side_cells // 2
    upper = colours(0, middle)
    up_rows = [v[0:4] for v in blended(upper, blend_up, half // 2)]
    for pair in range(2):
        both = jnp.where(lower_half, up_rows[2 * pair], up_rows[2 * pair + 1])
        vert_out[0, pair] = both.astype(BF16)
    send_rims(lambda dr: dr < 0)
    for_all(lambda n, m: batch(cells, n, send1, recv1).wait_send())

    lower = colours(middle, side_cells)
    both = [jnp.concatenate([a, b], axis=1) for a, b in zip(upper, lower)]
    values = blended(both, blend, 0)
    for h in range(2):
        here = [v[0:4, h * half : (h + 1) * half] for v in values]
        for q in range(4):
            own[h, q] = here[q]
        for k, rim in ((0, 0), (1, side_cells - HALO)):
            side_out[k, h] = pack_side(here, rim).astype(BF16)
    for pair in range(2):
        vert_out[1, pair] = pack_pair(here, pair).astype(BF16)
    send_rims(lambda dr: dr >= 0)

    lane_row = iota((8, half), 1) // side_cells
    sublane = iota((8, half), 0)
    keep = [lane_row == sublane + 8, lane_row == sublane]
    beyond_row = [lane_row % 8 == sublane, lane_row % 8 == sublane]

    def spread_rows(piece, c, mask):
        return jnp.where(mask, jnp.broadcast_to(piece[c : c + 1], (8, half)), 0.0)

    def placed(blocks, place):
        tall = jnp.concatenate(blocks, axis=0)
        top = tall.astype(BF16)
        low = (tall - top.astype(F32)).astype(BF16)
        got = dot(jnp.concatenate([top, low], axis=0), place)
        return got[: tall.shape[0]] + got[tall.shape[0] :]

    blocks = []
    for c in range(3):
        for h in range(2):
            mine = [own[h, q] * inverse[q, 0:4, h * half : (h + 1) * half] for q in range(4)]
            blocks.append(jnp.concatenate([spread_rows(p, c, keep[h]) for p in mine], axis=1))
    mine = placed(blocks, places[0])

    for_all(lambda n, m: batch(rims, m, send2, recv2).wait_recv())

    blocks = []
    for c in range(3):
        for h in range(2):
            got = [
                rims[h].astype(F32) * scales[h, 0],
                rims[2 + h].astype(F32) * scales[h, 1],
            ]
            for pair in range(2):
                left, right, straight = (rims[at + 2 * h + pair].astype(F32) for at in (4, 8, 12))
                straight = jnp.where(where_b < HALO, right, straight)
                straight = jnp.where(where_b < HALO + tile, straight, left)
                got.append(straight * scales[h, 2 + pair])
            masks = [keep[h], keep[h], beyond_row[h], beyond_row[h]]
            blocks.append(
                jnp.concatenate([spread_rows(p, c, m) for p, m in zip(got, masks)], axis=1)
            )
    rest = dot(jnp.concatenate(blocks, axis=0).astype(BF16), places[1])
    out[...] = (mine + rest).reshape(3, inner, inner)

    for_all(lambda n, m: batch(rims, m, send2, recv2).wait_send())


def kernel(nr, nc, *refs):
    def scoped(local_sem):
        body(nr, nc, *refs, local_sem)

    pl.run_scoped(scoped, pltpu.SemaphoreType.DMA((6,)))


def solution(mesh):
    nr, nc = mesh.shape["rows"], mesh.shape["cols"]

    def per_device(lat, w_in, w_mid, w_low, w_out, ramp_r, ramp_c, lim_r, lim_c):
        tile = lat.shape[1]
        inner = 4 * tile
        size = inner + 8 * HALO
        half = size * (tile + 2 * HALO) // 2
        anywhere = pl.BlockSpec(memory_space=pltpu.HBM)
        dma = pltpu.SemaphoreType.DMA
        return pl.pallas_call(
            functools.partial(kernel, nr, nc),
            out_shape=pltpu.VMEM((w_out.shape[1], inner, inner), F32),
            in_specs=[anywhere] * 9,
            out_specs=pl.BlockSpec(memory_space=pltpu.VMEM),
            scratch_shapes=[
                pltpu.VMEM((max(9, 6 + 2 * (lat.shape[1] // HALO)),) + lat.shape, BF16),
                pltpu.VMEM((lat.shape[0], 3, 16, 128), F32),
                pltpu.VMEM(w_in.shape, BF16),
                pltpu.VMEM(w_mid.shape, BF16),
                pltpu.VMEM(w_low.shape, BF16),
                pltpu.VMEM(w_out.shape, BF16),
                pltpu.VMEM((2,) + ramp_r.shape, jnp.int32),
                pltpu.SMEM((2,) + lim_r.shape, jnp.int32),
                pltpu.VMEM((9, 8, w_in.shape[2]), F32),
                pltpu.VMEM((9, 8, w_out.shape[2]), F32),
                pltpu.VMEM((384, w_in.shape[2]), BF16),
                pltpu.VMEM((w_mid.shape[2], 9 * w_mid.shape[1]), BF16),
                pltpu.VMEM((w_low.shape[2], 9 * w_low.shape[1]), BF16),
                pltpu.VMEM((4, 8, 2 * half), F32),
                pltpu.VMEM((4, 8, 2 * half), F32),
                pltpu.VMEM((2, 4 * half, inner), BF16),
                pltpu.VMEM((4, 8, half), F32),
                pltpu.VMEM((2, 4, 4, half), F32),
                pltpu.VMEM((2, 4, 4, half), F32),
                pltpu.VMEM((2, 2, 4, half), BF16),
                pltpu.VMEM((2, 2, 4, half), BF16),
                pltpu.VMEM((16, 4, half), BF16),
                pltpu.SemaphoreType.REGULAR((5,)),
                dma,
                dma,
            ],
            compiler_params=pltpu.CompilerParams(
                collective_id=0, has_side_effects=True
            ),
            name="decode",
        )(lat, w_in, w_mid, w_low, w_out, ramp_r, ramp_c, lim_r, lim_c)

    return jax.shard_map(
        per_device,
        mesh=mesh,
        in_specs=(P(None, ("groups", "rows"), "cols"), P(), P(), P(), P(), P(), P(), P(), P()),
        out_specs=P(None, ("groups", "rows"), "cols"),
        check_vma=False,
    )
```

```python
import functools

import jax
import jax.numpy as jnp
from jax import lax
from jax.experimental import pallas as pl
from jax.experimental.pallas import tpu as pltpu
from jax.sharding import PartitionSpec as P

MESH = pl.DeviceIdType.MESH
NGROUPS = 32
HALO = 2
F32 = jnp.float32
BF16 = jnp.bfloat16
AROUND = [(dr, dc) for dr in (-1, 0, 1) for dc in (-1, 0, 1) if (dr, dc) != (0, 0)]
FAR_FIRST = sorted(enumerate(AROUND), key=lambda e: -abs(e[1][0]) - abs(e[1][1]))
BY_COLUMN = [3 * (t % 3) + t // 3 for t in range(9)]
READY = {k: n for n, k in enumerate((3, 4, 5, 6, 7))}


def iota(shape, dim):
    return lax.broadcasted_iota(jnp.int32, shape, dim)


def nt_dot(a, b):
    return lax.dot_general(a, b, (((1,), (1,)), ((), ())), preferred_element_type=F32)


def dot(a, b):
    return jnp.dot(a, b, preferred_element_type=F32)


def down(x):
    return jnp.concatenate([jnp.zeros_like(x[:1]), x[:-1]], axis=0)


def up(x):
    return jnp.concatenate([x[1:], jnp.zeros_like(x[:1])], axis=0)


def right(x):
    rolled = pltpu.roll(x, 1, 1)
    return jnp.where(iota(x.shape, 1) == 0, 0.0, rolled)


def left(x):
    n = x.shape[1]
    rolled = pltpu.roll(x, n - 1, 1)
    return jnp.where(iota(x.shape, 1) == n - 1, 0.0, rolled)


def expand(products, fine, before, after):
    out = []
    for q in range(fine):
        t0, t1, t2 = products[q]
        prev = products[q - 1][0] if q > 0 else before(products[fine - 1][0])
        nxt = products[q + 1][2] if q < fine - 1 else after(products[0][2])
        out.append(prev + (t1 + t2))
        out.append((t0 + t1) + nxt)
    return out


def conv_up(taps, fine):
    by_col = [
        [
            expand(
                [[taps[py][px][3 * dy + dx] for dy in range(3)] for py in range(fine)],
                fine,
                down,
                up,
            )
            for dx in range(3)
        ]
        for px in range(fine)
    ]
    return [
        expand(
            [[by_col[px][dx][qy] for dx in range(3)] for px in range(fine)],
            fine,
            right,
            left,
        )
        for qy in range(2 * fine)
    ]


def group_sum(x, width):
    lane = iota(x.shape, 1) % width
    parts = [x]
    for k in range(1, width):
        parts.append(jnp.where(lane >= k, pltpu.roll(x, k, 1), 0.0))
        parts.append(jnp.where(lane < width - k, pltpu.roll(x, x.shape[1] - k, 1), 0.0))
    while len(parts) > 1:
        parts = [functools.reduce(jnp.add, parts[k : k + 2]) for k in range(0, len(parts), 2)]
    return parts[0]


def group_terms(phases, width):
    channels = phases[0].shape[-1]
    count = channels // 128
    positions = len(phases) * phases[0].shape[0] * phases[0].shape[1]
    scale = 1.0 / (positions * width)
    total = jnp.sum(functools.reduce(jnp.add, phases), axis=(0, 1)).reshape(1, channels)
    squares = functools.reduce(jnp.add, [p * p for p in phases])
    squares = jnp.sum(squares, axis=(0, 1)).reshape(1, channels)
    rows = [x[:, k * 128 : (k + 1) * 128] for x in (total, squares) for k in range(count)]
    rows = jnp.concatenate(rows + [jnp.zeros((1, 128), F32)] * (8 - len(rows)), axis=0)
    got = group_sum(rows, width) * scale
    center = got[:count]
    spread = jnp.maximum(got[count : 2 * count] - center * center, 0.0)
    factor = 0.5 * lax.rsqrt(spread + 1e-06)
    offset = center * factor
    factor = jnp.concatenate([factor[k : k + 1] for k in range(count)], axis=1)[None]
    offset = jnp.concatenate([offset[k : k + 1] for k in range(count)], axis=1)[None]
    return factor, offset


def silu(p, terms):
    half = p * terms[0] - terms[1]
    return half + half * jnp.tanh(half)


def group_silu(phases, width):
    terms = group_terms(phases, width)
    return [silu(p, terms) for p in phases]


def table_rows(table, limits, index, count, margin, inner):
    size = table.shape[1]
    pos = iota((1, size), 1)
    far = jnp.maximum(jnp.maximum(margin - pos, pos - (margin + inner) + 1), 0)
    rows = []
    for d in (-1, 0, 1):
        here = index + d
        limit = limits[jnp.clip(here, 0, count - 1)]
        picked = jnp.where(iota(table.shape, 0) == here, table, 0.0)
        row = jnp.sum(picked, axis=0, keepdims=True)
        rows.append(jnp.where(far <= limit, row, 0.0))
    above, own, below = rows
    other = jnp.where(pos < inner, jnp.roll(above, inner, 1), jnp.roll(below, inner, 1))
    pair = jnp.concatenate([own, own + other, jnp.zeros((6, size), F32)], axis=0)
    return pair.astype(BF16)


def body(
    nr, nc, lat, w_in, w_mid, w_low, w_out, ramp_r, ramp_c, lim_r, lim_c, out,
    cells, lined, wi, wm, wl, wo, tables, limits, wi32, wo32, wc, wmt, wlt,
    blend, inverse, places, blend_up, scales, own, side_out, vert_out, rims,
    ready, recv1, recv2, local_sem,
):
    row, col = lax.axis_index("rows"), lax.axis_index("cols")

    def exists(dr, dc):
        ok = None
        for d, here, n in ((dr, row, nr), (dc, col, nc)):
            test = None if d == 0 else (here > 0 if d < 0 else here < n - 1)
            if test is not None:
                ok = test if ok is None else jnp.logical_and(ok, test)
        return ok

    def device(dr, dc):
        return {"rows": row + dr, "cols": col + dc}

    loads = [
        pltpu.make_async_copy(src, dst, local_sem.at[k])
        for k, src, dst in [
            (0, lat, cells.at[4]),
            (1, w_in, wi),
            (2, ramp_r, tables.at[0]),
            (2, ramp_c, tables.at[1]),
            (3, lim_r, limits.at[0]),
            (3, lim_c, limits.at[1]),
            (4, w_mid, wm),
            (5, w_low, wl),
        ]
    ]
    load_out = pltpu.make_async_copy(w_out, wo, local_sem.at[1])
    send1, send2 = local_sem.at[0], local_sem.at[1]
    odd = col % 2 == 1

    def mutual(dr, dc):
        return jnp.logical_and(row == (0 if dr > 0 else 1), odd if dc > 0 else jnp.logical_not(odd))

    def leads(dr, dc):
        there = exists(dr, dc)
        return there if dr > 0 else jnp.logical_and(there, odd)

    def greets(dr, dc):
        there = exists(dr, dc)
        if dr < 0:
            return jnp.logical_and(there, mutual(dr, dc)) if dc else None
        return leads(dr, dc)

    def greeted_by(dr, dc):
        there = exists(dr, dc)
        if dr > 0:
            return jnp.logical_and(there, mutual(dr, dc)) if dc else None
        return there if dr < 0 else jnp.logical_and(there, jnp.logical_not(odd))

    def alone(test, other):
        return test if other is None else jnp.logical_and(test, jnp.logical_not(other))

    barrier = pltpu.get_barrier_semaphore()
    earlier = 0

    def greet(entries):
        for dr, dc in entries:
            test = greets(dr, dc)
            if test is not None:

                @pl.when(test)
                def _():
                    pl.semaphore_signal(
                        barrier, inc=1, device_id=device(dr, dc), device_id_type=MESH
                    )

    loads[0].start()
    greet([e for e in AROUND if e[0] < 0])
    for load in loads[1:]:
        load.start()
    greet([e for e in AROUND if e[0] >= 0])
    for dr, dc in AROUND:
        test = greeted_by(dr, dc)
        if test is not None:
            earlier += test.astype(jnp.int32)

    def slot_of(dr, dc):
        up_down, left_right = (dr + 1) // 2, (dc + 1) // 2
        if dr == 0:
            return rims.at[pl.ds(2 * left_right, 2)]
        if dc == 0:
            return rims.at[pl.ds(12 + 2 * up_down, 2)]
        return rims.at[pl.ds(4 + 4 * left_right + 2 * up_down, 2)]

    def packed(dr, dc):
        return side_out.at[(dc + 1) // 2] if dr == 0 else vert_out.at[(dr + 1) // 2]

    def rows_of(slot, dr):
        if dr == 0:
            return cells.at[slot]
        return cells.at[slot, :, pl.ds(0 if dr < 0 else lat.shape[1] - HALO, HALO)]

    def copies(k, dr, dc):
        first = pltpu.make_async_remote_copy(
            src_ref=rows_of(4, dr),
            dst_ref=rows_of((1 - dr) * 3 + 1 - dc, dr),
            send_sem=send1,
            recv_sem=recv1,
            device_id=device(dr, dc),
            device_id_type=MESH,
        )
        second = pltpu.make_async_remote_copy(
            src_ref=packed(dr, dc),
            dst_ref=slot_of(-dr, -dc),
            send_sem=send2,
            recv_sem=recv2,
            device_id=device(dr, dc),
            device_id_type=MESH,
        )
        return first, second

    above_below = (row > 0).astype(jnp.int32) + (row < nr - 1).astype(jnp.int32)
    beside = (col > 0).astype(jnp.int32) + (col < nc - 1).astype(jnp.int32)

    def for_all(wait):
        for v in range(min(nr, 2) - 1, min(nr, 3)):
            for h in range(min(nc, 2) - 1, min(nc, 3)):
                if v + h == 0:
                    continue

                @pl.when(jnp.logical_and(above_below == v, beside == h))
                def _():
                    wait(v + v * h + lat.shape[1] // HALO * h, 2 * (v + h + v * h))

    def batch(ref, n, send, recv):
        part = ref.at[pl.ds(0, n), :, pl.ds(0, HALO)] if ref is cells else ref.at[pl.ds(0, n)]
        return pltpu.make_async_remote_copy(
            src_ref=part,
            dst_ref=part,
            send_sem=send,
            recv_sem=recv,
            device_id=device(0, 0),
            device_id_type=MESH,
        )

    for k, (dr, dc) in enumerate(AROUND):

        @pl.when(jnp.logical_not(exists(dr, dc)))
        def _():
            slot = cells.at[(1 + dr) * 3 + 1 + dc]
            slot[...] = jnp.zeros(slot.shape, BF16)
            pixels = slot_of(dr, dc)
            pixels[...] = jnp.zeros(pixels.shape, BF16)

    @pl.when(earlier > 0)
    def _():
        pl.semaphore_wait(barrier, earlier)

    hurry = jnp.logical_or(greeted_by(1, -1), greeted_by(1, 1))

    @pl.when(hurry)
    def _():
        loads[0].wait()
        for k, dc in ((7, 1), (5, -1)):

            @pl.when(greeted_by(1, dc))
            def _():
                copies(k, 1, dc)[0].start()

    for k, (dr, dc) in FAR_FIRST:
        if dr <= 0:
            by = greeted_by(dr, dc)

            @pl.when(alone(by, greets(dr, dc) if dr * dc else None))
            def _():
                pl.semaphore_signal(
                    ready.at[READY[7 - k]], inc=1, device_id=device(dr, dc), device_id_type=MESH
                )

    @pl.when(jnp.logical_not(hurry))
    def _():
        loads[0].wait()

    for k, (dr, dc) in FAR_FIRST:
        if dr <= 0:

            @pl.when(greeted_by(dr, dc))
            def _():
                copies(k, dr, dc)[0].start()

    def send_later(entries, when=None):
        for k, (dr, dc) in entries:
            test = alone(leads(dr, dc), greeted_by(dr, dc) if dr else None)

            @pl.when(test if when is None else jnp.logical_and(test, when))
            def _():
                pl.semaphore_wait(ready.at[READY[k]], 1)
                copies(k, dr, dc)[0].start()

    below = [e for e in enumerate(AROUND) if e[1][0] > 0]
    send_later(below, hurry)
    send_later([e for e in enumerate(AROUND) if e[1][0] == 0])

    tile = lat.shape[1]
    side_cells = tile + 2 * HALO
    margin, inner = 4 * HALO, 4 * tile
    size = inner + 2 * margin
    chans = lat.shape[0]
    span = size * side_cells
    half = span // 2
    wide = chans * side_cells

    loads[1].wait()
    load_out.start()
    wi32[...] = jnp.zeros(wi32.shape, F32)
    wi32[:, 0 : wi.shape[1], :] = wi[...].astype(F32)
    wi72 = wi32[...].reshape(72, wi32.shape[2]).astype(BF16)
    src, dst = iota((384, 72), 0), iota((384, 72), 1)
    pick = (
        (dst // 8 == 3 * (src % 128 // wide) + src // 128)
        & (dst % 8 == (src // side_cells) % chans)
        & (src % 128 < 3 * wide)
    )
    wc[...] = dot(pick.astype(F32).astype(BF16), wi72).astype(BF16)
    pltpu.make_async_copy(tables, tables, local_sem.at[2]).wait()
    pltpu.make_async_copy(limits, limits, local_sem.at[3]).wait()

    spread_r = (iota((size, span), 1) // side_cells == iota((size, span), 0)).astype(F32)
    spread_c = [
        (4 * (iota((size, span), 1) % side_cells) + q == iota((size, span), 0)).astype(F32)
        for q in range(4)
    ]
    spread_c = jnp.concatenate(spread_c, axis=1)
    row_w = dot(table_rows(tables[0].astype(F32), limits.at[0], row, nr, margin, inner), spread_r.astype(BF16))
    col_w = dot(table_rows(tables[1].astype(F32), limits.at[1], col, nc, margin, inner), spread_c.astype(BF16))
    lane = iota((1, span), 1)
    r_of, b_of = lane // side_cells, lane % side_cells
    inside = (
        (r_of >= margin) & (r_of < margin + inner) & (b_of >= HALO) & (b_of < HALO + tile)
    )
    for q in range(4):
        cw = col_w[:, q * span : (q + 1) * span]
        blend[q] = jnp.broadcast_to(row_w[0:1] * cw[0:1], (8, span))
        upper = jnp.broadcast_to((row_w[0:1] * cw[0:1])[:, :half], (8, half))
        blend_up[q] = pltpu.roll(upper, half // 2, 1) if q % 2 else upper
        inverse[q] = jnp.broadcast_to(
            1.0 / jnp.where(inside, row_w[1:2] * cw[1:2], 1.0), (8, span)
        )

    send_later(below, jnp.logical_not(hurry))

    load_out.wait()
    wo32[...] = jnp.zeros(wo32.shape, F32)
    wo32[:, 0 : wo.shape[1], :] = wo[...].astype(F32)
    loads[6].wait()
    out_mid = wm.shape[1]
    for t in range(9):
        turned = wm[BY_COLUMN[t]].T
        for n in range(out_mid // 128):
            at = 128 * (9 * n + t)
            wmt[:, at : at + 128] = turned[:, 128 * n : 128 * (n + 1)]
    loads[7].wait()
    out_low = wl.shape[1]
    for t in range(9):
        wlt[:, out_low * t : out_low * (t + 1)] = wl[BY_COLUMN[t]].T

    where_b = iota((4, half), 1) % side_cells
    lower_half = iota((4, half), 1) < half // 2
    place_src, place_dst = iota((4 * half, inner), 0), iota((4 * half, inner), 1)
    place = place_dst == 4 * (place_src % side_cells - HALO) + place_src // half
    places[0] = place.astype(F32).astype(BF16)
    slot = place_src % side_cells
    from_left = place_dst == 4 * (slot % HALO) + slot // HALO
    from_right = place_dst == 4 * (tile - HALO + slot % HALO) + slot // HALO
    pair_q = 2 * (place_src // half - 2) + place_src % half // (half // 2)
    beside_by = jnp.where(slot < HALO, tile, jnp.where(slot < HALO + tile, 0, -tile))
    from_pair = place_dst == 4 * (slot - HALO + beside_by) + pair_q
    part = place_src // half
    places[1] = jnp.where(
        part == 0, from_left.astype(F32), jnp.where(part == 1, from_right.astype(F32), from_pair.astype(F32))
    ).astype(BF16)
    for h in range(2):
        here = [inverse[q, 0:4, h * half : (h + 1) * half] for q in range(4)]
        sides = []
        for rim in (HALO, tile):
            dense = pltpu.roll(here[0], (half - rim) % half, 1)
            for q in range(1, 4):
                turned = pltpu.roll(here[q], (HALO * q - rim) % half, 1)
                dense = jnp.where(where_b // HALO == q, turned, dense)
            sides.append(dense)
        for pair in range(2):
            even, odds = here[2 * pair], here[2 * pair + 1]
            if h == 0:
                even = pltpu.roll(even, half // 2, 1)
            else:
                odds = pltpu.roll(odds, half // 2, 1)
            inner_scale = jnp.where(lower_half, even, odds)
            onward = pltpu.roll(inner_scale, half - tile, 1)
            back = pltpu.roll(inner_scale, tile, 1)
            outer_scale = jnp.where(where_b < HALO, onward, back)
            within = jnp.logical_and(where_b >= HALO, where_b < HALO + tile)
            sides.append(jnp.where(within, inner_scale, outer_scale))
        for n, side in enumerate(sides):
            scales[h, n] = side

    lined[...] = jnp.zeros(lined.shape, F32)
    for_all(lambda n, m: batch(cells, n, send1, recv1).wait_recv())

    pieces = [[], [], []]
    cuts = (slice(tile - HALO, tile), slice(0, tile), slice(0, HALO))
    for c in range(chans):
        for j, cut in enumerate(cuts):
            at = 1
            for i in range(3):
                block = cells[3 * i + j, c].astype(F32)[cuts[i], :]
                lined[c, j, at : at + block.shape[0], 0:tile] = block
                at += block.shape[0]
            for dy in range(3):
                pieces[dy].append(lined[c, j, dy : dy + side_cells, cut])
    pieces = pieces[0] + pieces[1] + pieces[2]
    tall = jnp.concatenate(pieces + [jnp.zeros((side_cells, 128 - 3 * wide), F32)], axis=1)
    shape = (side_cells, side_cells, 128)
    spreaded = jnp.broadcast_to(tall[:, None, :], shape)
    gap = iota(shape, 2) % side_cells - iota(shape, 1)
    patches = [jnp.where(gap == dx - 1, spreaded, 0.0) for dx in range(3)]
    patches = jnp.concatenate(patches, axis=2).reshape(-1, 384).astype(BF16)
    first = dot(patches, wc[...]).reshape(side_cells, side_cells, -1)
    (first,) = group_silu([first], first.shape[2] // NGROUPS)
    first = first.reshape(side_cells * side_cells, -1).astype(BF16)

    taps = dot(first, wmt[...])
    chunks = []
    for n in range(out_mid // 128):
        part = [
            taps[:, 128 * (9 * n + t) : 128 * (9 * n + t + 1)].reshape(side_cells, side_cells, -1)
            for t in BY_COLUMN
        ]
        part = conv_up([[part]], 1)
        part = [part[py][px] for py in range(2) for px in range(2)]
        chunks.append(group_silu(part, out_mid // NGROUPS))
    second = [jnp.concatenate(parts, axis=2) for parts in zip(*chunks)]
    second = jnp.concatenate(second, axis=0)
    second = second.reshape(-1, second.shape[2]).astype(BF16)

    n = side_cells * side_cells
    products = dot(second, wlt[...])
    products = [products[:, out_low * t : out_low * (t + 1)] for t in BY_COLUMN]
    taps = [
        [
            [
                p[(2 * py + px) * n : (2 * py + px + 1) * n].reshape(side_cells, side_cells, -1)
                for p in products
            ]
            for px in range(2)
        ]
        for py in range(2)
    ]
    third = conv_up(taps, 2)
    third = [third[qy][qx] for qy in range(4) for qx in range(4)]
    terms = group_terms(third, out_low // NGROUPS)

    wo72 = wo32[...].reshape(72, wo32.shape[2]).astype(BF16)
    def colours(lo, hi):
        got = []
        for pair in range(2):
            rows = [
                jnp.stack([silu(third[4 * qy + qx][lo:hi], terms) for qy in range(4)], axis=1)
                for qx in (2 * pair, 2 * pair + 1)
            ]
            rows = jnp.concatenate([r.reshape(-1, r.shape[-1]) for r in rows], axis=0)
            both = nt_dot(wo72, rows.astype(BF16))
            got += [both[:, :half], both[:, half:]]
        return got

    def blended(colour, weight, turn):
        lanes = colour[0].shape[1]
        def tap(q, t):
            return colour[q][8 * t : 8 * t + 8]

        def moved(x, dy, dx, by):
            at = (iota((8, lanes), 1) + lanes - by) % lanes
            sub_b, sub_r = at % side_cells, at // side_cells
            row_ok = [sub_r > 0, None, sub_r < lanes // side_cells - 1]
            col_ok = [sub_b > 0, None, sub_b < side_cells - 1]
            shift = (side_cells * (1 - dy) + 1 - dx + by) % lanes
            x = pltpu.roll(x, shift, 1) if shift else x
            ok = [m for m in (row_ok[dy], col_ok[dx]) if m is not None]
            return jnp.where(functools.reduce(jnp.logical_and, ok), x, 0.0) if ok else x

        values = []
        for q in range(4):
            value, by = None, turn * (q % 2)
            for dy in range(3):
                near = tap(q, 3 * dy + 1)
                if q > 0:
                    near = near + tap(q - 1, 3 * dy)
                if q < 3:
                    near = near + tap(q + 1, 3 * dy + 2)
                term = moved(near, dy, 1, by)
                if q == 0:
                    term = term + moved(tap(3, 3 * dy), dy, 0, by)
                if q == 3:
                    term = term + moved(tap(0, 3 * dy + 2), dy, 2, by)
                value = term if value is None else value + term
            values.append(value * weight[q])
        return values

    def pack_side(x, rim):
        dense = pltpu.roll(x[0], (half - rim) % half, 1)
        for q in range(1, 4):
            turned = pltpu.roll(x[q], (HALO * q - rim) % half, 1)
            dense = jnp.where(where_b // HALO == q, turned, dense)
        return dense

    def pack_pair(x, pair):
        even = pltpu.roll(x[2 * pair], half // 2, 1)
        return jnp.where(lower_half, even, x[2 * pair + 1])

    def send_rims(wanted):
        for k, (dr, dc) in FAR_FIRST:
            if wanted(dr):

                @pl.when(exists(dr, dc))
                def _():
                    copies(k, dr, dc)[1].start()

    middle = side_cells // 2
    upper = colours(0, middle)
    up_rows = [v[0:4] for v in blended(upper, blend_up, half // 2)]
    for pair in range(2):
        both = jnp.where(lower_half, up_rows[2 * pair], up_rows[2 * pair + 1])
        vert_out[0, pair] = both.astype(BF16)
    send_rims(lambda dr: dr < 0)
    for_all(lambda n, m: batch(cells, n, send1, recv1).wait_send())

    lower = colours(middle, side_cells)
    both = [jnp.concatenate([a, b], axis=1) for a, b in zip(upper, lower)]
    values = blended(both, blend, 0)
    for h in range(2):
        here = [v[0:4, h * half : (h + 1) * half] for v in values]
        for q in range(4):
            own[h, q] = here[q]
        for k, rim in ((0, 0), (1, side_cells - HALO)):
            side_out[k, h] = pack_side(here, rim).astype(BF16)
    for pair in range(2):
        vert_out[1, pair] = pack_pair(here, pair).astype(BF16)
    send_rims(lambda dr: dr >= 0)

    lane_row = iota((8, half), 1) // side_cells
    sublane = iota((8, half), 0)
    keep = [lane_row == sublane + 8, lane_row == sublane]
    beyond_row = [lane_row % 8 == sublane, lane_row % 8 == sublane]

    def spread_rows(piece, c, mask):
        return jnp.where(mask, jnp.broadcast_to(piece[c : c + 1], (8, half)), 0.0)

    def placed(blocks, place):
        tall = jnp.concatenate(blocks, axis=0)
        top = tall.astype(BF16)
        low = (tall - top.astype(F32)).astype(BF16)
        got = dot(jnp.concatenate([top, low], axis=0), place)
        return got[: tall.shape[0]] + got[tall.shape[0] :]

    blocks = []
    for c in range(3):
        for h in range(2):
            mine = [own[h, q] * inverse[q, 0:4, h * half : (h + 1) * half] for q in range(4)]
            blocks.append(jnp.concatenate([spread_rows(p, c, keep[h]) for p in mine], axis=1))
    mine = placed(blocks, places[0])

    for_all(lambda n, m: batch(rims, m, send2, recv2).wait_recv())

    blocks = []
    for c in range(3):
        for h in range(2):
            got = [
                rims[h].astype(F32) * scales[h, 0],
                rims[2 + h].astype(F32) * scales[h, 1],
            ]
            for pair in range(2):
                left, right, straight = (rims[at + 2 * h + pair].astype(F32) for at in (4, 8, 12))
                straight = jnp.where(where_b < HALO, right, straight)
                straight = jnp.where(where_b < HALO + tile, straight, left)
                got.append(straight * scales[h, 2 + pair])
            masks = [keep[h], keep[h], beyond_row[h], beyond_row[h]]
            blocks.append(
                jnp.concatenate([spread_rows(p, c, m) for p, m in zip(got, masks)], axis=1)
            )
    rest = dot(jnp.concatenate(blocks, axis=0).astype(BF16), places[1])
    out[...] = (mine + rest).reshape(3, inner, inner)

    for_all(lambda n, m: batch(rims, m, send2, recv2).wait_send())


def kernel(nr, nc, *refs):
    def scoped(local_sem):
        body(nr, nc, *refs, local_sem)

    pl.run_scoped(scoped, pltpu.SemaphoreType.DMA((6,)))


def solution(mesh):
    nr, nc = mesh.shape["rows"], mesh.shape["cols"]

    def per_device(lat, w_in, w_mid, w_low, w_out, ramp_r, ramp_c, lim_r, lim_c):
        tile = lat.shape[1]
        inner = 4 * tile
        size = inner + 8 * HALO
        half = size * (tile + 2 * HALO) // 2
        anywhere = pl.BlockSpec(memory_space=pltpu.HBM)
        dma = pltpu.SemaphoreType.DMA
        return pl.pallas_call(
            functools.partial(kernel, nr, nc),
            out_shape=pltpu.VMEM((w_out.shape[1], inner, inner), F32),
            in_specs=[anywhere] * 9,
            out_specs=pl.BlockSpec(memory_space=pltpu.VMEM),
            scratch_shapes=[
                pltpu.VMEM((max(9, 6 + 2 * (lat.shape[1] // HALO)),) + lat.shape, BF16),
                pltpu.VMEM((lat.shape[0], 3, 16, 128), F32),
                pltpu.VMEM(w_in.shape, BF16),
                pltpu.VMEM(w_mid.shape, BF16),
                pltpu.VMEM(w_low.shape, BF16),
                pltpu.VMEM(w_out.shape, BF16),
                pltpu.VMEM((2,) + ramp_r.shape, jnp.int32),
                pltpu.SMEM((2,) + lim_r.shape, jnp.int32),
                pltpu.VMEM((9, 8, w_in.shape[2]), F32),
                pltpu.VMEM((9, 8, w_out.shape[2]), F32),
                pltpu.VMEM((384, w_in.shape[2]), BF16),
                pltpu.VMEM((w_mid.shape[2], 9 * w_mid.shape[1]), BF16),
                pltpu.VMEM((w_low.shape[2], 9 * w_low.shape[1]), BF16),
                pltpu.VMEM((4, 8, 2 * half), F32),
                pltpu.VMEM((4, 8, 2 * half), F32),
                pltpu.VMEM((2, 4 * half, inner), BF16),
                pltpu.VMEM((4, 8, half), F32),
                pltpu.VMEM((2, 4, 4, half), F32),
                pltpu.VMEM((2, 4, 4, half), F32),
                pltpu.VMEM((2, 2, 4, half), BF16),
                pltpu.VMEM((2, 2, 4, half), BF16),
                pltpu.VMEM((16, 4, half), BF16),
                pltpu.SemaphoreType.REGULAR((5,)),
                dma,
                dma,
            ],
            compiler_params=pltpu.CompilerParams(
                collective_id=0, has_side_effects=True
            ),
            name="decode",
        )(lat, w_in, w_mid, w_low, w_out, ramp_r, ramp_c, lim_r, lim_c)

    return jax.shard_map(
        per_device,
        mesh=mesh,
        in_specs=(P(None, ("groups", "rows"), "cols"), P(), P(), P(), P(), P(), P(), P(), P()),
        out_specs=P(None, ("groups", "rows"), "cols"),
        check_vma=False,
    )
```

```python
import functools

import jax
import jax.numpy as jnp
from jax import lax
from jax.experimental import pallas as pl
from jax.experimental.pallas import tpu as pltpu
from jax.sharding import PartitionSpec as P

MESH = pl.DeviceIdType.MESH
NGROUPS = 32
HALO = 2
F32 = jnp.float32
BF16 = jnp.bfloat16
AROUND = [(dr, dc) for dr in (-1, 0, 1) for dc in (-1, 0, 1) if (dr, dc) != (0, 0)]
FAR_FIRST = sorted(enumerate(AROUND), key=lambda e: -abs(e[1][0]) - abs(e[1][1]))
BY_COLUMN = [3 * (t % 3) + t // 3 for t in range(9)]
READY = {3: 0, 4: 0, 5: 1, 6: 2, 7: 3}


def iota(shape, dim):
    return lax.broadcasted_iota(jnp.int32, shape, dim)


def nt_dot(a, b):
    return lax.dot_general(a, b, (((1,), (1,)), ((), ())), preferred_element_type=F32)


def dot(a, b):
    return jnp.dot(a, b, preferred_element_type=F32)


def down(x):
    return jnp.concatenate([jnp.zeros_like(x[:1]), x[:-1]], axis=0)


def up(x):
    return jnp.concatenate([x[1:], jnp.zeros_like(x[:1])], axis=0)


def right(x):
    rolled = pltpu.roll(x, 1, 1)
    return jnp.where(iota(x.shape, 1) == 0, 0.0, rolled)


def left(x):
    n = x.shape[1]
    rolled = pltpu.roll(x, n - 1, 1)
    return jnp.where(iota(x.shape, 1) == n - 1, 0.0, rolled)


def expand(products, fine, before, after):
    out = []
    for q in range(fine):
        t0, t1, t2 = products[q]
        prev = products[q - 1][0] if q > 0 else before(products[fine - 1][0])
        nxt = products[q + 1][2] if q < fine - 1 else after(products[0][2])
        out.append(prev + (t1 + t2))
        out.append((t0 + t1) + nxt)
    return out


def conv_up(taps, fine):
    by_col = [
        [
            expand(
                [[taps[py][px][3 * dy + dx] for dy in range(3)] for py in range(fine)],
                fine,
                down,
                up,
            )
            for dx in range(3)
        ]
        for px in range(fine)
    ]
    return [
        expand(
            [[by_col[px][dx][qy] for dx in range(3)] for px in range(fine)],
            fine,
            right,
            left,
        )
        for qy in range(2 * fine)
    ]


def group_sum(x, width):
    lane = iota(x.shape, 1) % width
    parts = [x]
    for k in range(1, width):
        parts.append(jnp.where(lane >= k, pltpu.roll(x, k, 1), 0.0))
        parts.append(jnp.where(lane < width - k, pltpu.roll(x, x.shape[1] - k, 1), 0.0))
    while len(parts) > 1:
        parts = [functools.reduce(jnp.add, parts[k : k + 2]) for k in range(0, len(parts), 2)]
    return parts[0]


def group_terms(phases, width):
    channels = phases[0].shape[-1]
    count = channels // 128
    positions = len(phases) * phases[0].shape[0] * phases[0].shape[1]
    scale = 1.0 / (positions * width)
    total = jnp.sum(functools.reduce(jnp.add, phases), axis=(0, 1)).reshape(1, channels)
    squares = functools.reduce(jnp.add, [p * p for p in phases])
    squares = jnp.sum(squares, axis=(0, 1)).reshape(1, channels)
    rows = [x[:, k * 128 : (k + 1) * 128] for x in (total, squares) for k in range(count)]
    rows = jnp.concatenate(rows + [jnp.zeros((1, 128), F32)] * (8 - len(rows)), axis=0)
    got = group_sum(rows, width) * scale
    center = got[:count]
    spread = jnp.maximum(got[count : 2 * count] - center * center, 0.0)
    factor = 0.5 * lax.rsqrt(spread + 1e-06)
    offset = center * factor
    factor = jnp.concatenate([factor[k : k + 1] for k in range(count)], axis=1)[None]
    offset = jnp.concatenate([offset[k : k + 1] for k in range(count)], axis=1)[None]
    return factor, offset


def silu(p, terms):
    half = p * terms[0] - terms[1]
    return half + half * jnp.tanh(half)


def group_silu(phases, width):
    terms = group_terms(phases, width)
    return [silu(p, terms) for p in phases]


def table_rows(table, limits, index, count, margin, inner):
    size = table.shape[1]
    pos = iota((1, size), 1)
    far = jnp.maximum(jnp.maximum(margin - pos, pos - (margin + inner) + 1), 0)
    rows = []
    for d in (-1, 0, 1):
        here = index + d
        limit = limits[jnp.clip(here, 0, count - 1)]
        picked = jnp.where(iota(table.shape, 0) == here, table, 0.0)
        row = jnp.sum(picked, axis=0, keepdims=True)
        rows.append(jnp.where(far <= limit, row, 0.0))
    above, own, below = rows
    other = jnp.where(pos < inner, jnp.roll(above, inner, 1), jnp.roll(below, inner, 1))
    pair = jnp.concatenate([own, own + other, jnp.zeros((6, size), F32)], axis=0)
    return pair.astype(BF16)


def body(
    nr, nc, lat, w_in, w_mid, w_low, w_out, ramp_r, ramp_c, lim_r, lim_c, out,
    cells, lined, wi, wm, wl, wo, tables, limits, wi32, wo32, wc, wmt, wlt,
    blend, inverse, places, blend_up, scales, own, side_out, vert_out, rims,
    ready, recv1, recv2, local_sem,
):
    row, col = lax.axis_index("rows"), lax.axis_index("cols")

    def exists(dr, dc):
        ok = None
        for d, here, n in ((dr, row, nr), (dc, col, nc)):
            test = None if d == 0 else (here > 0 if d < 0 else here < n - 1)
            if test is not None:
                ok = test if ok is None else jnp.logical_and(ok, test)
        return ok

    def device(dr, dc):
        return {"rows": row + dr, "cols": col + dc}

    loads = [
        pltpu.make_async_copy(src, dst, local_sem.at[k])
        for k, src, dst in [
            (0, lat, cells.at[4]),
            (1, w_in, wi),
            (2, ramp_r, tables.at[0]),
            (2, ramp_c, tables.at[1]),
            (3, lim_r, limits.at[0]),
            (3, lim_c, limits.at[1]),
            (4, w_mid, wm),
            (5, w_low, wl),
        ]
    ]
    load_out = pltpu.make_async_copy(w_out, wo, local_sem.at[1])
    send1, send2 = local_sem.at[0], local_sem.at[1]
    odd = col % 2 == 1

    def mutual(dr, dc):
        return jnp.logical_and(row == (0 if dr > 0 else 1), odd if dc > 0 else jnp.logical_not(odd))

    def leads(dr, dc):
        there = exists(dr, dc)
        return there if dr > 0 else jnp.logical_and(there, odd)

    def greets(dr, dc):
        there = exists(dr, dc)
        if dr < 0:
            return jnp.logical_and(there, mutual(dr, dc)) if dc else None
        return leads(dr, dc)

    def greeted_by(dr, dc):
        there = exists(dr, dc)
        if dr > 0:
            return jnp.logical_and(there, mutual(dr, dc)) if dc else None
        return there if dr < 0 else jnp.logical_and(there, jnp.logical_not(odd))

    def alone(test, other):
        return test if other is None else jnp.logical_and(test, jnp.logical_not(other))

    barrier = pltpu.get_barrier_semaphore()
    earlier = 0

    def greet(entries):
        for dr, dc in entries:
            test = greets(dr, dc)
            if test is not None:

                @pl.when(test)
                def _():
                    pl.semaphore_signal(
                        barrier, inc=1, device_id=device(dr, dc), device_id_type=MESH
                    )

    loads[0].start()
    greet([e for e in AROUND if e[0] < 0])
    for load in loads[1:]:
        load.start()
    greet([e for e in AROUND if e[0] >= 0])
    for dr, dc in AROUND:
        test = greeted_by(dr, dc)
        if test is not None:
            earlier += test.astype(jnp.int32)

    def slot_of(dr, dc):
        up_down, left_right = (dr + 1) // 2, (dc + 1) // 2
        if dr == 0:
            return rims.at[pl.ds(2 * left_right, 2)]
        if dc == 0:
            return rims.at[pl.ds(12 + 2 * up_down, 2)]
        return rims.at[pl.ds(4 + 4 * left_right + 2 * up_down, 2)]

    def packed(dr, dc):
        return side_out.at[(dc + 1) // 2] if dr == 0 else vert_out.at[(dr + 1) // 2]

    def rows_of(slot, dr):
        if dr == 0:
            return cells.at[slot]
        return cells.at[slot, :, pl.ds(0 if dr < 0 else lat.shape[1] - HALO, HALO)]

    def copies(k, dr, dc):
        first = pltpu.make_async_remote_copy(
            src_ref=rows_of(4, dr),
            dst_ref=rows_of((1 - dr) * 3 + 1 - dc, dr),
            send_sem=send1,
            recv_sem=recv1,
            device_id=device(dr, dc),
            device_id_type=MESH,
        )
        second = pltpu.make_async_remote_copy(
            src_ref=packed(dr, dc),
            dst_ref=slot_of(-dr, -dc),
            send_sem=send2,
            recv_sem=recv2,
            device_id=device(dr, dc),
            device_id_type=MESH,
        )
        return first, second

    above_below = (row > 0).astype(jnp.int32) + (row < nr - 1).astype(jnp.int32)
    beside = (col > 0).astype(jnp.int32) + (col < nc - 1).astype(jnp.int32)

    def for_all(wait):
        for v in range(min(nr, 2) - 1, min(nr, 3)):
            for h in range(min(nc, 2) - 1, min(nc, 3)):
                if v + h == 0:
                    continue

                @pl.when(jnp.logical_and(above_below == v, beside == h))
                def _():
                    wait(v + v * h + lat.shape[1] // HALO * h, 2 * (v + h + v * h))

    def batch(ref, n, send, recv):
        part = ref.at[pl.ds(0, n), :, pl.ds(0, HALO)] if ref is cells else ref.at[pl.ds(0, n)]
        return pltpu.make_async_remote_copy(
            src_ref=part,
            dst_ref=part,
            send_sem=send,
            recv_sem=recv,
            device_id=device(0, 0),
            device_id_type=MESH,
        )

    for k, (dr, dc) in enumerate(AROUND):

        @pl.when(jnp.logical_not(exists(dr, dc)))
        def _():
            slot = cells.at[(1 + dr) * 3 + 1 + dc]
            slot[...] = jnp.zeros(slot.shape, BF16)
            pixels = slot_of(dr, dc)
            pixels[...] = jnp.zeros(pixels.shape, BF16)

    @pl.when(earlier > 0)
    def _():
        pl.semaphore_wait(barrier, earlier)

    hurry = jnp.logical_or(greeted_by(1, -1), greeted_by(1, 1))

    @pl.when(hurry)
    def _():
        loads[0].wait()
        for k, dc in ((7, 1), (5, -1)):

            @pl.when(greeted_by(1, dc))
            def _():
                copies(k, 1, dc)[0].start()

    for k, (dr, dc) in FAR_FIRST:
        if dr <= 0:
            by = greeted_by(dr, dc)

            @pl.when(alone(by, greets(dr, dc) if dr * dc else None))
            def _():
                pl.semaphore_signal(
                    ready.at[READY[7 - k]], inc=1, device_id=device(dr, dc), device_id_type=MESH
                )

    @pl.when(jnp.logical_not(hurry))
    def _():
        loads[0].wait()

    for k, (dr, dc) in FAR_FIRST:
        if dr <= 0:

            @pl.when(greeted_by(dr, dc))
            def _():
                copies(k, dr, dc)[0].start()

    def send_later(entries, when=None):
        for k, (dr, dc) in entries:
            test = alone(leads(dr, dc), greeted_by(dr, dc) if dr else None)

            @pl.when(test if when is None else jnp.logical_and(test, when))
            def _():
                pl.semaphore_wait(ready.at[READY[k]], 1)
                copies(k, dr, dc)[0].start()

    below = [e for e in enumerate(AROUND) if e[1][0] > 0]
    send_later(below, hurry)

    @pl.when(jnp.logical_and(odd, beside > 0))
    def _():
        pl.semaphore_wait(ready.at[READY[3]], beside)

    for k, dc in ((3, -1), (4, 1)):

        @pl.when(leads(0, dc))
        def _():
            copies(k, 0, dc)[0].start()


    tile = lat.shape[1]
    side_cells = tile + 2 * HALO
    margin, inner = 4 * HALO, 4 * tile
    size = inner + 2 * margin
    chans = lat.shape[0]
    span = size * side_cells
    half = span // 2
    wide = chans * side_cells

    loads[1].wait()
    load_out.start()
    wi32[...] = jnp.zeros(wi32.shape, F32)
    wi32[:, 0 : wi.shape[1], :] = wi[...].astype(F32)
    wi72 = wi32[...].reshape(72, wi32.shape[2]).astype(BF16)
    src, dst = iota((384, 72), 0), iota((384, 72), 1)
    pick = (
        (dst // 8 == 3 * (src % 128 // wide) + src // 128)
        & (dst % 8 == (src // side_cells) % chans)
        & (src % 128 < 3 * wide)
    )
    wc[...] = dot(pick.astype(F32).astype(BF16), wi72).astype(BF16)
    pltpu.make_async_copy(tables, tables, local_sem.at[2]).wait()
    pltpu.make_async_copy(limits, limits, local_sem.at[3]).wait()

    spread_r = (iota((size, span), 1) // side_cells == iota((size, span), 0)).astype(F32)
    spread_c = [
        (4 * (iota((size, span), 1) % side_cells) + q == iota((size, span), 0)).astype(F32)
        for q in range(4)
    ]
    spread_c = jnp.concatenate(spread_c, axis=1)
    row_w = dot(table_rows(tables[0].astype(F32), limits.at[0], row, nr, margin, inner), spread_r.astype(BF16))
    col_w = dot(table_rows(tables[1].astype(F32), limits.at[1], col, nc, margin, inner), spread_c.astype(BF16))
    lane = iota((1, span), 1)
    r_of, b_of = lane // side_cells, lane % side_cells
    inside = (
        (r_of >= margin) & (r_of < margin + inner) & (b_of >= HALO) & (b_of < HALO + tile)
    )
    for q in range(4):
        cw = col_w[:, q * span : (q + 1) * span]
        blend[q] = jnp.broadcast_to(row_w[0:1] * cw[0:1], (8, span))
        upper = jnp.broadcast_to((row_w[0:1] * cw[0:1])[:, :half], (8, half))
        blend_up[q] = pltpu.roll(upper, half // 2, 1) if q % 2 else upper
        inverse[q] = jnp.broadcast_to(
            1.0 / jnp.where(inside, row_w[1:2] * cw[1:2], 1.0), (8, span)
        )

    send_later(below, jnp.logical_not(hurry))

    load_out.wait()
    wo32[...] = jnp.zeros(wo32.shape, F32)
    wo32[:, 0 : wo.shape[1], :] = wo[...].astype(F32)
    loads[6].wait()
    out_mid = wm.shape[1]
    for t in range(9):
        turned = wm[BY_COLUMN[t]].T
        for n in range(out_mid // 128):
            at = 128 * (9 * n + t)
            wmt[:, at : at + 128] = turned[:, 128 * n : 128 * (n + 1)]
    loads[7].wait()
    out_low = wl.shape[1]
    for t in range(9):
        wlt[:, out_low * t : out_low * (t + 1)] = wl[BY_COLUMN[t]].T

    where_b = iota((4, half), 1) % side_cells
    lower_half = iota((4, half), 1) < half // 2
    place_src, place_dst = iota((4 * half, inner), 0), iota((4 * half, inner), 1)
    place = place_dst == 4 * (place_src % side_cells - HALO) + place_src // half
    places[0] = place.astype(F32).astype(BF16)
    slot = place_src % side_cells
    from_left = place_dst == 4 * (slot % HALO) + slot // HALO
    from_right = place_dst == 4 * (tile - HALO + slot % HALO) + slot // HALO
    pair_q = 2 * (place_src // half - 2) + place_src % half // (half // 2)
    beside_by = jnp.where(slot < HALO, tile, jnp.where(slot < HALO + tile, 0, -tile))
    from_pair = place_dst == 4 * (slot - HALO + beside_by) + pair_q
    part = place_src // half
    places[1] = jnp.where(
        part == 0, from_left.astype(F32), jnp.where(part == 1, from_right.astype(F32), from_pair.astype(F32))
    ).astype(BF16)
    for h in range(2):
        here = [inverse[q, 0:4, h * half : (h + 1) * half] for q in range(4)]
        sides = []
        for rim in (HALO, tile):
            dense = pltpu.roll(here[0], (half - rim) % half, 1)
            for q in range(1, 4):
                turned = pltpu.roll(here[q], (HALO * q - rim) % half, 1)
                dense = jnp.where(where_b // HALO == q, turned, dense)
            sides.append(dense)
        for pair in range(2):
            even, odds = here[2 * pair], here[2 * pair + 1]
            if h == 0:
                even = pltpu.roll(even, half // 2, 1)
            else:
                odds = pltpu.roll(odds, half // 2, 1)
            inner_scale = jnp.where(lower_half, even, odds)
            onward = pltpu.roll(inner_scale, half - tile, 1)
            back = pltpu.roll(inner_scale, tile, 1)
            outer_scale = jnp.where(where_b < HALO, onward, back)
            within = jnp.logical_and(where_b >= HALO, where_b < HALO + tile)
            sides.append(jnp.where(within, inner_scale, outer_scale))
        for n, side in enumerate(sides):
            scales[h, n] = side

    lined[...] = jnp.zeros(lined.shape, F32)
    for_all(lambda n, m: batch(cells, n, send1, recv1).wait_recv())

    pieces = [[], [], []]
    cuts = (slice(tile - HALO, tile), slice(0, tile), slice(0, HALO))
    for c in range(chans):
        for j, cut in enumerate(cuts):
            at = 1
            for i in range(3):
                block = cells[3 * i + j, c].astype(F32)[cuts[i], :]
                lined[c, j, at : at + block.shape[0], 0:tile] = block
                at += block.shape[0]
            for dy in range(3):
                pieces[dy].append(lined[c, j, dy : dy + side_cells, cut])
    pieces = pieces[0] + pieces[1] + pieces[2]
    tall = jnp.concatenate(pieces + [jnp.zeros((side_cells, 128 - 3 * wide), F32)], axis=1)
    shape = (side_cells, side_cells, 128)
    spreaded = jnp.broadcast_to(tall[:, None, :], shape)
    gap = iota(shape, 2) % side_cells - iota(shape, 1)
    patches = [jnp.where(gap == dx - 1, spreaded, 0.0) for dx in range(3)]
    patches = jnp.concatenate(patches, axis=2).reshape(-1, 384).astype(BF16)
    first = dot(patches, wc[...]).reshape(side_cells, side_cells, -1)
    (first,) = group_silu([first], first.shape[2] // NGROUPS)
    first = first.reshape(side_cells * side_cells, -1).astype(BF16)

    taps = dot(first, wmt[...])
    chunks = []
    for n in range(out_mid // 128):
        part = [
            taps[:, 128 * (9 * n + t) : 128 * (9 * n + t + 1)].reshape(side_cells, side_cells, -1)
            for t in BY_COLUMN
        ]
        part = conv_up([[part]], 1)
        part = [part[py][px] for py in range(2) for px in range(2)]
        chunks.append(group_silu(part, out_mid // NGROUPS))
    second = [jnp.concatenate(parts, axis=2) for parts in zip(*chunks)]
    second = jnp.concatenate(second, axis=0)
    second = second.reshape(-1, second.shape[2]).astype(BF16)

    n = side_cells * side_cells
    products = dot(second, wlt[...])
    products = [products[:, out_low * t : out_low * (t + 1)] for t in BY_COLUMN]
    taps = [
        [
            [
                p[(2 * py + px) * n : (2 * py + px + 1) * n].reshape(side_cells, side_cells, -1)
                for p in products
            ]
            for px in range(2)
        ]
        for py in range(2)
    ]
    third = conv_up(taps, 2)
    third = [third[qy][qx] for qy in range(4) for qx in range(4)]
    terms = group_terms(third, out_low // NGROUPS)

    wo72 = wo32[...].reshape(72, wo32.shape[2]).astype(BF16)
    def colours(lo, hi):
        got = []
        for pair in range(2):
            rows = [
                jnp.stack([silu(third[4 * qy + qx][lo:hi], terms) for qy in range(4)], axis=1)
                for qx in (2 * pair, 2 * pair + 1)
            ]
            rows = jnp.concatenate([r.reshape(-1, r.shape[-1]) for r in rows], axis=0)
            both = nt_dot(wo72, rows.astype(BF16))
            got += [both[:, :half], both[:, half:]]
        return got

    def blended(colour, weight, turn):
        lanes = colour[0].shape[1]
        def tap(q, t):
            return colour[q][8 * t : 8 * t + 8]

        def moved(x, dy, dx, by):
            at = (iota((8, lanes), 1) + lanes - by) % lanes
            sub_b, sub_r = at % side_cells, at // side_cells
            row_ok = [sub_r > 0, None, sub_r < lanes // side_cells - 1]
            col_ok = [sub_b > 0, None, sub_b < side_cells - 1]
            shift = (side_cells * (1 - dy) + 1 - dx + by) % lanes
            x = pltpu.roll(x, shift, 1) if shift else x
            ok = [m for m in (row_ok[dy], col_ok[dx]) if m is not None]
            return jnp.where(functools.reduce(jnp.logical_and, ok), x, 0.0) if ok else x

        values = []
        for q in range(4):
            value, by = None, turn * (q % 2)
            for dy in range(3):
                near = tap(q, 3 * dy + 1)
                if q > 0:
                    near = near + tap(q - 1, 3 * dy)
                if q < 3:
                    near = near + tap(q + 1, 3 * dy + 2)
                term = moved(near, dy, 1, by)
                if q == 0:
                    term = term + moved(tap(3, 3 * dy), dy, 0, by)
                if q == 3:
                    term = term + moved(tap(0, 3 * dy + 2), dy, 2, by)
                value = term if value is None else value + term
            values.append(value * weight[q])
        return values

    def pack_side(x, rim):
        dense = pltpu.roll(x[0], (half - rim) % half, 1)
        for q in range(1, 4):
            turned = pltpu.roll(x[q], (HALO * q - rim) % half, 1)
            dense = jnp.where(where_b // HALO == q, turned, dense)
        return dense

    def pack_pair(x, pair):
        even = pltpu.roll(x[2 * pair], half // 2, 1)
        return jnp.where(lower_half, even, x[2 * pair + 1])

    def send_rims(wanted):
        for k, (dr, dc) in FAR_FIRST:
            if wanted(dr):

                @pl.when(exists(dr, dc))
                def _():
                    copies(k, dr, dc)[1].start()

    middle = side_cells // 2
    upper = colours(0, middle)
    up_rows = [v[0:4] for v in blended(upper, blend_up, half // 2)]
    for pair in range(2):
        both = jnp.where(lower_half, up_rows[2 * pair], up_rows[2 * pair + 1])
        vert_out[0, pair] = both.astype(BF16)
    send_rims(lambda dr: dr < 0)
    for_all(lambda n, m: batch(cells, n, send1, recv1).wait_send())

    lower = colours(middle, side_cells)
    both = [jnp.concatenate([a, b], axis=1) for a, b in zip(upper, lower)]
    values = blended(both, blend, 0)
    for h in range(2):
        here = [v[0:4, h * half : (h + 1) * half] for v in values]
        for q in range(4):
            own[h, q] = here[q]
        for k, rim in ((0, 0), (1, side_cells - HALO)):
            side_out[k, h] = pack_side(here, rim).astype(BF16)
    for pair in range(2):
        vert_out[1, pair] = pack_pair(here, pair).astype(BF16)
    send_rims(lambda dr: dr >= 0)

    lane_row = iota((8, half), 1) // side_cells
    sublane = iota((8, half), 0)
    keep = [lane_row == sublane + 8, lane_row == sublane]
    beyond_row = [lane_row % 8 == sublane, lane_row % 8 == sublane]

    def spread_rows(piece, c, mask):
        return jnp.where(mask, jnp.broadcast_to(piece[c : c + 1], (8, half)), 0.0)

    def placed(blocks, place):
        tall = jnp.concatenate(blocks, axis=0)
        top = tall.astype(BF16)
        low = (tall - top.astype(F32)).astype(BF16)
        got = dot(jnp.concatenate([top, low], axis=0), place)
        return got[: tall.shape[0]] + got[tall.shape[0] :]

    blocks = []
    for c in range(3):
        for h in range(2):
            mine = [own[h, q] * inverse[q, 0:4, h * half : (h + 1) * half] for q in range(4)]
            blocks.append(jnp.concatenate([spread_rows(p, c, keep[h]) for p in mine], axis=1))
    mine = placed(blocks, places[0])

    for_all(lambda n, m: batch(rims, m, send2, recv2).wait_recv())

    blocks = []
    for c in range(3):
        for h in range(2):
            got = [
                rims[h].astype(F32) * scales[h, 0],
                rims[2 + h].astype(F32) * scales[h, 1],
            ]
            for pair in range(2):
                left, right, straight = (rims[at + 2 * h + pair].astype(F32) for at in (4, 8, 12))
                straight = jnp.where(where_b < HALO, right, straight)
                straight = jnp.where(where_b < HALO + tile, straight, left)
                got.append(straight * scales[h, 2 + pair])
            masks = [keep[h], keep[h], beyond_row[h], beyond_row[h]]
            blocks.append(
                jnp.concatenate([spread_rows(p, c, m) for p, m in zip(got, masks)], axis=1)
            )
    rest = dot(jnp.concatenate(blocks, axis=0).astype(BF16), places[1])
    out[...] = (mine + rest).reshape(3, inner, inner)

    for_all(lambda n, m: batch(rims, m, send2, recv2).wait_send())


def kernel(nr, nc, *refs):
    def scoped(local_sem):
        body(nr, nc, *refs, local_sem)

    pl.run_scoped(scoped, pltpu.SemaphoreType.DMA((6,)))


def solution(mesh):
    nr, nc = mesh.shape["rows"], mesh.shape["cols"]

    def per_device(lat, w_in, w_mid, w_low, w_out, ramp_r, ramp_c, lim_r, lim_c):
        tile = lat.shape[1]
        inner = 4 * tile
        size = inner + 8 * HALO
        half = size * (tile + 2 * HALO) // 2
        anywhere = pl.BlockSpec(memory_space=pltpu.HBM)
        dma = pltpu.SemaphoreType.DMA
        return pl.pallas_call(
            functools.partial(kernel, nr, nc),
            out_shape=pltpu.VMEM((w_out.shape[1], inner, inner), F32),
            in_specs=[anywhere] * 9,
            out_specs=pl.BlockSpec(memory_space=pltpu.VMEM),
            scratch_shapes=[
                pltpu.VMEM((max(9, 6 + 2 * (lat.shape[1] // HALO)),) + lat.shape, BF16),
                pltpu.VMEM((lat.shape[0], 3, 16, 128), F32),
                pltpu.VMEM(w_in.shape, BF16),
                pltpu.VMEM(w_mid.shape, BF16),
                pltpu.VMEM(w_low.shape, BF16),
                pltpu.VMEM(w_out.shape, BF16),
                pltpu.VMEM((2,) + ramp_r.shape, jnp.int32),
                pltpu.SMEM((2,) + lim_r.shape, jnp.int32),
                pltpu.VMEM((9, 8, w_in.shape[2]), F32),
                pltpu.VMEM((9, 8, w_out.shape[2]), F32),
                pltpu.VMEM((384, w_in.shape[2]), BF16),
                pltpu.VMEM((w_mid.shape[2], 9 * w_mid.shape[1]), BF16),
                pltpu.VMEM((w_low.shape[2], 9 * w_low.shape[1]), BF16),
                pltpu.VMEM((4, 8, 2 * half), F32),
                pltpu.VMEM((4, 8, 2 * half), F32),
                pltpu.VMEM((2, 4 * half, inner), BF16),
                pltpu.VMEM((4, 8, half), F32),
                pltpu.VMEM((2, 4, 4, half), F32),
                pltpu.VMEM((2, 4, 4, half), F32),
                pltpu.VMEM((2, 2, 4, half), BF16),
                pltpu.VMEM((2, 2, 4, half), BF16),
                pltpu.VMEM((16, 4, half), BF16),
                pltpu.SemaphoreType.REGULAR((4,)),
                dma,
                dma,
            ],
            compiler_params=pltpu.CompilerParams(
                collective_id=0, has_side_effects=True
            ),
            name="decode",
        )(lat, w_in, w_mid, w_low, w_out, ramp_r, ramp_c, lim_r, lim_c)

    return jax.shard_map(
        per_device,
        mesh=mesh,
        in_specs=(P(None, ("groups", "rows"), "cols"), P(), P(), P(), P(), P(), P(), P(), P()),
        out_specs=P(None, ("groups", "rows"), "cols"),
        check_vma=False,
    )
```
